32 devices in a mesh: grp: 2 (over y), lat: 4 (over z), lon: 2 (over x), ch: 2 (over core).
Axes of the slice: x: 2, y: 2, z: 4, core: 2. Of those that a mesh axis runs over, the one named last changes fastest.
Arguments:
- noisy_state: bfloat16 [256, 32, 512], P(('grp', 'ch'), 'lat', 'lon'), parts along dimension 0, may hold values from -6 to 6
- kernel_in: bfloat16 [3, 3, 128, 128], replicated, may hold values from -0.1875 to 0.1875
- bias_in: float32 [128], replicated, may hold values from -4 to 4
- kernel_out: bfloat16 [3, 3, 128, 128], replicated, may hold values from -0.1875 to 0.1875
- interp_weight: bfloat16 [64, 128, 128], P(('grp', 'lat', 'lon')), parts along dimension 0, may hold values from -0.5 to 0.5
- observed: bfloat16 [64, 128, 128], P(('grp', 'lat', 'lon'), 'ch'), parts along dimension 0, may hold values from -6 to 6
- obs_precision: bfloat16 [64, 128], P(('grp', 'lat', 'lon')), parts along dimension 0, may hold values from 0.29882812 to 3
- dest_tile: int32 [64], P(('grp', 'lat', 'lon')), parts along dimension 0, may hold values from 0 to 3, as said below
- row_offset: int32 [64], P(('grp', 'lat', 'lon')), parts along dimension 0, may hold values from 0 to 4
- col_offset: int32 [64], P(('grp', 'lat', 'lon')), parts along dimension 0, may hold values from 0 to 224
Outputs:
- next_state: float32 [256, 32, 512], P(('grp', 'ch'), 'lat', 'lon'), parts along dimension 0
- innovation: bfloat16 [64, 128, 128], P(('grp', 'lat', 'lon'), 'ch'), parts along dimension 0
The draws below stay inside these ranges and needn't reach their ends.
There are 2 independent parts, one for each index of `grp`. The reference program is written for one: setup_inputs(seed, part) draws one part's arguments, and reference() takes and returns one part's arrays. A program takes and returns all parts, laid end to end along the dimension named above; an argument that names none is the same for every part. Nothing has to cross between parts.
Inputs may be any that keep to these rules, and one draw needn't show every extreme that they name: `dest_tile`: the 4 blocks of one device name any one latitude tile at most 2 times; a block's tile lies in the longitude column of the device that holds the block.
All inputs are finite; a program needn't handle non-finite values.
Results may differ from the reference program's by a relative error of at most 0.0085.
Values may be sent and summed in bfloat16 or wider, within the bound.
No kernel may reach another device: no remote copies, remote signals or barrier semaphores. Data moves between devices by JAX's collectives and lax.ppermute only.
A program may use at most 64 MiB of HBM per device.

```python
import math
import jax
import jax.numpy as jnp
from jax import lax

C = 128
TH = 8
TW = 256
OBS = 128
PH = 4
PW = 32
CAP = 2
P_SIZE = 128
NB_DEV = 4
BLOCKS = 32
GRID_LAT = 32
GRID_LON = 512
N_LAT = 4
N_LON = 2


def draw_dest_tile(key, part):
    base = jax.random.fold_in(key, 101)
    key_busiest, key_popular, key_scores, key_reorder = jax.random.split(base, 4)
    sources = N_LAT * N_LON
    entries = N_LAT * CAP
    busiest = jax.random.randint(key_busiest, (), 0, N_LAT)
    popular = jax.random.randint(key_popular, (N_LAT,), 0, 4)
    entry_tile = jnp.arange(entries, dtype=jnp.int32) // CAP
    random_part = jax.random.randint(key_scores, (sources, entries), 0, 65536)
    scores = random_part + popular[entry_tile][None, :] * 16384 + jnp.where(entry_tile == busiest, 1048576, 0)[None, :]
    scores = scores * entries + jnp.arange(entries, dtype=jnp.int32)[None, :]
    picked = lax.top_k(scores, NB_DEV)[1]
    lat_tiles = picked // CAP
    reorder_key = jax.random.randint(key_reorder, (sources, NB_DEV), 0, 65536) * NB_DEV + jnp.arange(NB_DEV, dtype=jnp.int32)[None, :]
    reorder = jnp.argsort(reorder_key, axis=1, stable=True)
    return jnp.take_along_axis(lat_tiles, reorder, axis=1).reshape(-1).astype(jnp.int32)


def place_ends(drawn, stream_key, least, largest):
    longest = drawn.shape.index(max(drawn.shape))
    spots = []
    for shift in (0, 1):
        where = [jax.random.randint(jax.random.fold_in(stream_key, axis), (), 0, length) for axis, length in enumerate(drawn.shape)]
        where[longest] = (where[longest] + shift) % drawn.shape[longest]
        spots.append(tuple(where))
    return drawn.at[spots[0]].set(least).at[spots[1]].set(largest)


def steps_of(key, extent, shards, low, top_value):
    level, own = 1.0, jax.random.fold_in(key, 6)
    for axis_at, shards_of in shards:
        draws = jnp.exp(jax.random.uniform(jax.random.fold_in(own, axis_at), (shards_of,), jnp.float32, low / len(shards), top_value / len(shards)))
        level = level * jnp.repeat(draws, extent[axis_at] // shards_of).reshape([-1 if axis == axis_at else 1 for axis in range(len(extent))])
    return level


def gaussian(rng, extent, deviation, most, cuts=(), held_as=jnp.bfloat16):
    result = jax.random.normal(rng, extent, jnp.float32) * deviation
    if len(cuts) > 0:
        result = steps_of(rng, extent, cuts, -0.22, 0.18) * result
    return jnp.clip(result, min=-most, max=most).astype(held_as)


def setup_inputs(seed: int = 0, part: int = 0) -> dict:
    splits = jax.random.split(jax.random.key(seed), 11)
    own_keys = jax.random.split(jax.random.fold_in(splits[10], part), 11)
    noisy_state = gaussian(own_keys[0], (C, GRID_LAT, GRID_LON), 1.0, 6.0, ((0, 2), (1, 4), (2, 2)))
    kernel_in = gaussian(splits[1], (3, 3, C, C), (9 * C) ** -0.5, 0.1875)
    bias_in = gaussian(splits[2], (C,), 1.0, 4.0, (), jnp.float32)
    kernel_out = gaussian(splits[3], (3, 3, C, C), (9 * C) ** -0.5, 0.1875)
    interp_weight = gaussian(own_keys[4], (BLOCKS, OBS, P_SIZE), P_SIZE ** -0.5, 0.5, ((0, 8),))
    observed = gaussian(own_keys[5], (BLOCKS, C, OBS), 1.0, 6.0, ((0, 8), (1, 2)))
    obs_precision = jnp.clip(jnp.exp(math.log(3.0) - 2.306499 * jax.random.uniform(own_keys[6], (BLOCKS, OBS), jnp.float32) ** steps_of(own_keys[6], (BLOCKS, OBS), ((0, 8),), -0.2, 0.2)), 0.29882812, 3.0).astype(jnp.bfloat16)
    dest_tile = draw_dest_tile(jax.random.fold_in(jax.random.fold_in(splits[10], part), 71), part)
    row_offset = place_ends(jax.random.randint(own_keys[8], (BLOCKS,), 0, TH - PH + 1), jax.random.fold_in(own_keys[8], 1), 0, TH - PH).astype(jnp.int32)
    col_offset = place_ends(jax.random.randint(own_keys[9], (BLOCKS,), 0, TW - PW + 1), jax.random.fold_in(own_keys[9], 1), 0, TW - PW).astype(jnp.int32)
    return {"noisy_state": noisy_state, "kernel_in": kernel_in, "bias_in": bias_in, "kernel_out": kernel_out, "interp_weight": interp_weight, "observed": observed, "obs_precision": obs_precision, "dest_tile": dest_tile, "row_offset": row_offset, "col_offset": col_offset}


def pad_field(grid_field):
    taller = jnp.pad(grid_field, ((0, 0), (1, 1), (0, 0)))
    return jnp.concatenate([taller[:, :, -1:], taller, taller[:, :, :1]], axis=2)


def convolve(grid_field, kernel):
    padded = pad_field(grid_field)
    channels, grid_rows, grid_cols = grid_field.shape
    summed = jnp.zeros((kernel.shape[2], grid_rows * grid_cols), jnp.float32)
    for tap_row in range(3):
        for tap_col in range(3):
            window = padded[:, tap_row:tap_row + grid_rows, tap_col:tap_col + grid_cols].reshape(channels, grid_rows * grid_cols)
            summed = summed + jnp.dot(kernel[tap_row, tap_col], window, preferred_element_type=jnp.float32)
    return summed.reshape(kernel.shape[2], grid_rows, grid_cols)


def adjoint_kernel(kernel):
    return jnp.transpose(kernel[::-1, ::-1], (0, 1, 3, 2))


def extract(grid_field, patch_rows, patch_cols):
    def take_one(row_start, col_start):
        return lax.dynamic_slice(grid_field, (jnp.zeros((), jnp.int32), row_start, col_start), (grid_field.shape[0], PH, PW))
    return jax.vmap(take_one)(patch_rows, patch_cols)


def spread(grad_patch, patch_rows, patch_cols, grid_shape):
    cell_rows = patch_rows[:, None, None] + lax.broadcasted_iota(jnp.int32, (1, PH, 1), 1)
    cell_cols = patch_cols[:, None, None] + lax.broadcasted_iota(jnp.int32, (1, 1, PW), 2)
    return jnp.zeros(grid_shape, jnp.float32).at[:, cell_rows, cell_cols].add(jnp.moveaxis(grad_patch, 1, 0))


def reference(noisy_state, kernel_in, bias_in, kernel_out, interp_weight, observed, obs_precision, dest_tile, row_offset, col_offset):
    pre_act = convolve(noisy_state, kernel_in) + bias_in[:, None, None]
    hidden = jax.nn.silu(pre_act).astype(jnp.bfloat16)
    denoised = (noisy_state.astype(jnp.float32) + convolve(hidden, kernel_out)).astype(jnp.bfloat16)
    blocks = dest_tile.shape[0]
    device_of = jnp.arange(blocks, dtype=jnp.int32) // NB_DEV
    patch_rows = (dest_tile * TH + row_offset).astype(jnp.int32)
    patch_cols = ((device_of % N_LON) * TW + col_offset).astype(jnp.int32)
    patches = extract(denoised, patch_rows, patch_cols).reshape(blocks, noisy_state.shape[0], PH * PW)
    predicted = jnp.einsum("scp,sop->sco", patches.astype(jnp.float32), interp_weight.astype(jnp.float32))
    residual = predicted - observed.astype(jnp.float32)
    innovation = residual.astype(jnp.bfloat16)
    weighted = (residual * obs_precision.astype(jnp.float32)[:, None, :]).astype(jnp.bfloat16)
    pulled = jnp.einsum("sco,sop->scp", weighted.astype(jnp.float32), interp_weight.astype(jnp.float32))
    grad_field = spread(pulled.reshape(blocks, noisy_state.shape[0], PH, PW), patch_rows, patch_cols, noisy_state.shape)
    grad_round = grad_field.astype(jnp.bfloat16)
    back_hidden = convolve(grad_round, adjoint_kernel(kernel_out))
    sigmoid_act = jax.nn.sigmoid(pre_act)
    grad_pre = (back_hidden * sigmoid_act * (1.0 + pre_act * (1.0 - sigmoid_act))).astype(jnp.bfloat16)
    grad_state = grad_field + convolve(grad_pre, adjoint_kernel(kernel_in))
    next_state = 0.6 * noisy_state.astype(jnp.float32) + 0.4 * denoised.astype(jnp.float32) - 0.3 * grad_state
    return next_state, innovation
```

```python
import functools

import jax
import jax.numpy as jnp
from jax import lax
from jax.experimental import pallas as pl
from jax.experimental.pallas import tpu as pltpu
from jax.sharding import PartitionSpec as P

PH = 4
PW = 32
CAP = 2
TAIL = 16
META = 16

keep_rate = 0.6
blend_rate = 0.4
guide_rate = 0.3

F32 = jnp.float32
BF16 = jnp.bfloat16
VMEM = pltpu.VMEM
SMEM = pltpu.SMEM


def call(kernel, out_shape, n_smem, n_vmem, scratch, name):
    return pl.pallas_call(
        kernel,
        out_shape=out_shape,
        in_specs=[pl.BlockSpec(memory_space=SMEM)] * n_smem + [pl.BlockSpec(memory_space=VMEM)] * n_vmem,
        out_specs=jax.tree.map(lambda _: pl.BlockSpec(memory_space=VMEM), out_shape),
        scratch_shapes=scratch,
        name=name,
    )


def weights_kernel(kin_ref, kout_ref, w1_ref, w2_ref, w3_ref, w4_ref):
    c = kin_ref.shape[-1]
    for w_ref, k_ref, adjoint in (
        (w1_ref, kin_ref, False),
        (w2_ref, kout_ref, False),
        (w3_ref, kout_ref, True),
        (w4_ref, kin_ref, True),
    ):
        for b in range(3):
            for row in range(2):
                at = (2 * b + row) * c
                for k in range(4):
                    a = k - row
                    if not 0 <= a < 3:
                        tap = jnp.zeros((c, c), BF16)
                    elif adjoint:
                        tap = k_ref[2 - a, 2 - b]
                    else:
                        tap = k_ref[a, b].astype(F32).T.astype(BF16)
                    w_ref[k * c : (k + 1) * c, at : at + c] = tap


def tail_of(row_ref, width):
    lane_rows = lax.broadcasted_iota(jnp.int32, (TAIL, row_ref.shape[-1]), 0)
    first = row_ref[0:TAIL, :].astype(F32)
    last = row_ref[width - TAIL : width, :].astype(F32)
    zero = jnp.zeros_like(first)
    return jnp.where(lane_rows < 2, first, jnp.where(lane_rows >= TAIL - 2, last, zero)).astype(BF16)


def write_edges(x_ref, top_ref, bottom_ref, tail_ref, tail_top_ref, tail_bottom_ref):
    rows, width = x_ref.shape[0], x_ref.shape[1]
    for i in range(2):
        top_ref[i] = x_ref[i]
        bottom_ref[i] = x_ref[rows - 2 + i]
    for h in range(rows):
        tail_ref[h] = tail_of(x_ref.at[h], width)
    for i in range(2):
        tail_top_ref[i] = tail_ref[i]
        tail_bottom_ref[i] = tail_ref[rows - 2 + i]


def prep_kernel(
    dest_ref,
    row_ref,
    col_ref,
    own_ref,
    other_ref,
    own_obs_ref,
    other_obs_ref,
    weight_ref,
    precision_ref,
    x_ref,
    top_ref,
    bottom_ref,
    tail_ref,
    tail_top_ref,
    tail_bottom_ref,
    chunk_ref,
    flat_ref,
    scale_ref,
):
    core = lax.axis_index("ch")
    half, rows, width = own_ref.shape
    obs = weight_ref.shape[1]
    cells = weight_ref.shape[2]
    blocks = weight_ref.shape[0]

    def place(ref, first):
        for part in range(width // 128):
            piece = ref[:, :, part * 128 : (part + 1) * 128].astype(F32)
            flat_ref[part, pl.ds(pl.multiple_of(first * rows, 8), half * rows), :] = piece.reshape(half * rows, 128)

    place(own_ref, core * half)
    place(other_ref, (1 - core) * half)
    for h in range(rows):
        for part in range(width // 128):
            plane = flat_ref[part, pl.ds(h, 2 * half, stride=rows), :]
            x_ref[h, part * 128 : (part + 1) * 128, :] = plane.T.astype(BF16)
    write_edges(x_ref, top_ref, bottom_ref, tail_ref, tail_top_ref, tail_bottom_ref)

    def clear(slot, _):
        chunk_ref[slot] = jnp.zeros(chunk_ref.shape[1:], BF16)
        return 0

    lax.fori_loop(0, chunk_ref.shape[0], clear, 0)
    scale_ref[...] = precision_ref[...].astype(F32)
    meta_rows = lax.broadcasted_iota(jnp.int32, (META, obs), 0)

    def pack(b, _):
        dest = dest_ref[b]
        rank = lax.fori_loop(0, b, lambda j, n: n + (dest_ref[j] == dest).astype(jnp.int32), 0)
        slot = dest * CAP + rank
        chunk_ref[slot, 0:obs, :] = weight_ref[b]
        chunk_ref[slot, pl.ds(pl.multiple_of(obs + core * half, 16), half), :] = own_obs_ref[b]
        chunk_ref[slot, pl.ds(pl.multiple_of(obs + (1 - core) * half, 16), half), :] = other_obs_ref[b]
        row = row_ref[b].astype(F32)
        high = lax.div(col_ref[b], 16).astype(F32)
        low = lax.rem(col_ref[b], 16).astype(F32)
        meta = jnp.where(
            meta_rows == 0,
            jnp.broadcast_to(scale_ref[pl.ds(b, 1), :], (META, obs)),
            jnp.where(meta_rows == 1, row, jnp.where(meta_rows == 2, high, low)),
        )
        chunk_ref[slot, obs + 2 * half : obs + 2 * half + META, :] = meta.astype(BF16)
        return 0

    lax.fori_loop(0, blocks, pack, 0)


def fill_extended(ext_ref, x_ref, tail_ref, up_ref, up_tail_ref, down_ref, down_tail_ref):
    rows, width = x_ref.shape[0], x_ref.shape[1]
    for i in range(2):
        ext_ref[i, 0:width, :] = up_ref[i]
        ext_ref[i, width : width + TAIL, :] = up_tail_ref[i]
        ext_ref[rows + 2 + i, 0:width, :] = down_ref[i]
        ext_ref[rows + 2 + i, width : width + TAIL, :] = down_tail_ref[i]
    for h in range(rows):
        ext_ref[h + 2, 0:width, :] = x_ref[h]
        ext_ref[h + 2, width : width + TAIL, :] = tail_ref[h]


def row_pair(src_ref, w_ref, first):
    c = src_ref.shape[-1]
    wide = src_ref.shape[1]
    lhs = jnp.concatenate([src_ref[first + k] for k in range(4)], axis=1)
    y = jnp.dot(lhs, w_ref[...], preferred_element_type=F32)
    out = []
    for row in range(2):
        left, mid, right = (y[:, (2 * b + row) * c : (2 * b + row + 1) * c] for b in range(3))
        out.append(pltpu.roll(left, 1, 0) + mid + pltpu.roll(right, wide - 1, 0))
    return out


def inside(ext_row, ext_rows):
    at = lax.axis_index("lat")
    last = lax.axis_size("lat") - 1
    return ((ext_row > 0) | (at > 0)) & ((ext_row < ext_rows - 1) | (at < last))


def forward_kernel(
    x_ref,
    tail_ref,
    up_ref,
    up_tail_ref,
    down_ref,
    down_tail_ref,
    w1_ref,
    w2_ref,
    bias_ref,
    block_ref,
    pre_ref,
    base_ref,
    g_ref,
    top_ref,
    bottom_ref,
    gtail_ref,
    tail_top_ref,
    tail_bottom_ref,
    inn_ref,
    ext_ref,
    hidden_ref,
    den_ref,
    field_ref,
):
    core = lax.axis_index("ch")
    rows, width, c = x_ref.shape
    half = inn_ref.shape[1]
    slots, obs = block_ref.shape[0], block_ref.shape[2]
    fill_extended(ext_ref, x_ref, tail_ref, up_ref, up_tail_ref, down_ref, down_tail_ref)
    bias = bias_ref[...]

    def first_conv(g, _):
        for i, y in enumerate(row_pair(ext_ref, w1_ref, 2 * g)):
            r = 2 * g + i
            pre = y + bias
            pre_ref[r] = pre
            hidden = pre / (1.0 + jnp.exp(-pre))
            hidden_ref[r] = jnp.where(inside(r, rows + 2), hidden, 0.0).astype(BF16)
        return 0

    lax.fori_loop(0, (rows + 2) // 2, first_conv, 0)

    def second_conv(g, _):
        for i, y in enumerate(row_pair(hidden_ref, w2_ref, 2 * g)):
            r = 2 * g + i
            noisy = x_ref[r].astype(F32)
            den = (noisy + y[0:width, :]).astype(BF16).astype(F32)
            den_ref[r] = den
            base_ref[r] = keep_rate * noisy + blend_rate * den
            field_ref[r] = jnp.zeros((width, c), F32)
        return 0

    lax.fori_loop(0, rows // 2, second_conv, 0)

    def observe(slot, _):
        meta = block_ref[slot, obs + c : obs + c + META, :].astype(F32)
        row = jnp.max(meta[1:2, :]).astype(jnp.int32)
        col = jnp.max(meta[2:3, :]).astype(jnp.int32) * 16 + jnp.max(meta[3:4, :]).astype(jnp.int32)
        weight = block_ref[slot, 0:obs, :]
        patch = jnp.concatenate([den_ref[row + i, pl.ds(col, PW), :] for i in range(PH)], axis=0)
        predicted = lax.dot_general(
            patch.T.astype(BF16), weight, (((1,), (1,)), ((), ())), preferred_element_type=F32
        )
        residual = predicted - block_ref[slot, obs : obs + c, :].astype(F32)
        inn_ref[slot] = jnp.where(core == 0, residual[0:half], residual[half : 2 * half]).astype(BF16)
        weighted = (residual * meta[0:1, :]).astype(BF16)
        pulled = jnp.dot(weighted, weight, preferred_element_type=F32).T
        for i in range(PH):
            field_ref[row + i, pl.ds(col, PW), :] += pulled[i * PW : (i + 1) * PW, :]
        return 0

    lax.fori_loop(0, slots, observe, 0)

    for r in range(rows):
        field = field_ref[r]
        base_ref[r] -= guide_rate * field
        g_ref[r] = field.astype(BF16)
    write_edges(g_ref, top_ref, bottom_ref, gtail_ref, tail_top_ref, tail_bottom_ref)


def backward_kernel(
    x_ref,
    tail_ref,
    up_ref,
    up_tail_ref,
    down_ref,
    down_tail_ref,
    w3_ref,
    w4_ref,
    pre_ref,
    base_ref,
    next_ref,
    ext_ref,
    grad_ref,
    flat_ref,
):
    core = lax.axis_index("ch")
    rows, width, c = x_ref.shape
    half = next_ref.shape[0]
    fill_extended(ext_ref, x_ref, tail_ref, up_ref, up_tail_ref, down_ref, down_tail_ref)

    def first_conv(g, _):
        for i, y in enumerate(row_pair(ext_ref, w3_ref, 2 * g)):
            r = 2 * g + i
            pre = pre_ref[r]
            s = 1.0 / (1.0 + jnp.exp(-pre))
            grad = y * s * (1.0 + pre * (1.0 - s))
            grad_ref[r] = jnp.where(inside(r, rows + 2), grad, 0.0).astype(BF16)
        return 0

    lax.fori_loop(0, (rows + 2) // 2, first_conv, 0)

    for g in range(rows // 2):
        for i, y in enumerate(row_pair(grad_ref, w4_ref, 2 * g)):
            r = 2 * g + i
            out = base_ref[r] - guide_rate * y[0:width, :]
            for part in range(width // 128):
                plane = out[part * 128 : (part + 1) * 128, :].T
                own = jnp.where(core == 0, plane[0:half], plane[half : 2 * half])
                flat_ref[part, pl.ds(r, half, stride=rows), :] = own
    for part in range(width // 128):
        next_ref[:, :, part * 128 : (part + 1) * 128] = flat_ref[part].reshape(half, rows, 128)


def return_kernel(dest_ref, back_ref, inn_ref):
    def take(b, _):
        dest = dest_ref[b]
        rank = lax.fori_loop(0, b, lambda j, n: n + (dest_ref[j] == dest).astype(jnp.int32), 0)
        inn_ref[b] = back_ref[dest * CAP + rank]
        return 0

    lax.fori_loop(0, inn_ref.shape[0], take, 0)


def shifted(value, lat_step, lon_step):
    lats, lons = lax.axis_size("lat"), lax.axis_size("lon")
    pairs = [
        (i * lons + j, (i + lat_step) * lons + (j + lon_step) % lons)
        for i in range(lats)
        for j in range(lons)
        if 0 <= i + lat_step < lats
    ]
    return lax.ppermute(value, ("lat", "lon"), pairs)


def tails(value, lat_step):
    if lax.axis_size("lon") == 2:
        return shifted(value, lat_step, 1)
    from_right = shifted(value, lat_step, -1)
    from_left = shifted(value, lat_step, 1)
    at = lax.broadcasted_iota(jnp.int32, (1, TAIL, 1), 1)
    return jnp.where(at < TAIL // 2, from_right, from_left)


def exchanged(top, bottom, tail, tail_top, tail_bottom):
    up = shifted(bottom, 1, 0)
    down = shifted(top, -1, 0)
    beside = tails(tail, 0)
    up_tail = tails(tail_bottom, 1)
    down_tail = tails(tail_top, -1)
    return beside, up, up_tail, down, down_tail


def shape(dims, dtype):
    return jax.ShapeDtypeStruct(dims, dtype)


def edge_shapes(rows, width, c):
    return (
        shape((2, width, c), BF16),
        shape((2, width, c), BF16),
        shape((rows, TAIL, c), BF16),
        shape((2, TAIL, c), BF16),
        shape((2, TAIL, c), BF16),
    )


def body(
    noisy_state,
    kernel_in,
    bias_in,
    kernel_out,
    interp_weight,
    observed,
    obs_precision,
    dest_tile,
    row_offset,
    col_offset,
):
    half, rows, width = noisy_state.shape
    c = kernel_in.shape[-1]
    obs = interp_weight.shape[1]
    lats = lax.axis_size("lat")
    slots = lats * CAP
    wide = width + TAIL
    swap = [(0, 1), (1, 0)]
    other = lax.ppermute(noisy_state, "ch", swap)
    other_obs = lax.ppermute(observed, "ch", swap)
    w1, w2, w3, w4 = call(weights_kernel, (shape((4 * c, 6 * c), BF16),) * 4, 0, 2, [], "weights")(
        kernel_in, kernel_out
    )
    x, *edges, chunk = call(
        prep_kernel,
        (shape((rows, width, c), BF16), *edge_shapes(rows, width, c), shape((slots, obs + c + META, obs), BF16)),
        3,
        6,
        [VMEM((width // 128, c * rows, 128), F32), VMEM(obs_precision.shape, F32)],
        "prep",
    )(dest_tile, row_offset, col_offset, noisy_state, other, observed, other_obs, interp_weight, obs_precision)
    block = lax.all_to_all(chunk, "lat", split_axis=0, concat_axis=0, tiled=True)
    halo = exchanged(*edges)
    pre, base, g, *edges, inn = call(
        forward_kernel,
        (
            shape((rows + 2, wide, c), F32),
            shape((rows, width, c), F32),
            shape((rows, width, c), BF16),
            *edge_shapes(rows, width, c),
            shape((slots, half, obs), BF16),
        ),
        0,
        10,
        [
            VMEM((rows + 4, wide, c), BF16),
            VMEM((rows + 2, wide, c), BF16),
            VMEM((rows, width, c), F32),
            VMEM((rows, width, c), F32),
        ],
        "forward",
    )(x, *halo, w1, w2, bias_in.reshape(1, c), block)
    halo = exchanged(*edges)
    back = lax.all_to_all(inn, "lat", split_axis=0, concat_axis=0, tiled=True)
    next_state = call(
        backward_kernel,
        shape((half, rows, width), F32),
        0,
        10,
        [
            VMEM((rows + 4, wide, c), BF16),
            VMEM((rows + 2, wide, c), BF16),
            VMEM((width // 128, half * rows, 128), F32),
        ],
        "backward",
    )(g, *halo, w3, w4, pre, base)
    innovation = call(return_kernel, shape(observed.shape, BF16), 1, 1, [], "innovation")(dest_tile, back)
    return next_state, innovation


def solution(mesh):
    return jax.shard_map(
        body,
        mesh=mesh,
        in_specs=(
            P(("grp", "ch"), "lat", "lon"),
            P(),
            P(),
            P(),
            P(("grp", "lat", "lon"), None, None),
            P(("grp", "lat", "lon"), "ch", None),
            P(("grp", "lat", "lon"), None),
            P(("grp", "lat", "lon")),
            P(("grp", "lat", "lon")),
            P(("grp", "lat", "lon")),
        ),
        out_specs=(P(("grp", "ch"), "lat", "lon"), P(("grp", "lat", "lon"), "ch", None)),
        check_vma=False,
    )
```

```python
import functools

import jax
import jax.numpy as jnp
from jax import lax
from jax.experimental import pallas as pl
from jax.experimental.pallas import tpu as pltpu
from jax.sharding import PartitionSpec as P

PH = 4
PW = 32
CAP = 2
TAIL = 16
META = 16

keep_rate = 0.6
blend_rate = 0.4
guide_rate = 0.3

F32 = jnp.float32
BF16 = jnp.bfloat16
VMEM = pltpu.VMEM
SMEM = pltpu.SMEM
HBM = pltpu.MemorySpace.HBM
OUT = "out"


def call(kernel, outs, ins, scratch, name):
    near = lambda v, space: v if space == OUT else space(v.shape, v.dtype)
    spec = lambda space: pl.BlockSpec(memory_space=VMEM if space == OUT else space)
    run = pl.pallas_call(
        kernel,
        out_shape=[near(v, space) for v, space in outs],
        in_specs=[spec(space) for space in ins],
        out_specs=[spec(space) for _, space in outs],
        scratch_shapes=scratch,
        compiler_params=pltpu.CompilerParams(vmem_limit_bytes=24 * 1024 * 1024),
        name=name,
    )

    def apply(*args):
        return run(
            *(pltpu.with_memory_space_constraint(a, space) if space in (VMEM, HBM) else a for a, space in zip(args, ins))
        )

    return apply


def place_taps(w_ref, tap_of):
    c = w_ref.shape[0] // 4
    for b in range(3):
        for a in range(3):
            tap = tap_of(a, b)
            for row in range(2):
                at = (2 * b + row) * c
                w_ref[(a + row) * c : (a + row + 1) * c, at : at + c] = tap
        w_ref[3 * c : 4 * c, 2 * b * c : (2 * b + 1) * c] = jnp.zeros((c, c), BF16)
        w_ref[0:c, (2 * b + 1) * c : (2 * b + 2) * c] = jnp.zeros((c, c), BF16)


def weights_kernel(kin_ref, kout_ref, w1_ref, w2_ref):
    for w_ref, k_ref in ((w1_ref, kin_ref), (w2_ref, kout_ref)):
        place_taps(w_ref, lambda a, b: k_ref[a, b].astype(F32).T.astype(BF16))


def tail_of(row_ref, width):
    lane_rows = lax.broadcasted_iota(jnp.int32, (TAIL, row_ref.shape[-1]), 0)
    first = row_ref[0:TAIL, :].astype(F32)
    last = row_ref[width - TAIL : width, :].astype(F32)
    zero = jnp.zeros_like(first)
    return jnp.where(lane_rows < 2, first, jnp.where(lane_rows >= TAIL - 2, last, zero)).astype(BF16)


def write_edges(x_ref, edge_ref, tail_ref, edge_tail_ref):
    rows, width = x_ref.shape[0], x_ref.shape[1]
    first = lax.axis_index("ch") * (rows - 2)
    for h in range(rows):
        tail_ref[h] = tail_of(x_ref.at[h], width)
    for i in range(2):
        edge_ref[i] = x_ref[first + i]
        edge_tail_ref[i] = tail_ref[first + i]


def prep_kernel(
    dest_ref,
    row_ref,
    col_ref,
    own_ref,
    other_ref,
    own_obs_ref,
    other_obs_ref,
    weight_ref,
    precision_ref,
    x_ref,
    edge_ref,
    tail_ref,
    edge_tail_ref,
    chunk_ref,
    flat_ref,
    scale_ref,
):
    core = lax.axis_index("ch")
    half, rows, width = own_ref.shape
    obs = weight_ref.shape[1]
    cells = weight_ref.shape[2]
    blocks = weight_ref.shape[0]

    def place(ref, first):
        for part in range(width // 128):
            piece = ref[:, :, part * 128 : (part + 1) * 128].astype(F32)
            flat_ref[part, pl.ds(pl.multiple_of(first * rows, 8), half * rows), :] = piece.reshape(half * rows, 128)

    place(own_ref, core * half)
    place(other_ref, (1 - core) * half)
    for h in range(rows):
        for part in range(width // 128):
            plane = flat_ref[part, pl.ds(h, 2 * half, stride=rows), :]
            x_ref[h, part * 128 : (part + 1) * 128, :] = plane.T.astype(BF16)
    write_edges(x_ref, edge_ref, tail_ref, edge_tail_ref)

    def clear(slot, _):
        chunk_ref[slot] = jnp.zeros(chunk_ref.shape[1:], BF16)
        return 0

    lax.fori_loop(0, chunk_ref.shape[0], clear, 0)
    scale_ref[...] = precision_ref[...].astype(F32)
    meta_rows = lax.broadcasted_iota(jnp.int32, (META, obs), 0)

    def pack(b, _):
        dest = dest_ref[b]
        rank = lax.fori_loop(0, b, lambda j, n: n + (dest_ref[j] == dest).astype(jnp.int32), 0)

        @pl.when(rank == core)
        def _():
            fill(b, dest)

        return 0

    def fill(b, slot):
        chunk_ref[slot, 0:obs, :] = weight_ref[b]
        chunk_ref[slot, pl.ds(pl.multiple_of(obs + core * half, 16), half), :] = own_obs_ref[b]
        chunk_ref[slot, pl.ds(pl.multiple_of(obs + (1 - core) * half, 16), half), :] = other_obs_ref[b]
        row = row_ref[b].astype(F32)
        high = lax.div(col_ref[b], 16).astype(F32)
        low = lax.rem(col_ref[b], 16).astype(F32)
        meta = jnp.where(
            meta_rows == 0,
            jnp.broadcast_to(scale_ref[pl.ds(b, 1), :], (META, obs)),
            jnp.where(meta_rows == 1, row, jnp.where(meta_rows == 2, high, low)),
        )
        chunk_ref[slot, obs + 2 * half : obs + 2 * half + META, :] = meta.astype(BF16)

    lax.fori_loop(0, blocks, pack, 0)


def fill_extended(ext_ref, x_ref, tail_ref, mine_ref, mine_tail_ref, other_ref, other_tail_ref):
    rows, width = x_ref.shape[0], x_ref.shape[1]
    core = lax.axis_index("ch")
    for i in range(2):
        mine = core * (rows + 2) + i
        other = (1 - core) * (rows + 2) + i
        ext_ref[mine, 0:width, :] = mine_ref[i]
        ext_ref[mine, width : width + TAIL, :] = mine_tail_ref[i]
        ext_ref[other, 0:width, :] = other_ref[i]
        ext_ref[other, width : width + TAIL, :] = other_tail_ref[i]
    for h in range(rows):
        ext_ref[h + 2, 0:width, :] = x_ref[h]
        ext_ref[h + 2, width : width + TAIL, :] = tail_ref[h]


def row_pair(src_ref, w_ref, first):
    c = src_ref.shape[-1]
    wide = src_ref.shape[1]
    lhs = jnp.concatenate([src_ref[first + k] for k in range(4)], axis=1)
    y = jnp.dot(lhs, w_ref[...], preferred_element_type=F32)
    out = []
    for row in range(2):
        left, mid, right = (y[:, (2 * b + row) * c : (2 * b + row + 1) * c] for b in range(3))
        out.append(pltpu.roll(left, 1, 0) + mid + pltpu.roll(right, wide - 1, 0))
    return out


def inside(ext_row, ext_rows):
    at = lax.axis_index("lat")
    last = lax.axis_size("lat") - 1
    return ((ext_row > 0) | (at > 0)) & ((ext_row < ext_rows - 1) | (at < last))


def forward_kernel(
    x_ref,
    tail_ref,
    mine_ref,
    mine_tail_ref,
    other_ref,
    other_tail_ref,
    w1_ref,
    w2_ref,
    bias_ref,
    block_ref,
    other_block_ref,
    slope_out_ref,
    base_ref,
    g_ref,
    edge_ref,
    gtail_ref,
    edge_tail_ref,
    inn_ref,
    ext_ref,
    hidden_ref,
    den_ref,
    field_ref,
    slope_ref,
    save_sem,
):
    core = lax.axis_index("ch")
    rows, width, c = x_ref.shape
    half = inn_ref.shape[1]
    sources, obs = block_ref.shape[0], block_ref.shape[2]
    fill_extended(ext_ref, x_ref, tail_ref, mine_ref, mine_tail_ref, other_ref, other_tail_ref)
    bias = bias_ref[...]

    def first_conv(g, _):
        for i, y in enumerate(row_pair(ext_ref, w1_ref, 2 * g)):
            r = 2 * g + i
            pre = y + bias
            s = 1.0 / (1.0 + jnp.exp(-pre))
            slope_ref[r] = s * (1.0 + pre * (1.0 - s))
            hidden = pre * s
            hidden_ref[r] = jnp.where(inside(r, rows + 2), hidden, 0.0).astype(BF16)
        return 0

    lax.fori_loop(0, (rows + 2) // 2, first_conv, 0)
    save = pltpu.make_async_copy(slope_ref, slope_out_ref, save_sem)
    save.start()

    def second_conv(g, _):
        for i, y in enumerate(row_pair(hidden_ref, w2_ref, 2 * g)):
            r = 2 * g + i
            noisy = x_ref[r].astype(F32)
            den = (noisy + y[0:width, :]).astype(BF16).astype(F32)
            den_ref[r] = den
            base_ref[r] = keep_rate * noisy + blend_rate * den
            field_ref[r] = jnp.zeros((width, c), F32)
        return 0

    lax.fori_loop(0, rows // 2, second_conv, 0)

    def observe(source, cap):
        slot = source * CAP + cap

        def read(first, count):
            at = slice(first, first + count)
            return jnp.where(core == cap, block_ref[source, at, :], other_block_ref[source, at, :])

        meta = read(obs + c, META).astype(F32)
        row = jnp.max(meta[1:2, :]).astype(jnp.int32)
        col = jnp.max(meta[2:3, :]).astype(jnp.int32) * 16 + jnp.max(meta[3:4, :]).astype(jnp.int32)
        weight = read(0, obs)
        patch = jnp.concatenate([den_ref[row + i, pl.ds(col, PW), :] for i in range(PH)], axis=0)
        predicted = lax.dot_general(
            patch.T.astype(BF16), weight, (((1,), (1,)), ((), ())), preferred_element_type=F32
        )
        residual = predicted - read(obs, c).astype(F32)
        inn_ref[slot] = jnp.where(core == 0, residual[0:half], residual[half : 2 * half]).astype(BF16)
        weighted = (residual * meta[0:1, :]).astype(BF16)
        pulled = jnp.dot(weighted, weight, preferred_element_type=F32).T
        for i in range(PH):
            field_ref[row + i, pl.ds(col, PW), :] += pulled[i * PW : (i + 1) * PW, :]

    def observe_source(source, _):
        for cap in range(CAP):
            observe(source, cap)
        return 0

    lax.fori_loop(0, sources, observe_source, 0)

    for r in range(rows):
        field = field_ref[r]
        base_ref[r] -= guide_rate * field
        g_ref[r] = field.astype(BF16)
    write_edges(g_ref, edge_ref, gtail_ref, edge_tail_ref)
    save.wait()


def backward_kernel(
    x_ref,
    tail_ref,
    mine_ref,
    mine_tail_ref,
    other_ref,
    other_tail_ref,
    kin_ref,
    kout_ref,
    base_ref,
    slope_in_ref,
    next_ref,
    ext_ref,
    grad_ref,
    flat_ref,
    w3_ref,
    w4_ref,
    slope_ref,
    load_sems,
):
    core = lax.axis_index("ch")
    rows, width, c = x_ref.shape
    half = next_ref.shape[0]
    groups = (rows + 2) // 2

    def load(g):
        at = pl.ds(2 * g, 2)
        return pltpu.make_async_copy(slope_in_ref.at[at], slope_ref.at[at], load_sems.at[g])

    for g in range(groups):
        load(g).start()
    fill_extended(ext_ref, x_ref, tail_ref, mine_ref, mine_tail_ref, other_ref, other_tail_ref)
    place_taps(w3_ref, lambda a, b: kout_ref[2 - a, 2 - b])
    place_taps(w4_ref, lambda a, b: kin_ref[2 - a, 2 - b])

    for g in range(groups):
        load(g).wait()
        for i, y in enumerate(row_pair(ext_ref, w3_ref, 2 * g)):
            r = 2 * g + i
            grad = y * slope_ref[r]
            grad_ref[r] = jnp.where(inside(r, rows + 2), grad, 0.0).astype(BF16)

    for g in range(rows // 2):
        for i, y in enumerate(row_pair(grad_ref, w4_ref, 2 * g)):
            r = 2 * g + i
            out = base_ref[r] - guide_rate * y[0:width, :]
            for part in range(width // 128):
                plane = out[part * 128 : (part + 1) * 128, :].T
                own = jnp.where(core == 0, plane[0:half], plane[half : 2 * half])
                flat_ref[part, pl.ds(r, half, stride=rows), :] = own
    for part in range(width // 128):
        next_ref[:, :, part * 128 : (part + 1) * 128] = flat_ref[part].reshape(half, rows, 128)


def return_kernel(dest_ref, back_ref, inn_ref):
    def take(b, _):
        dest = dest_ref[b]
        rank = lax.fori_loop(0, b, lambda j, n: n + (dest_ref[j] == dest).astype(jnp.int32), 0)
        inn_ref[b] = back_ref[dest * CAP + rank]
        return 0

    lax.fori_loop(0, inn_ref.shape[0], take, 0)


def swapped(value):
    return lax.ppermute(value, "ch", [(0, 1), (1, 0)])


def from_row_neighbour(value, lon_step):
    lats, lons = lax.axis_size("lat"), lax.axis_size("lon")
    pairs = []
    for i in range(lats):
        for j in range(lons):
            for core, step in ((0, -1), (1, 1)):
                if 0 <= i + step < lats:
                    to = (i + step) * lons + (j + lon_step) % lons
                    pairs.append(((i * lons + j) * 2 + core, to * 2 + 1 - core))
    return lax.ppermute(value, ("lat", "lon", "ch"), pairs)


def from_lon_neighbour(value, lon_step):
    lons = lax.axis_size("lon")
    return lax.ppermute(value, "lon", [(j, (j + lon_step) % lons) for j in range(lons)])


def both_sides(move, value):
    if lax.axis_size("lon") == 2:
        return move(value, 1)
    from_right = move(value, -1)
    from_left = move(value, 1)
    at = lax.broadcasted_iota(jnp.int32, (1, TAIL, 1), 1)
    return jnp.where(at < TAIL // 2, from_right, from_left)


def exchanged(edge, tail, edge_tail, along):
    mine = from_row_neighbour(edge, 0)
    beside = both_sides(from_lon_neighbour, tail)
    mine_tail = both_sides(from_row_neighbour, edge_tail)
    *halo, along = lax.optimization_barrier((beside, mine, mine_tail, along))
    return tuple(halo), along


def shape(dims, dtype):
    return jax.ShapeDtypeStruct(dims, dtype)


def edge_shapes(rows, width, c):
    return [
        (shape((2, width, c), BF16), VMEM),
        (shape((rows, TAIL, c), BF16), VMEM),
        (shape((2, TAIL, c), BF16), VMEM),
    ]


def body(
    noisy_state,
    kernel_in,
    bias_in,
    kernel_out,
    interp_weight,
    observed,
    obs_precision,
    dest_tile,
    row_offset,
    col_offset,
):
    half, rows, width = noisy_state.shape
    c = kernel_in.shape[-1]
    obs = interp_weight.shape[1]
    lats = lax.axis_size("lat")
    slots = lats * CAP
    wide = width + TAIL
    other = swapped(noisy_state)
    other_obs = swapped(observed)
    w1, w2 = call(weights_kernel, [(shape((4 * c, 6 * c), BF16), VMEM)] * 2, [VMEM] * 2, [], "weights")(
        kernel_in, kernel_out
    )
    x, *edges, chunk = call(
        prep_kernel,
        [
            (shape((rows, width, c), BF16), VMEM),
            *edge_shapes(rows, width, c),
            (shape((lats, obs + c + META, obs), BF16), VMEM),
        ],
        [SMEM] * 3 + [VMEM] * 6,
        [VMEM((width // 128, c * rows, 128), F32), VMEM(obs_precision.shape, F32)],
        "prep",
    )(dest_tile, row_offset, col_offset, noisy_state, other, observed, other_obs, interp_weight, obs_precision)
    block = lax.all_to_all(chunk, "lat", split_axis=0, concat_axis=0, tiled=True)
    halo, block = exchanged(*edges, block)
    halo = halo + (swapped(halo[1]), swapped(halo[2]))
    slope, base, g, *edges, inn = call(
        forward_kernel,
        [
            (shape((rows + 2, wide, c), F32), HBM),
            (shape((rows, width, c), F32), VMEM),
            (shape((rows, width, c), BF16), VMEM),
            *edge_shapes(rows, width, c),
            (shape((slots, half, obs), BF16), VMEM),
        ],
        [VMEM] * 11,
        [
            VMEM((rows + 4, wide, c), BF16),
            VMEM((rows + 2, wide, c), BF16),
            VMEM((rows, width, c), F32),
            VMEM((rows, width, c), F32),
            VMEM((rows + 2, wide, c), F32),
            pltpu.SemaphoreType.DMA,
        ],
        "forward",
    )(x, *halo, w1, w2, bias_in.reshape(1, c), block, swapped(block))
    back = lax.all_to_all(inn, "lat", split_axis=0, concat_axis=0, tiled=True)
    halo, _ = exchanged(*edges, ())
    halo = halo + (swapped(halo[1]), swapped(halo[2]))
    (next_state,) = call(
        backward_kernel,
        [(shape((half, rows, width), F32), OUT)],
        [VMEM] * 9 + [HBM],
        [
            VMEM((rows + 4, wide, c), BF16),
            VMEM((rows + 2, wide, c), BF16),
            VMEM((width // 128, half * rows, 128), F32),
            VMEM((4 * c, 6 * c), BF16),
            VMEM((4 * c, 6 * c), BF16),
            VMEM((rows + 2, wide, c), F32),
            pltpu.SemaphoreType.DMA(((rows + 2) // 2,)),
        ],
        "backward",
    )(g, *halo, kernel_in, kernel_out, base, slope)
    (innovation,) = call(return_kernel, [(shape(observed.shape, BF16), OUT)], [SMEM, VMEM], [], "innovation")(
        dest_tile, back
    )
    return next_state, innovation


def solution(mesh):
    return jax.shard_map(
        body,
        mesh=mesh,
        in_specs=(
            P(("grp", "ch"), "lat", "lon"),
            P(),
            P(),
            P(),
            P(("grp", "lat", "lon"), None, None),
            P(("grp", "lat", "lon"), "ch", None),
            P(("grp", "lat", "lon"), None),
            P(("grp", "lat", "lon")),
            P(("grp", "lat", "lon")),
            P(("grp", "lat", "lon")),
        ),
        out_specs=(P(("grp", "ch"), "lat", "lon"), P(("grp", "lat", "lon"), "ch", None)),
        check_vma=False,
    )
```

```python
import jax
import jax.numpy as jnp
from jax import lax
from jax.experimental import pallas as pl
from jax.experimental.pallas import tpu as pltpu
from jax.sharding import PartitionSpec as P


PH = 4
PW = 32
CAP = 2
TAIL = 16
META = 16

keep_rate = 0.6
blend_rate = 0.4
guide_rate = 0.3

F32 = jnp.float32
BF16 = jnp.bfloat16
VMEM = pltpu.VMEM
SMEM = pltpu.SMEM
HBM = pltpu.MemorySpace.HBM
OUT = "out"


def call(kernel, outs, ins, scratch, aliases={}):
    near = lambda v, space: v if space == OUT else space(v.shape, v.dtype)
    spec = lambda space: pl.BlockSpec(memory_space=VMEM if space == OUT else space)
    run = pl.pallas_call(
        kernel,
        out_shape=[near(v, space) for v, space in outs],
        in_specs=[spec(space) for space in ins],
        out_specs=[spec(space) for _, space in outs],
        scratch_shapes=scratch,
        compiler_params=pltpu.CompilerParams(vmem_limit_bytes=24 * 1024 * 1024),
        input_output_aliases=aliases,
    )

    def apply(*args):
        return run(
            *(pltpu.with_memory_space_constraint(a, space) if space in (VMEM, HBM) else a for a, space in zip(args, ins))
        )

    return apply


def place_taps(w_ref, tap_of):
    c = w_ref.shape[0] // 4
    for b in range(3):
        for a in range(3):
            tap = tap_of(a, b)
            for row in range(2):
                at = (2 * b + row) * c
                w_ref[(a + row) * c : (a + row + 1) * c, at : at + c] = tap
        w_ref[3 * c : 4 * c, 2 * b * c : (2 * b + 1) * c] = jnp.zeros((c, c), BF16)
        w_ref[0:c, (2 * b + 1) * c : (2 * b + 2) * c] = jnp.zeros((c, c), BF16)


def weights_kernel(kin_ref, kout_ref, w1_ref, w2_ref):
    for w_ref, k_ref in ((w1_ref, kin_ref), (w2_ref, kout_ref)):
        place_taps(w_ref, lambda a, b: k_ref[a, b].astype(F32).T.astype(BF16))


def tail_of(row_ref, width):
    lane_rows = lax.broadcasted_iota(jnp.int32, (TAIL, row_ref.shape[-1]), 0)
    first = row_ref[0:TAIL, :].astype(F32)
    last = row_ref[width - TAIL : width, :].astype(F32)
    zero = jnp.zeros_like(first)
    return jnp.where(lane_rows < 2, first, jnp.where(lane_rows >= TAIL - 2, last, zero)).astype(BF16)


def write_edges(x_ref, edge_ref, tail_ref, edge_tail_ref):
    rows, width = x_ref.shape[0], x_ref.shape[1]
    first = lax.axis_index("ch") * (rows - 2)
    for h in range(rows):
        tail_ref[h] = tail_of(x_ref.at[h], width)
    for i in range(2):
        edge_ref[i] = x_ref[first + i]
        edge_tail_ref[i] = tail_ref[first + i]


def pack_kernel(
    dest_hbm,
    row_hbm,
    col_hbm,
    weight_hbm,
    obs_hbm,
    precision_hbm,
    noisy_hbm,
    chunk_ref,
    near_ref,
    dest_ref,
    row_ref,
    col_ref,
    weight_ref,
    obs_ref,
    precision_ref,
    scale_ref,
    sems,
):
    pairs = (
        (dest_hbm, dest_ref),
        (row_hbm, row_ref),
        (col_hbm, col_ref),
        (weight_hbm, weight_ref),
        (obs_hbm, obs_ref),
        (precision_hbm, precision_ref),
        (noisy_hbm, near_ref),
    )
    copies = [pltpu.make_async_copy(source, target, sems.at[n]) for n, (source, target) in enumerate(pairs)]
    for copy in copies:
        copy.start()
    core = lax.axis_index("ch")
    blocks, obs, _ = weight_ref.shape
    half = obs_ref.shape[1]
    first_meta = obs + CAP * half

    def clear(slot, _):
        chunk_ref[slot] = jnp.zeros(chunk_ref.shape[1:], BF16)
        return 0

    lax.fori_loop(0, chunk_ref.shape[0], clear, 0)
    for copy in copies[:-1]:
        copy.wait()
    scale_ref[...] = precision_ref[...].astype(F32)
    meta_rows = lax.broadcasted_iota(jnp.int32, (META, obs), 0)

    def pack(b, _):
        dest = dest_ref[b]
        rank = lax.fori_loop(0, b, lambda j, n: n + (dest_ref[j] == dest).astype(jnp.int32), 0)
        chunk_ref[dest, pl.ds(pl.multiple_of(obs + rank * half, 16), half), :] = obs_ref[b]

        @pl.when(rank == core)
        def _():
            chunk_ref[dest, 0:obs, :] = weight_ref[b]
            row = row_ref[b].astype(F32)
            high = lax.div(col_ref[b], 16).astype(F32)
            low = lax.rem(col_ref[b], 16).astype(F32)
            meta = jnp.where(
                meta_rows == 0,
                jnp.broadcast_to(scale_ref[pl.ds(b, 1), :], (META, obs)),
                jnp.where(meta_rows == 1, row, jnp.where(meta_rows == 2, high, low)),
            )
            chunk_ref[dest, first_meta : first_meta + META, :] = meta.astype(BF16)

        return 0

    lax.fori_loop(0, blocks, pack, 0)
    copies[-1].wait()


def prep_kernel(own_ref, other_ref, x_ref, edge_ref, tail_ref, edge_tail_ref, flat_ref):
    core = lax.axis_index("ch")
    half, rows, width = own_ref.shape

    def place(ref, first):
        for part in range(width // 128):
            piece = ref[:, :, part * 128 : (part + 1) * 128].astype(F32)
            flat_ref[part, pl.ds(pl.multiple_of(first * rows, 8), half * rows), :] = piece.reshape(half * rows, 128)

    place(own_ref, core * half)
    place(other_ref, (1 - core) * half)
    for h in range(rows):
        for part in range(width // 128):
            plane = flat_ref[part, pl.ds(h, 2 * half, stride=rows), :]
            x_ref[h, part * 128 : (part + 1) * 128, :] = plane.T.astype(BF16)
    write_edges(x_ref, edge_ref, tail_ref, edge_tail_ref)


def fill_extended(ext_ref, x_ref, tail_ref, mine_ref, mine_tail_ref, other_ref, other_tail_ref):
    rows, width = x_ref.shape[0], x_ref.shape[1]
    core = lax.axis_index("ch")
    for i in range(2):
        mine = core * (rows + 2) + i
        other = (1 - core) * (rows + 2) + i
        ext_ref[mine, 0:width, :] = mine_ref[i]
        ext_ref[mine, width : width + TAIL, :] = mine_tail_ref[i]
        ext_ref[other, 0:width, :] = other_ref[i]
        ext_ref[other, width : width + TAIL, :] = other_tail_ref[i]
    for h in range(rows):
        ext_ref[h + 2, 0:width, :] = x_ref[h]
        ext_ref[h + 2, width : width + TAIL, :] = tail_ref[h]


def row_pair(src_ref, w_ref, first):
    c = src_ref.shape[-1]
    wide = src_ref.shape[1]
    lhs = jnp.concatenate([src_ref[first + k] for k in range(4)], axis=1)
    y = jnp.dot(lhs, w_ref[...], preferred_element_type=F32)
    out = []
    for row in range(2):
        left, mid, right = (y[:, (2 * b + row) * c : (2 * b + row + 1) * c] for b in range(3))
        out.append(pltpu.roll(left, 1, 0) + mid + pltpu.roll(right, wide - 1, 0))
    return out


def inside(ext_row, ext_rows):
    at = lax.axis_index("lat")
    last = lax.axis_size("lat") - 1
    return ((ext_row > 0) | (at > 0)) & ((ext_row < ext_rows - 1) | (at < last))


def own_pair(first, second):
    core = lax.axis_index("ch")
    half = first.shape[-1] // 2
    lane = lax.broadcasted_iota(jnp.int32, first.shape, len(first.shape) - 1)
    stays = jnp.where(core == 0, first, second)
    moves = pltpu.roll(jnp.where(core == 0, second, first), half, len(first.shape) - 1)
    low = (lane < half).astype(jnp.int32)
    return jnp.where(low == 1 - core, stays, moves)


def forward_kernel(
    x_ref,
    tail_ref,
    mine_ref,
    mine_tail_ref,
    other_ref,
    other_tail_ref,
    w1_ref,
    w2_ref,
    bias_ref,
    block_ref,
    other_block_ref,
    slope_ref,
    base_ref,
    g_ref,
    edge_ref,
    gtail_ref,
    edge_tail_ref,
    inn_ref,
    ext_ref,
    hidden_ref,
    den_ref,
    field_ref,
    turned_ref,
    value_ref,
    scale_ref,
    code_ref,
):
    core = lax.axis_index("ch")
    rows, width, c = x_ref.shape
    half = inn_ref.shape[1]
    sources, obs = block_ref.shape[0], block_ref.shape[2]
    fill_extended(ext_ref, x_ref, tail_ref, mine_ref, mine_tail_ref, other_ref, other_tail_ref)

    def read(source, cap, first, count):
        at = slice(first, first + count)
        return jnp.where(core == cap, block_ref[source, at, :], other_block_ref[source, at, :])

    def locate(source, cap):
        meta = read(source, cap, obs + c, META).astype(F32)
        code = meta[1:2, :] * 65536.0 + meta[2:3, :] * 16.0 + meta[3:4, :]
        code_ref[source * CAP + cap] = jnp.max(code).astype(jnp.int32)

    def turn(source, cap):
        slot = source * CAP + cap
        turned_ref[slot] = read(source, cap, 0, obs).T
        at = slice(obs + cap * half, obs + (cap + 1) * half)
        mine, theirs = block_ref[source, at, :], other_block_ref[source, at, :]
        low, high = jnp.where(core == 0, mine, theirs), jnp.where(core == 0, theirs, mine)
        value_ref[slot] = jnp.concatenate([low, high], axis=0).T
        row = read(source, cap, obs + c, META).astype(F32)[0:1, :]
        scale_ref[slot] = jnp.broadcast_to(row, (c, obs)).T

    def each(task, first, last):
        if last - first <= 8:
            for source in range(first, last):
                for cap in range(CAP):
                    task(source, cap)
            return

        def step(source, _):
            for cap in range(CAP):
                task(source, cap)
            return 0

        lax.fori_loop(first, last, step, 0)

    each(locate, 0, sources)
    bias = bias_ref[...]
    for g in range((rows + 2) // 2):
        for i, y in enumerate(row_pair(ext_ref, w1_ref, 2 * g)):
            r = 2 * g + i
            pre = y + bias
            s = 1.0 / (1.0 + jnp.exp(-pre))
            slope_ref[r] = s * (1.0 + pre * (1.0 - s))
            hidden_ref[r] = jnp.where(inside(r, rows + 2), pre * s, 0.0).astype(BF16)
    groups = rows // 2
    for g in range(groups):
        each(turn, sources * g // groups, sources * (g + 1) // groups)
        for i, y in enumerate(row_pair(hidden_ref, w2_ref, 2 * g)):
            r = 2 * g + i
            noisy = x_ref[r].astype(F32)
            den_ref[r] = (noisy + y[0:width, :]).astype(BF16).astype(F32)
            field_ref[r] = jnp.zeros((width, c), F32)

    def observe(source, cap):
        slot = source * CAP + cap
        code = code_ref[slot]
        row = lax.shift_right_logical(code, 16)
        col = lax.bitwise_and(code, 65535)
        patch = jnp.concatenate([den_ref[row + i, pl.ds(col, PW), :] for i in range(PH)], axis=0).astype(BF16)
        predicted = jnp.dot(read(source, cap, 0, obs), patch, preferred_element_type=F32)
        residual = predicted - value_ref[slot].astype(F32)
        weighted = (residual * scale_ref[slot]).astype(BF16)
        pulled = jnp.dot(turned_ref[slot], weighted, preferred_element_type=F32)
        for i in range(PH):
            field_ref[row + i, pl.ds(col, PW), :] += pulled[i * PW : (i + 1) * PW, :]
        turned = residual.astype(BF16).T
        inn_ref[slot] = jnp.where(core == 0, turned[0:half], turned[half : 2 * half])

    each(observe, 0, sources)

    for g in range(groups):
        base = []
        for r in (2 * g, 2 * g + 1):
            field = field_ref[r]
            noisy = ext_ref[r + 2, 0:width, :].astype(F32)
            base.append(keep_rate * noisy + blend_rate * den_ref[r] - guide_rate * field)
            g_ref[r] = field.astype(BF16)
        base_ref[g] = own_pair(*base)
    write_edges(g_ref, edge_ref, gtail_ref, edge_tail_ref)


def backward_kernel(
    x_ref,
    tail_ref,
    mine_ref,
    mine_tail_ref,
    other_ref,
    other_tail_ref,
    kin_ref,
    kout_ref,
    base_ref,
    slope_ref,
    next_ref,
    ext_ref,
    grad_ref,
    flat_ref,
    w3_ref,
    w4_ref,
):
    rows, width, c = x_ref.shape
    wide = ext_ref.shape[1]
    half = next_ref.shape[0]
    fill_extended(ext_ref, x_ref, tail_ref, mine_ref, mine_tail_ref, other_ref, other_tail_ref)
    place_taps(w3_ref, lambda a, b: kout_ref[2 - a, 2 - b])
    zero = jnp.zeros((c, c), F32)
    for b in range(3):
        taps = [zero] + [kin_ref[2 - a, 2 - b].astype(F32) for a in range(3)] + [zero]
        for k in range(4):
            w4_ref[k * c : (k + 1) * c, b * c : (b + 1) * c] = own_pair(taps[k + 1], taps[k]).astype(BF16)

    for g in range((rows + 2) // 2):
        for i, y in enumerate(row_pair(ext_ref, w3_ref, 2 * g)):
            r = 2 * g + i
            grad_ref[r] = jnp.where(inside(r, rows + 2), y * slope_ref[r], 0.0).astype(BF16)

    for g in range(rows // 2):
        lhs = jnp.concatenate([grad_ref[2 * g + k] for k in range(4)], axis=1)
        y = jnp.dot(lhs, w4_ref[...], preferred_element_type=F32)
        y = pltpu.roll(y[:, 0:c], 1, 0) + y[:, c : 2 * c] + pltpu.roll(y[:, 2 * c : 3 * c], wide - 1, 0)
        out = base_ref[g] - guide_rate * y[0:width, :]
        for part in range(width // 128):
            plane = out[part * 128 : (part + 1) * 128, :].T
            for i in range(2):
                flat_ref[part, pl.ds(2 * g + i, half, stride=rows), :] = plane[i * half : (i + 1) * half]
    for part in range(width // 128):
        next_ref[:, :, part * 128 : (part + 1) * 128] = flat_ref[part].reshape(half, rows, 128)


def return_kernel(dest_ref, back_ref, inn_ref):
    def take(b, _):
        dest = dest_ref[b]
        rank = lax.fori_loop(0, b, lambda j, n: n + (dest_ref[j] == dest).astype(jnp.int32), 0)
        inn_ref[b] = back_ref[dest * CAP + rank]
        return 0

    lax.fori_loop(0, inn_ref.shape[0], take, 0)


def swapped(value):
    return lax.ppermute(value, "ch", [(0, 1), (1, 0)])


def from_row_neighbour(value, lon_step):
    lats, lons = lax.axis_size("lat"), lax.axis_size("lon")
    pairs = []
    for i in range(lats):
        for j in range(lons):
            for core, step in ((0, -1), (1, 1)):
                if 0 <= i + step < lats:
                    to = (i + step) * lons + (j + lon_step) % lons
                    pairs.append(((i * lons + j) * 2 + core, to * 2 + 1 - core))
    return lax.ppermute(value, ("lat", "lon", "ch"), pairs)


def from_lon_neighbour(value, lon_step):
    lons = lax.axis_size("lon")
    return lax.ppermute(value, "lon", [(j, (j + lon_step) % lons) for j in range(lons)])


def both_sides(move, value):
    if lax.axis_size("lon") == 2:
        return move(value, 1)
    from_right = move(value, -1)
    from_left = move(value, 1)
    at = lax.broadcasted_iota(jnp.int32, (1, TAIL, 1), 1)
    return jnp.where(at < TAIL // 2, from_right, from_left)


def exchanged(edge, tail, edge_tail, along):
    mine_tail = both_sides(from_row_neighbour, edge_tail)
    mine = from_row_neighbour(edge, 0)
    beside = both_sides(from_lon_neighbour, tail)
    *halo, along = lax.optimization_barrier((beside, mine, mine_tail, along))
    halo = tuple(halo) + (swapped(halo[1]), swapped(halo[2]))
    return halo, along


def shape(dims, dtype):
    return jax.ShapeDtypeStruct(dims, dtype)


def edge_shapes(rows, width, c):
    return [
        (shape((2, width, c), BF16), VMEM),
        (shape((rows, TAIL, c), BF16), VMEM),
        (shape((2, TAIL, c), BF16), VMEM),
    ]


def body(
    noisy_state,
    kernel_in,
    bias_in,
    kernel_out,
    interp_weight,
    observed,
    obs_precision,
    dest_tile,
    row_offset,
    col_offset,
):
    half, rows, width = noisy_state.shape
    c = kernel_in.shape[-1]
    blocks, obs, _ = interp_weight.shape
    lats = lax.axis_size("lat")
    slots = lats * CAP
    wide = width + TAIL
    other = swapped(noisy_state)
    chunk_shape = shape((lats, obs + CAP * half + META, obs), BF16)
    chunk, near = call(
        pack_kernel,
        [(chunk_shape, VMEM), (shape(noisy_state.shape, BF16), VMEM)],
        [HBM] * 7,
        [
            SMEM((blocks,), jnp.int32),
            SMEM((blocks,), jnp.int32),
            SMEM((blocks,), jnp.int32),
            VMEM(interp_weight.shape, BF16),
            VMEM(observed.shape, BF16),
            VMEM(obs_precision.shape, BF16),
            VMEM(obs_precision.shape, F32),
            pltpu.SemaphoreType.DMA((7,)),
        ],
    )(dest_tile, row_offset, col_offset, interp_weight, observed, obs_precision, noisy_state)
    block = lax.all_to_all(chunk, "lat", split_axis=0, concat_axis=0, tiled=True)
    x, *edges = call(
        prep_kernel,
        [(shape((rows, width, c), BF16), VMEM), *edge_shapes(rows, width, c)],
        [VMEM] * 2,
        [VMEM((width // 128, c * rows, 128), F32)],
    )(near, other)
    w1, w2 = call(weights_kernel, [(shape((4 * c, 6 * c), BF16), VMEM)] * 2, [VMEM] * 2, [])(kernel_in, kernel_out)
    halo, block = exchanged(*edges, block)
    slope, base, g, *edges, inn = call(
        forward_kernel,
        [
            (shape((rows + 2, wide, c), F32), VMEM),
            (shape((rows // 2, width, c), F32), VMEM),
            (shape((rows, width, c), BF16), VMEM),
            *edge_shapes(rows, width, c),
            (shape((slots, half, obs), BF16), VMEM),
        ],
        [VMEM] * 11,
        [
            VMEM((rows + 4, wide, c), BF16),
            VMEM((rows + 2, wide, c), BF16),
            VMEM((rows, width, c), F32),
            VMEM((rows, width, c), F32),
            VMEM((slots, obs, obs), BF16),
            VMEM((slots, obs, c), BF16),
            VMEM((slots, obs, c), F32),
            SMEM((slots,), jnp.int32),
        ],
        {0: 2, 2: 3, 1: 4, 3: 5},
    )(x, *halo, w1, w2, bias_in.reshape(1, c), block, swapped(block))
    halo, _ = exchanged(*edges, ())
    back = lax.all_to_all(inn, "lat", split_axis=0, concat_axis=0, tiled=True)
    (next_state,) = call(
        backward_kernel,
        [(shape((half, rows, width), F32), OUT)],
        [VMEM] * 10,
        [
            VMEM((rows + 4, wide, c), BF16),
            VMEM((rows + 2, wide, c), BF16),
            VMEM((width // 128, half * rows, 128), F32),
            VMEM((4 * c, 6 * c), BF16),
            VMEM((4 * c, 3 * c), BF16),
        ],
    )(g, *halo, kernel_in, kernel_out, base, slope)
    (innovation,) = call(return_kernel, [(shape(observed.shape, BF16), OUT)], [SMEM, VMEM], [])(dest_tile, back)
    return next_state, innovation


def solution(mesh):
    return jax.shard_map(
        body,
        mesh=mesh,
        in_specs=(
            P(("grp", "ch"), "lat", "lon"),
            P(),
            P(),
            P(),
            P(("grp", "lat", "lon"), None, None),
            P(("grp", "lat", "lon"), "ch", None),
            P(("grp", "lat", "lon"), None),
            P(("grp", "lat", "lon")),
            P(("grp", "lat", "lon")),
            P(("grp", "lat", "lon")),
        ),
        out_specs=(P(("grp", "ch"), "lat", "lon"), P(("grp", "lat", "lon"), "ch", None)),
        check_vma=False,
    )
```

```python
import jax
import jax.numpy as jnp
from jax import lax
from jax.experimental import pallas as pl
from jax.experimental.pallas import tpu as pltpu
from jax.sharding import PartitionSpec as P


PH = 4
PW = 32
CAP = 2
TAIL = 16
META = 16

keep_rate = 0.6
blend_rate = 0.4
guide_rate = 0.3

F32 = jnp.float32
BF16 = jnp.bfloat16
VMEM = pltpu.VMEM
SMEM = pltpu.SMEM
HBM = pltpu.MemorySpace.HBM
OUT = "out"


def call(kernel, outs, ins, scratch, aliases={}):
    near = lambda v, space: v if space == OUT else space(v.shape, v.dtype)
    spec = lambda space: pl.BlockSpec(memory_space=VMEM if space == OUT else space)
    run = pl.pallas_call(
        kernel,
        out_shape=[near(v, space) for v, space in outs],
        in_specs=[spec(space) for space in ins],
        out_specs=[spec(space) for _, space in outs],
        scratch_shapes=scratch,
        compiler_params=pltpu.CompilerParams(vmem_limit_bytes=24 * 1024 * 1024),
        input_output_aliases=aliases,
    )

    def apply(*args):
        return run(
            *(pltpu.with_memory_space_constraint(a, space) if space in (VMEM, HBM) else a for a, space in zip(args, ins))
        )

    return apply


def place_taps(w_ref, tap_of):
    c = w_ref.shape[0] // 4
    for b in range(3):
        for a in range(3):
            tap = tap_of(a, b)
            for row in range(2):
                at = (2 * b + row) * c
                w_ref[(a + row) * c : (a + row + 1) * c, at : at + c] = tap
        w_ref[3 * c : 4 * c, 2 * b * c : (2 * b + 1) * c] = jnp.zeros((c, c), BF16)
        w_ref[0:c, (2 * b + 1) * c : (2 * b + 2) * c] = jnp.zeros((c, c), BF16)


def weights_kernel(kin_ref, kout_ref, w1_ref, w2_ref):
    for w_ref, k_ref in ((w1_ref, kin_ref), (w2_ref, kout_ref)):
        place_taps(w_ref, lambda a, b: k_ref[a, b].astype(F32).T.astype(BF16))


def tail_of(row_ref, width):
    lane_rows = lax.broadcasted_iota(jnp.int32, (TAIL, row_ref.shape[-1]), 0)
    first = row_ref[0:TAIL, :].astype(F32)
    last = row_ref[width - TAIL : width, :].astype(F32)
    zero = jnp.zeros_like(first)
    return jnp.where(lane_rows < 2, first, jnp.where(lane_rows >= TAIL - 2, last, zero)).astype(BF16)


def write_tails(x_ref, tail_ref):
    for h in range(x_ref.shape[0]):
        tail_ref[h] = tail_of(x_ref.at[h], x_ref.shape[1])


def edge_kernel(x_ref, tail_ref, edge_ref):
    rows, width, _ = x_ref.shape
    first = lax.axis_index("ch") * (rows - 2)
    for i in range(2):
        edge_ref[i, 0:width, :] = x_ref[first + i]
        edge_ref[i, width : width + TAIL, :] = tail_ref[first + i]


def pack_kernel(
    dest_hbm,
    row_hbm,
    col_hbm,
    weight_hbm,
    obs_hbm,
    precision_hbm,
    noisy_hbm,
    chunk_ref,
    near_ref,
    dest_ref,
    row_ref,
    col_ref,
    weight_ref,
    obs_ref,
    precision_ref,
    scale_ref,
    sems,
):
    pairs = (
        (dest_hbm, dest_ref),
        (row_hbm, row_ref),
        (col_hbm, col_ref),
        (weight_hbm, weight_ref),
        (obs_hbm, obs_ref),
        (precision_hbm, precision_ref),
        (noisy_hbm, near_ref),
    )
    copies = [pltpu.make_async_copy(source, target, sems.at[n]) for n, (source, target) in enumerate(pairs)]
    for copy in copies:
        copy.start()
    core = lax.axis_index("ch")
    blocks, obs, _ = weight_ref.shape
    half = obs_ref.shape[1]
    first_meta = obs + CAP * half

    def clear(slot, _):
        chunk_ref[slot] = jnp.zeros(chunk_ref.shape[1:], BF16)
        return 0

    lax.fori_loop(0, chunk_ref.shape[0], clear, 0)
    for copy in copies[:-1]:
        copy.wait()
    scale_ref[...] = precision_ref[...].astype(F32)
    meta_rows = lax.broadcasted_iota(jnp.int32, (META, obs), 0)

    def pack(b, _):
        dest = dest_ref[b]
        rank = lax.fori_loop(0, b, lambda j, n: n + (dest_ref[j] == dest).astype(jnp.int32), 0)
        chunk_ref[dest, pl.ds(pl.multiple_of(obs + rank * half, 16), half), :] = obs_ref[b]

        @pl.when(rank == core)
        def _():
            chunk_ref[dest, 0:obs, :] = weight_ref[b]
            row = row_ref[b].astype(F32)
            high = lax.div(col_ref[b], 16).astype(F32)
            low = lax.rem(col_ref[b], 16).astype(F32)
            meta = jnp.where(
                meta_rows == 0,
                jnp.broadcast_to(scale_ref[pl.ds(b, 1), :], (META, obs)),
                jnp.where(meta_rows == 1, row, jnp.where(meta_rows == 2, high, low)),
            )
            chunk_ref[dest, first_meta : first_meta + META, :] = meta.astype(BF16)

        return 0

    lax.fori_loop(0, blocks, pack, 0)
    copies[-1].wait()


def prep_kernel(own_ref, other_ref, x_ref, tail_ref, flat_ref):
    core = lax.axis_index("ch")
    half, rows, width = own_ref.shape

    def place(ref, first):
        for part in range(width // 128):
            piece = ref[:, :, part * 128 : (part + 1) * 128].astype(F32)
            flat_ref[part, pl.ds(pl.multiple_of(first * rows, 8), half * rows), :] = piece.reshape(half * rows, 128)

    place(own_ref, core * half)
    place(other_ref, (1 - core) * half)
    for h in range(rows):
        for part in range(width // 128):
            plane = flat_ref[part, pl.ds(h, 2 * half, stride=rows), :]
            x_ref[h, part * 128 : (part + 1) * 128, :] = plane.T.astype(BF16)
    write_tails(x_ref, tail_ref)


def fill_extended(ext_ref, x_ref, tail_ref, mine_ref, other_ref):
    rows, width = x_ref.shape[0], x_ref.shape[1]
    core = lax.axis_index("ch")
    for i in range(2):
        ext_ref[core * (rows + 2) + i] = mine_ref[i]
        ext_ref[(1 - core) * (rows + 2) + i] = other_ref[i]
    for h in range(rows):
        ext_ref[h + 2, 0:width, :] = x_ref[h]
        ext_ref[h + 2, width : width + TAIL, :] = tail_ref[h]


def row_pair(src_ref, w_ref, first):
    c = src_ref.shape[-1]
    wide = src_ref.shape[1]
    lhs = jnp.concatenate([src_ref[first + k] for k in range(4)], axis=1)
    y = jnp.dot(lhs, w_ref[...], preferred_element_type=F32)
    out = []
    for row in range(2):
        left, mid, right = (y[:, (2 * b + row) * c : (2 * b + row + 1) * c] for b in range(3))
        out.append(pltpu.roll(left, 1, 0) + mid + pltpu.roll(right, wide - 1, 0))
    return out


def inside(ext_row, ext_rows):
    at = lax.axis_index("lat")
    last = lax.axis_size("lat") - 1
    return ((ext_row > 0) | (at > 0)) & ((ext_row < ext_rows - 1) | (at < last))


def own_pair(first, second):
    core = lax.axis_index("ch")
    half = first.shape[-1] // 2
    lane = lax.broadcasted_iota(jnp.int32, first.shape, len(first.shape) - 1)
    stays = jnp.where(core == 0, first, second)
    moves = pltpu.roll(jnp.where(core == 0, second, first), half, len(first.shape) - 1)
    low = (lane < half).astype(jnp.int32)
    return jnp.where(low == 1 - core, stays, moves)


def forward_kernel(
    x_ref,
    tail_ref,
    mine_ref,
    other_ref,
    w1_ref,
    w2_ref,
    bias_ref,
    block_ref,
    other_block_ref,
    slope_ref,
    base_ref,
    g_ref,
    gtail_ref,
    inn_ref,
    ext_ref,
    hidden_ref,
    den_ref,
    field_ref,
    turned_ref,
    value_ref,
    scale_ref,
    code_ref,
):
    core = lax.axis_index("ch")
    rows, width, c = x_ref.shape
    half = inn_ref.shape[1]
    sources, obs = block_ref.shape[0], block_ref.shape[2]
    fill_extended(ext_ref, x_ref, tail_ref, mine_ref, other_ref)

    def read(source, cap, first, count):
        at = slice(first, first + count)
        return jnp.where(core == cap, block_ref[source, at, :], other_block_ref[source, at, :])

    def locate(source, cap):
        meta = read(source, cap, obs + c, META).astype(F32)
        code = meta[1:2, :] * 65536.0 + meta[2:3, :] * 16.0 + meta[3:4, :]
        code_ref[source * CAP + cap] = jnp.max(code).astype(jnp.int32)

    def turn(source, cap):
        slot = source * CAP + cap
        turned_ref[slot] = read(source, cap, 0, obs).T
        at = slice(obs + cap * half, obs + (cap + 1) * half)
        mine, theirs = block_ref[source, at, :], other_block_ref[source, at, :]
        low, high = jnp.where(core == 0, mine, theirs), jnp.where(core == 0, theirs, mine)
        value_ref[slot] = jnp.concatenate([low, high], axis=0).T
        row = read(source, cap, obs + c, META).astype(F32)[0:1, :]
        scale_ref[slot] = jnp.broadcast_to(row, (c, obs)).T

    def each(task, first, last):
        if last - first <= 8:
            for source in range(first, last):
                for cap in range(CAP):
                    task(source, cap)
            return

        def step(source, _):
            for cap in range(CAP):
                task(source, cap)
            return 0

        lax.fori_loop(first, last, step, 0)

    each(locate, 0, sources)
    bias = bias_ref[...]
    for g in range((rows + 2) // 2):
        for i, y in enumerate(row_pair(ext_ref, w1_ref, 2 * g)):
            r = 2 * g + i
            pre = y + bias
            s = 1.0 / (1.0 + jnp.exp(-pre))
            slope_ref[r] = s * (1.0 + pre * (1.0 - s))
            hidden_ref[r] = jnp.where(inside(r, rows + 2), pre * s, 0.0).astype(BF16)
    groups = rows // 2
    for g in range(groups):
        each(turn, sources * g // groups, sources * (g + 1) // groups)
        for i, y in enumerate(row_pair(hidden_ref, w2_ref, 2 * g)):
            r = 2 * g + i
            noisy = x_ref[r].astype(F32)
            den_ref[r] = (noisy + y[0:width, :]).astype(BF16).astype(F32)
            field_ref[r] = jnp.zeros((width, c), F32)

    def observe(source, cap):
        slot = source * CAP + cap
        code = code_ref[slot]
        row = lax.shift_right_logical(code, 16)
        col = lax.bitwise_and(code, 65535)
        patch = jnp.concatenate([den_ref[row + i, pl.ds(col, PW), :] for i in range(PH)], axis=0).astype(BF16)
        predicted = jnp.dot(read(source, cap, 0, obs), patch, preferred_element_type=F32)
        residual = predicted - value_ref[slot].astype(F32)
        weighted = (residual * scale_ref[slot]).astype(BF16)
        pulled = jnp.dot(turned_ref[slot], weighted, preferred_element_type=F32)
        for i in range(PH):
            field_ref[row + i, pl.ds(col, PW), :] += pulled[i * PW : (i + 1) * PW, :]
        turned = residual.astype(BF16).T
        inn_ref[slot] = jnp.where(core == 0, turned[0:half], turned[half : 2 * half])

    each(observe, 0, sources)

    for g in range(groups):
        base = []
        for r in (2 * g, 2 * g + 1):
            field = field_ref[r]
            noisy = ext_ref[r + 2, 0:width, :].astype(F32)
            base.append(keep_rate * noisy + blend_rate * den_ref[r] - guide_rate * field)
            g_ref[r] = field.astype(BF16)
        base_ref[g] = own_pair(*base)
    write_tails(g_ref, gtail_ref)


def backward_kernel(
    x_ref,
    tail_ref,
    mine_ref,
    other_ref,
    kin_ref,
    kout_ref,
    base_ref,
    slope_ref,
    back_ref,
    dest_hbm,
    next_ref,
    inn_hbm,
    ext_ref,
    grad_ref,
    flat_ref,
    w3_ref,
    w4_ref,
    dest_ref,
    dest_sem,
    inn_sems,
):
    dest_copy = pltpu.make_async_copy(dest_hbm, dest_ref, dest_sem)
    dest_copy.start()
    rows, width, c = x_ref.shape
    wide = ext_ref.shape[1]
    half = next_ref.shape[0]
    fill_extended(ext_ref, x_ref, tail_ref, mine_ref, other_ref)
    place_taps(w3_ref, lambda a, b: kout_ref[2 - a, 2 - b])
    zero = jnp.zeros((c, c), F32)
    for b in range(3):
        taps = [zero] + [kin_ref[2 - a, 2 - b].astype(F32) for a in range(3)] + [zero]
        for k in range(4):
            w4_ref[k * c : (k + 1) * c, b * c : (b + 1) * c] = own_pair(taps[k + 1], taps[k]).astype(BF16)

    for g in range((rows + 2) // 2):
        for i, y in enumerate(row_pair(ext_ref, w3_ref, 2 * g)):
            r = 2 * g + i
            grad_ref[r] = jnp.where(inside(r, rows + 2), y * slope_ref[r], 0.0).astype(BF16)

    dest_copy.wait()

    def give(b):
        dest = dest_ref[b]
        rank = lax.fori_loop(0, b, lambda j, n: n + (dest_ref[j] == dest).astype(jnp.int32), 0)
        return pltpu.make_async_copy(back_ref.at[dest * CAP + rank], inn_hbm.at[b], inn_sems.at[b])

    def start(b, _):
        give(b).start()
        return 0

    def finish(b, _):
        pltpu.make_async_copy(back_ref.at[0], inn_hbm.at[b], inn_sems.at[b]).wait()
        return 0

    lax.fori_loop(0, inn_hbm.shape[0], start, 0)
    for g in range(rows // 2):
        lhs = jnp.concatenate([grad_ref[2 * g + k] for k in range(4)], axis=1)
        y = jnp.dot(lhs, w4_ref[...], preferred_element_type=F32)
        y = pltpu.roll(y[:, 0:c], 1, 0) + y[:, c : 2 * c] + pltpu.roll(y[:, 2 * c : 3 * c], wide - 1, 0)
        out = base_ref[g] - guide_rate * y[0:width, :]
        for part in range(width // 128):
            plane = out[part * 128 : (part + 1) * 128, :].T
            for i in range(2):
                flat_ref[part, pl.ds(2 * g + i, half, stride=rows), :] = plane[i * half : (i + 1) * half]
    for part in range(width // 128):
        next_ref[:, :, part * 128 : (part + 1) * 128] = flat_ref[part].reshape(half, rows, 128)
    lax.fori_loop(0, inn_hbm.shape[0], finish, 0)


def swapped(value):
    return lax.ppermute(value, "ch", [(0, 1), (1, 0)])


def from_row_neighbour(value):
    lats = lax.axis_size("lat")
    steps = ((0, -1), (1, 1))
    pairs = [
        (i * 2 + core, (i + step) * 2 + 1 - core) for i in range(lats) for core, step in steps if 0 <= i + step < lats
    ]
    return lax.ppermute(value, ("lat", "ch"), pairs)


def from_lon_neighbours(value):
    lons = lax.axis_size("lon")
    move = lambda step: lax.ppermute(value, "lon", [(j, (j + step) % lons) for j in range(lons)])
    if lons == 2:
        return move(1)
    at = lax.broadcasted_iota(jnp.int32, (1, TAIL, 1), 1)
    return jnp.where(at < TAIL // 2, move(-1), move(1))


def exchanged(x, tail, along):
    _, width, c = x.shape
    beside = from_lon_neighbours(tail)
    (edge,) = call(edge_kernel, [(shape((2, width + TAIL, c), BF16), VMEM)], [VMEM] * 2, [])(x, beside)
    mine = from_row_neighbour(edge)
    mine, along = lax.optimization_barrier((mine, along))
    return (beside, mine, swapped(mine)), along


def shape(dims, dtype):
    return jax.ShapeDtypeStruct(dims, dtype)


def body(
    noisy_state,
    kernel_in,
    bias_in,
    kernel_out,
    interp_weight,
    observed,
    obs_precision,
    dest_tile,
    row_offset,
    col_offset,
):
    half, rows, width = noisy_state.shape
    c = kernel_in.shape[-1]
    blocks, obs, _ = interp_weight.shape
    lats = lax.axis_size("lat")
    slots = lats * CAP
    wide = width + TAIL
    other = swapped(noisy_state)
    chunk_shape = shape((lats, obs + CAP * half + META, obs), BF16)
    chunk, near = call(
        pack_kernel,
        [(chunk_shape, VMEM), (shape(noisy_state.shape, BF16), VMEM)],
        [HBM] * 7,
        [
            SMEM((blocks,), jnp.int32),
            SMEM((blocks,), jnp.int32),
            SMEM((blocks,), jnp.int32),
            VMEM(interp_weight.shape, BF16),
            VMEM(observed.shape, BF16),
            VMEM(obs_precision.shape, BF16),
            VMEM(obs_precision.shape, F32),
            pltpu.SemaphoreType.DMA((7,)),
        ],
    )(dest_tile, row_offset, col_offset, interp_weight, observed, obs_precision, noisy_state)
    block = lax.all_to_all(chunk, "lat", split_axis=0, concat_axis=0, tiled=True)
    tail_shape = shape((rows, TAIL, c), BF16)
    x, tail = call(
        prep_kernel,
        [(shape((rows, width, c), BF16), VMEM), (tail_shape, VMEM)],
        [VMEM] * 2,
        [VMEM((width // 128, c * rows, 128), F32)],
    )(near, other)
    w1, w2 = call(weights_kernel, [(shape((4 * c, 6 * c), BF16), VMEM)] * 2, [VMEM] * 2, [])(kernel_in, kernel_out)
    halo, block = exchanged(x, tail, block)
    slope, base, g, tail, inn = call(
        forward_kernel,
        [
            (shape((rows + 2, wide, c), F32), VMEM),
            (shape((rows // 2, width, c), F32), VMEM),
            (shape((rows, width, c), BF16), VMEM),
            (tail_shape, VMEM),
            (shape((slots, half, obs), BF16), VMEM),
        ],
        [VMEM] * 9,
        [
            VMEM((rows + 4, wide, c), BF16),
            VMEM((rows + 2, wide, c), BF16),
            VMEM((rows, width, c), F32),
            VMEM((rows, width, c), F32),
            VMEM((slots, obs, obs), BF16),
            VMEM((slots, obs, c), BF16),
            VMEM((slots, obs, c), F32),
            SMEM((slots,), jnp.int32),
        ],
        {0: 2, 1: 3},
    )(x, *halo, w1, w2, bias_in.reshape(1, c), block, swapped(block))
    halo, _ = exchanged(g, tail, ())
    back = lax.all_to_all(inn, "lat", split_axis=0, concat_axis=0, tiled=True)
    next_state, innovation = call(
        backward_kernel,
        [(shape((half, rows, width), F32), OUT), (shape(observed.shape, BF16), HBM)],
        [VMEM] * 9 + [HBM],
        [
            VMEM((rows + 4, wide, c), BF16),
            VMEM((rows + 2, wide, c), BF16),
            VMEM((width // 128, half * rows, 128), F32),
            VMEM((4 * c, 6 * c), BF16),
            VMEM((4 * c, 3 * c), BF16),
            SMEM((blocks,), jnp.int32),
            pltpu.SemaphoreType.DMA,
            pltpu.SemaphoreType.DMA((blocks,)),
        ],
    )(g, *halo, kernel_in, kernel_out, base, slope, back, dest_tile)
    return next_state, innovation


def solution(mesh):
    return jax.shard_map(
        body,
        mesh=mesh,
        in_specs=(
            P(("grp", "ch"), "lat", "lon"),
            P(),
            P(),
            P(),
            P(("grp", "lat", "lon"), None, None),
            P(("grp", "lat", "lon"), "ch", None),
            P(("grp", "lat", "lon"), None),
            P(("grp", "lat", "lon")),
            P(("grp", "lat", "lon")),
            P(("grp", "lat", "lon")),
        ),
        out_specs=(P(("grp", "ch"), "lat", "lon"), P(("grp", "lat", "lon"), "ch", None)),
        check_vma=False,
    )
```

```python
import jax
import jax.numpy as jnp
from jax import lax
from jax.experimental import pallas as pl
from jax.experimental.pallas import tpu as pltpu
from jax.sharding import PartitionSpec as P


PH = 4
PW = 32
CAP = 2
TAIL = 16
META = 16

keep_rate = 0.6
blend_rate = 0.4
guide_rate = 0.3

F32 = jnp.float32
BF16 = jnp.bfloat16
VMEM = pltpu.VMEM
SMEM = pltpu.SMEM
HBM = pltpu.MemorySpace.HBM
OUT = "out"


def call(kernel, outs, ins, scratch, aliases={}):
    near = lambda v, space: v if space == OUT else space(v.shape, v.dtype)
    spec = lambda space: pl.BlockSpec(memory_space=VMEM if space == OUT else space)
    run = pl.pallas_call(
        kernel,
        out_shape=[near(v, space) for v, space in outs],
        in_specs=[spec(space) for space in ins],
        out_specs=[spec(space) for _, space in outs],
        scratch_shapes=scratch,
        compiler_params=pltpu.CompilerParams(vmem_limit_bytes=24 * 1024 * 1024),
        input_output_aliases=aliases,
    )

    def apply(*args):
        return run(
            *(pltpu.with_memory_space_constraint(a, space) if space in (VMEM, HBM) else a for a, space in zip(args, ins))
        )

    return apply


def place_taps(w_ref, tap_of):
    c = w_ref.shape[0] // 4
    for b in range(3):
        for a in range(3):
            tap = tap_of(a, b)
            for row in range(2):
                at = (2 * b + row) * c
                w_ref[(a + row) * c : (a + row + 1) * c, at : at + c] = tap
        w_ref[3 * c : 4 * c, 2 * b * c : (2 * b + 1) * c] = jnp.zeros((c, c), BF16)
        w_ref[0:c, (2 * b + 1) * c : (2 * b + 2) * c] = jnp.zeros((c, c), BF16)


def forward_taps(w1_ref, w2_ref, kin_ref, kout_ref):
    for w_ref, k_ref in ((w1_ref, kin_ref), (w2_ref, kout_ref)):
        place_taps(w_ref, lambda a, b: k_ref[a, b].astype(F32).T.astype(BF16))


def own_pair(first, second):
    core = lax.axis_index("ch")
    half = first.shape[-1] // 2
    lane = lax.broadcasted_iota(jnp.int32, first.shape, len(first.shape) - 1)
    stays = jnp.where(core == 0, first, second)
    moves = pltpu.roll(jnp.where(core == 0, second, first), half, len(first.shape) - 1)
    low = (lane < half).astype(jnp.int32)
    return jnp.where(low == 1 - core, stays, moves)


def backward_taps(w3_ref, w4_ref, kin_ref, kout_ref):
    c = kin_ref.shape[-1]
    place_taps(w3_ref, lambda a, b: kout_ref[2 - a, 2 - b])
    zero = jnp.zeros((c, c), F32)
    for b in range(3):
        taps = [zero] + [kin_ref[2 - a, 2 - b].astype(F32) for a in range(3)] + [zero]
        for k in range(4):
            w4_ref[k * c : (k + 1) * c, b * c : (b + 1) * c] = own_pair(taps[k + 1], taps[k]).astype(BF16)


def tail_of(row_ref, width):
    lane_rows = lax.broadcasted_iota(jnp.int32, (TAIL, row_ref.shape[-1]), 0)
    first = row_ref[0:TAIL, :].astype(F32)
    last = row_ref[width - TAIL : width, :].astype(F32)
    zero = jnp.zeros_like(first)
    return jnp.where(lane_rows < 2, first, jnp.where(lane_rows >= TAIL - 2, last, zero)).astype(BF16)


def write_tails(x_ref, tail_ref):
    for h in range(x_ref.shape[0]):
        tail_ref[h] = tail_of(x_ref.at[h], x_ref.shape[1])


def edge_kernel(x_ref, tail_ref, edge_ref):
    rows, width, _ = x_ref.shape
    first = lax.axis_index("ch") * (rows - 2)
    for i in range(2):
        edge_ref[i, 0:width, :] = x_ref[first + i]
        edge_ref[i, width : width + TAIL, :] = tail_ref[first + i]


def pack_kernel(
    dest_hbm,
    row_hbm,
    col_hbm,
    weight_hbm,
    obs_hbm,
    precision_hbm,
    noisy_hbm,
    chunk_ref,
    near_ref,
    dest_ref,
    row_ref,
    col_ref,
    weight_ref,
    obs_ref,
    precision_ref,
    scale_ref,
    sems,
):
    pairs = (
        (dest_hbm, dest_ref),
        (row_hbm, row_ref),
        (col_hbm, col_ref),
        (weight_hbm, weight_ref),
        (obs_hbm, obs_ref),
        (precision_hbm, precision_ref),
        (noisy_hbm, near_ref),
    )
    copies = [pltpu.make_async_copy(source, target, sems.at[n]) for n, (source, target) in enumerate(pairs)]
    for copy in copies:
        copy.start()
    core = lax.axis_index("ch")
    blocks, obs, _ = weight_ref.shape
    half = obs_ref.shape[1]
    first_meta = obs + CAP * half

    def clear(slot, _):
        chunk_ref[slot] = jnp.zeros(chunk_ref.shape[1:], BF16)
        return 0

    lax.fori_loop(0, chunk_ref.shape[0], clear, 0)
    for copy in copies[:-1]:
        copy.wait()
    scale_ref[...] = precision_ref[...].astype(F32)
    meta_rows = lax.broadcasted_iota(jnp.int32, (META, obs), 0)

    def pack(b, _):
        dest = dest_ref[b]
        rank = lax.fori_loop(0, b, lambda j, n: n + (dest_ref[j] == dest).astype(jnp.int32), 0)
        chunk_ref[dest, pl.ds(pl.multiple_of(obs + rank * half, 16), half), :] = obs_ref[b]

        @pl.when(rank == core)
        def _():
            chunk_ref[dest, 0:obs, :] = weight_ref[b]
            row = row_ref[b].astype(F32)
            high = lax.div(col_ref[b], 16).astype(F32)
            low = lax.rem(col_ref[b], 16).astype(F32)
            meta = jnp.where(
                meta_rows == 0,
                jnp.broadcast_to(scale_ref[pl.ds(b, 1), :], (META, obs)),
                jnp.where(meta_rows == 1, row, jnp.where(meta_rows == 2, high, low)),
            )
            chunk_ref[dest, first_meta : first_meta + META, :] = meta.astype(BF16)

        return 0

    lax.fori_loop(0, blocks, pack, 0)
    copies[-1].wait()


def prep_kernel(own_ref, other_ref, x_ref, tail_ref, flat_ref):
    core = lax.axis_index("ch")
    half, rows, width = own_ref.shape

    def place(ref, first):
        for part in range(width // 128):
            piece = ref[:, :, part * 128 : (part + 1) * 128].astype(F32)
            flat_ref[part, pl.ds(pl.multiple_of(first * rows, 8), half * rows), :] = piece.reshape(half * rows, 128)

    place(own_ref, core * half)
    place(other_ref, (1 - core) * half)
    for h in range(rows):
        for part in range(width // 128):
            plane = flat_ref[part, pl.ds(h, 2 * half, stride=rows), :]
            x_ref[h, part * 128 : (part + 1) * 128, :] = plane.T.astype(BF16)
    write_tails(x_ref, tail_ref)


def row_pair(src_ref, w_ref, first):
    c = src_ref.shape[-1]
    wide = src_ref.shape[1]
    lhs = jnp.concatenate([src_ref[first + k] for k in range(4)], axis=1)
    y = jnp.dot(lhs, w_ref[...], preferred_element_type=F32)
    out = []
    for row in range(2):
        left, mid, right = (y[:, (2 * b + row) * c : (2 * b + row + 1) * c] for b in range(3))
        out.append(pltpu.roll(left, 1, 0) + mid + pltpu.roll(right, wide - 1, 0))
    return out


def own_row_pair(src_ref, w_ref, base, first):
    c = src_ref.shape[-1]
    wide = src_ref.shape[1]
    width = base.shape[0]
    lhs = jnp.concatenate([src_ref[first + k] for k in range(4)], axis=1)
    y = jnp.dot(lhs, w_ref[...], preferred_element_type=F32)
    y = pltpu.roll(y[:, 0:c], 1, 0) + y[:, c : 2 * c] + pltpu.roll(y[:, 2 * c : 3 * c], wide - 1, 0)
    out = base - guide_rate * y[0:width, :]
    return [out[at : at + 128, :].T for at in range(0, width, 128)]


def inside(ext_row, ext_rows):
    at = lax.axis_index("lat")
    last = lax.axis_size("lat") - 1
    return ((ext_row > 0) | (at > 0)) & ((ext_row < ext_rows - 1) | (at < last))


def activate(y, bias):
    pre = y + bias
    s = 1.0 / (1.0 + jnp.exp(-pre))
    return pre * s, s * (1.0 + pre * (1.0 - s))


def copy_row(target_ref, at, x_ref, tail_ref, row):
    width = x_ref.shape[1]
    target_ref[at, 0:width, :] = x_ref[row]
    target_ref[at, width : width + TAIL, :] = tail_ref[row]


def fill_end(ext_ref, end, x_ref, tail_ref, halo_ref):
    rows = x_ref.shape[0]
    for i in range(2):
        ext_ref[2 * end + i] = halo_ref[i]
        copy_row(ext_ref, 2 * (1 - end) + i, x_ref, tail_ref, (rows - 2) * end + i)


def fill_between(between_ref, end, new, kept_ref):
    for i in range(2):
        between_ref[2 * end + i] = new[i]
        between_ref[2 * (1 - end) + i] = kept_ref[2 * end + i]


def forward_middle_kernel(
    x_ref,
    tail_ref,
    kin_ref,
    kout_ref,
    bias_ref,
    slope_hbm,
    kept_ref,
    den_ref,
    ext_ref,
    hidden_ref,
    w1_ref,
    w2_ref,
    slope_ref,
    save_sem,
):
    rows, width, _ = x_ref.shape
    forward_taps(w1_ref, w2_ref, kin_ref, kout_ref)
    for h in range(rows):
        copy_row(ext_ref, h, x_ref, tail_ref, h)
    bias = bias_ref[...]
    for g in range((rows - 2) // 2):
        for i, y in enumerate(row_pair(ext_ref, w1_ref, 2 * g)):
            hidden, slope = activate(y, bias)
            slope_ref[2 * g + i] = slope
            hidden_ref[2 * g + i] = hidden.astype(BF16)
    save = pltpu.make_async_copy(slope_ref, slope_hbm, save_sem)
    save.start()
    for i in range(2):
        kept_ref[i] = hidden_ref[i]
        kept_ref[2 + i] = hidden_ref[rows - 4 + i]
    for g in range((rows - 4) // 2):
        for i, y in enumerate(row_pair(hidden_ref, w2_ref, 2 * g)):
            den_ref[2 * g + i] = (x_ref[2 + 2 * g + i].astype(F32) + y[0:width, :]).astype(BF16)
    save.wait()


def forward_end(end, x_ref, tail_ref, halo_ref, kept_ref, w1_ref, w2_ref, bias_ref, slope_ref, ext_ref, between_ref):
    rows, width, _ = x_ref.shape
    fill_end(ext_ref, end, x_ref, tail_ref, halo_ref)
    bias = bias_ref[...]
    new = []
    for i, y in enumerate(row_pair(ext_ref, w1_ref, 0)):
        hidden, slope = activate(y, bias)
        slope_ref[i] = slope
        new.append(jnp.where(inside(rows * end + i, rows + 2), hidden, 0.0).astype(BF16))
    fill_between(between_ref, end, new, kept_ref)
    return [
        (x_ref[(rows - 2) * end + i].astype(F32) + y[0:width, :]).astype(BF16)
        for i, y in enumerate(row_pair(between_ref, w2_ref, 0))
    ]


def forward_own_kernel(
    x_ref, tail_ref, halo_ref, kept_ref, kin_ref, kout_ref, bias_ref, slope_ref, den_ref, w1_ref, w2_ref, ext_ref, between_ref
):
    forward_taps(w1_ref, w2_ref, kin_ref, kout_ref)
    core = lax.axis_index("ch")
    den = forward_end(
        core, x_ref, tail_ref, halo_ref, kept_ref, w1_ref, w2_ref, bias_ref, slope_ref, ext_ref, between_ref
    )
    for i in range(2):
        den_ref[i] = den[i]


def forward_kernel(
    x_ref,
    tail_ref,
    halo_ref,
    kept_ref,
    w1_ref,
    w2_ref,
    bias_ref,
    den_middle_ref,
    den_own_ref,
    block_ref,
    other_block_ref,
    slope_ref,
    base_ref,
    g_ref,
    gtail_ref,
    inn_ref,
    ext_ref,
    between_ref,
    den_ref,
    field_ref,
    turned_ref,
    value_ref,
    scale_ref,
    code_ref,
):
    core = lax.axis_index("ch")
    rows, width, c = x_ref.shape
    half = inn_ref.shape[1]
    sources, obs = block_ref.shape[0], block_ref.shape[2]

    def read(source, cap, first, count):
        at = slice(first, first + count)
        return jnp.where(core == cap, block_ref[source, at, :], other_block_ref[source, at, :])

    def locate(source, cap):
        meta = read(source, cap, obs + c, META).astype(F32)
        code = meta[1:2, :] * 65536.0 + meta[2:3, :] * 16.0 + meta[3:4, :]
        code_ref[source * CAP + cap] = jnp.max(code).astype(jnp.int32)

    def turn(source, cap):
        slot = source * CAP + cap
        turned_ref[slot] = read(source, cap, 0, obs).T
        at = slice(obs + cap * half, obs + (cap + 1) * half)
        mine, theirs = block_ref[source, at, :], other_block_ref[source, at, :]
        low, high = jnp.where(core == 0, mine, theirs), jnp.where(core == 0, theirs, mine)
        value_ref[slot] = jnp.concatenate([low, high], axis=0).T
        row = read(source, cap, obs + c, META).astype(F32)[0:1, :]
        scale_ref[slot] = jnp.broadcast_to(row, (c, obs)).T

    def each(task):
        if sources <= 4:
            for source in range(sources):
                for cap in range(CAP):
                    task(source, cap)
            return

        def one(source, _):
            for cap in range(CAP):
                task(source, cap)
            return 0

        lax.fori_loop(0, sources, one, 0)

    each(locate)
    each(turn)
    end = 1 - core
    den = forward_end(
        end, x_ref, tail_ref, halo_ref, kept_ref, w1_ref, w2_ref, bias_ref, slope_ref, ext_ref, between_ref
    )
    for i in range(2):
        den_ref[(rows - 2) * end + i] = den[i].astype(F32)
        den_ref[(rows - 2) * core + i] = den_own_ref[i].astype(F32)
    for h in range(rows - 4):
        den_ref[2 + h] = den_middle_ref[h].astype(F32)
    for r in range(rows):
        field_ref[r] = jnp.zeros((width, c), F32)

    def observe(source, cap):
        slot = source * CAP + cap
        code = code_ref[slot]
        row = lax.shift_right_logical(code, 16)
        col = lax.bitwise_and(code, 65535)
        patch = jnp.concatenate([den_ref[row + i, pl.ds(col, PW), :] for i in range(PH)], axis=0).astype(BF16)
        predicted = jnp.dot(read(source, cap, 0, obs), patch, preferred_element_type=F32)
        residual = predicted - value_ref[slot].astype(F32)
        weighted = (residual * scale_ref[slot]).astype(BF16)
        pulled = jnp.dot(turned_ref[slot], weighted, preferred_element_type=F32)
        for i in range(PH):
            field_ref[row + i, pl.ds(col, PW), :] += pulled[i * PW : (i + 1) * PW, :]
        turned = residual.astype(BF16).T
        inn_ref[slot] = jnp.where(core == 0, turned[0:half], turned[half : 2 * half])

    each(observe)

    for g in range(rows // 2):
        base = []
        for r in (2 * g, 2 * g + 1):
            field = field_ref[r]
            base.append(keep_rate * x_ref[r].astype(F32) + blend_rate * den_ref[r] - guide_rate * field)
            g_ref[r] = field.astype(BF16)
        base_ref[g] = own_pair(*base)
    write_tails(g_ref, gtail_ref)


def backward_middle_kernel(
    x_ref,
    tail_ref,
    kin_ref,
    kout_ref,
    base_ref,
    slope_hbm,
    kept_ref,
    out_ref,
    ext_ref,
    grad_ref,
    w3_ref,
    w4_ref,
    slope_ref,
    load_sems,
):
    rows = x_ref.shape[0]

    def load(g):
        at = pl.ds(2 * g, 2)
        return pltpu.make_async_copy(slope_hbm.at[at], slope_ref.at[at], load_sems.at[g])

    for g in range((rows - 2) // 2):
        load(g).start()
    backward_taps(w3_ref, w4_ref, kin_ref, kout_ref)
    for h in range(rows):
        copy_row(ext_ref, h, x_ref, tail_ref, h)
    for g in range((rows - 2) // 2):
        pair = row_pair(ext_ref, w3_ref, 2 * g)
        load(g).wait()
        for i, y in enumerate(pair):
            grad_ref[2 * g + i] = (y * slope_ref[2 * g + i]).astype(BF16)
    for i in range(2):
        kept_ref[i] = grad_ref[i]
        kept_ref[2 + i] = grad_ref[rows - 4 + i]
    for g in range((rows - 4) // 2):
        for part, plane in enumerate(own_row_pair(grad_ref, w4_ref, base_ref[1 + g], 2 * g)):
            out_ref[g, part] = plane


def backward_end(end, x_ref, tail_ref, halo_ref, kept_ref, w3_ref, w4_ref, base_ref, slope_ref, ext_ref, between_ref):
    rows = x_ref.shape[0]
    fill_end(ext_ref, end, x_ref, tail_ref, halo_ref)
    new = [
        jnp.where(inside(rows * end + i, rows + 2), y * slope_ref[i], 0.0).astype(BF16)
        for i, y in enumerate(row_pair(ext_ref, w3_ref, 0))
    ]
    fill_between(between_ref, end, new, kept_ref)
    return own_row_pair(between_ref, w4_ref, base_ref[(rows // 2 - 1) * end], 0)


def backward_own_kernel(
    x_ref, tail_ref, halo_ref, kept_ref, kin_ref, kout_ref, base_ref, slope_ref, out_ref, ext_ref, between_ref, w3_ref, w4_ref
):
    backward_taps(w3_ref, w4_ref, kin_ref, kout_ref)
    planes = backward_end(
        lax.axis_index("ch"), x_ref, tail_ref, halo_ref, kept_ref, w3_ref, w4_ref, base_ref, slope_ref, ext_ref, between_ref
    )
    for part, plane in enumerate(planes):
        out_ref[part] = plane


def backward_kernel(
    x_ref,
    tail_ref,
    halo_ref,
    kept_ref,
    kin_ref,
    kout_ref,
    base_ref,
    slope_ref,
    out_middle_ref,
    out_own_ref,
    back_ref,
    dest_hbm,
    next_ref,
    inn_hbm,
    ext_ref,
    between_ref,
    flat_ref,
    w3_ref,
    w4_ref,
    dest_ref,
    dest_sem,
    inn_sems,
):
    dest_copy = pltpu.make_async_copy(dest_hbm, dest_ref, dest_sem)
    dest_copy.start()
    core = lax.axis_index("ch")
    rows = x_ref.shape[0]
    half = next_ref.shape[0]
    parts = flat_ref.shape[0]

    def put(pair, part, plane):
        for i in range(2):
            flat_ref[part, pl.ds(2 * pair + i, half, stride=rows), :] = plane[i * half : (i + 1) * half]

    backward_taps(w3_ref, w4_ref, kin_ref, kout_ref)
    planes = backward_end(
        1 - core, x_ref, tail_ref, halo_ref, kept_ref, w3_ref, w4_ref, base_ref, slope_ref, ext_ref, between_ref
    )
    for part in range(parts):
        for g in range((rows - 4) // 2):
            put(1 + g, part, out_middle_ref[g, part])
        put((rows // 2 - 1) * core, part, out_own_ref[part])
        put((rows // 2 - 1) * (1 - core), part, planes[part])
    dest_copy.wait()

    def start(b, _):
        dest = dest_ref[b]
        rank = lax.fori_loop(0, b, lambda j, n: n + (dest_ref[j] == dest).astype(jnp.int32), 0)
        pltpu.make_async_copy(back_ref.at[dest * CAP + rank], inn_hbm.at[b], inn_sems.at[b]).start()
        return 0

    def finish(b, _):
        pltpu.make_async_copy(back_ref.at[0], inn_hbm.at[b], inn_sems.at[b]).wait()
        return 0

    lax.fori_loop(0, inn_hbm.shape[0], start, 0)
    for part in range(parts):
        next_ref[:, :, part * 128 : (part + 1) * 128] = flat_ref[part].reshape(half, rows, 128)
    lax.fori_loop(0, inn_hbm.shape[0], finish, 0)


def swapped(value):
    return lax.ppermute(value, "ch", [(0, 1), (1, 0)])


def from_row_neighbour(value):
    lats = lax.axis_size("lat")
    steps = ((0, -1), (1, 1))
    pairs = [
        (i * 2 + core, (i + step) * 2 + 1 - core) for i in range(lats) for core, step in steps if 0 <= i + step < lats
    ]
    return lax.ppermute(value, ("lat", "ch"), pairs)


def from_lon_neighbours(value):
    lons = lax.axis_size("lon")

    def move(step):
        pairs = [(j * 2 + core, (j + step) % lons * 2 + 1 - core) for j in range(lons) for core in range(2)]
        return lax.ppermute(value, ("lon", "ch"), pairs)

    if lons == 2:
        return move(1)
    at = lax.broadcasted_iota(jnp.int32, (1, TAIL, 1), 1)
    return jnp.where(at < TAIL // 2, move(-1), move(1))


def exchanged(x, tail):
    _, width, c = x.shape
    beside = from_lon_neighbours(tail)
    (edge,) = call(edge_kernel, [(shape((2, width + TAIL, c), BF16), VMEM)], [VMEM] * 2, [])(x, beside)
    mine = from_row_neighbour(edge)
    return beside, mine


def shape(dims, dtype):
    return jax.ShapeDtypeStruct(dims, dtype)


def body(
    noisy_state,
    kernel_in,
    bias_in,
    kernel_out,
    interp_weight,
    observed,
    obs_precision,
    dest_tile,
    row_offset,
    col_offset,
):
    half, rows, width = noisy_state.shape
    c = kernel_in.shape[-1]
    blocks, obs, _ = interp_weight.shape
    lats = lax.axis_size("lat")
    slots = lats * CAP
    wide = width + TAIL
    other = swapped(noisy_state)
    chunk_shape = shape((lats, obs + CAP * half + META, obs), BF16)
    chunk, near = call(
        pack_kernel,
        [(chunk_shape, VMEM), (shape(noisy_state.shape, BF16), VMEM)],
        [HBM] * 7,
        [
            SMEM((blocks,), jnp.int32),
            SMEM((blocks,), jnp.int32),
            SMEM((blocks,), jnp.int32),
            VMEM(interp_weight.shape, BF16),
            VMEM(observed.shape, BF16),
            VMEM(obs_precision.shape, BF16),
            VMEM(obs_precision.shape, F32),
            pltpu.SemaphoreType.DMA((7,)),
        ],
    )(dest_tile, row_offset, col_offset, interp_weight, observed, obs_precision, noisy_state)
    block = lax.all_to_all(chunk, "lat", split_axis=0, concat_axis=0, tiled=True)
    tail_shape = shape((rows, TAIL, c), BF16)
    x, tail = call(
        prep_kernel,
        [(shape((rows, width, c), BF16), VMEM), (tail_shape, VMEM)],
        [VMEM] * 2,
        [VMEM((width // 128, c * rows, 128), F32)],
    )(near, other)
    bias = bias_in.reshape(1, c)
    pair = shape((2, wide, c), F32)
    taps = shape((4 * c, 6 * c), BF16)
    own_taps = shape((4 * c, 3 * c), BF16)
    kept_shape = shape((4, wide, c), BF16)
    four_rows, most_rows, all_rows = VMEM((4, wide, c), BF16), VMEM((rows - 2, wide, c), BF16), VMEM((rows, wide, c), BF16)
    most_slopes = VMEM((rows - 2, wide, c), F32)
    keep = lambda dims, dtype: VMEM(dims.shape, dtype)

    beside, mine = exchanged(x, tail)
    slope_middle, kept, den_middle = call(
        forward_middle_kernel,
        [(shape((rows - 2, wide, c), F32), HBM), (kept_shape, VMEM), (shape((rows - 4, width, c), BF16), VMEM)],
        [VMEM] * 5,
        [all_rows, most_rows, keep(taps, BF16), keep(taps, BF16), most_slopes, pltpu.SemaphoreType.DMA],
    )(x, beside, kernel_in, kernel_out, bias)
    mine, block, kept, slope_middle, den_middle = lax.optimization_barrier((mine, block, kept, slope_middle, den_middle))
    others = swapped(mine)
    slope_own, den_own, w1, w2 = call(
        forward_own_kernel,
        [(pair, VMEM), (shape((2, width, c), BF16), VMEM), (taps, VMEM), (taps, VMEM)],
        [VMEM] * 7,
        [four_rows, four_rows],
    )(x, beside, mine, kept, kernel_in, kernel_out, bias)
    slope_other, base, g, tail, inn = call(
        forward_kernel,
        [
            (pair, VMEM),
            (shape((rows // 2, width, c), F32), VMEM),
            (shape((rows, width, c), BF16), VMEM),
            (tail_shape, VMEM),
            (shape((slots, half, obs), BF16), VMEM),
        ],
        [VMEM] * 11,
        [
            four_rows,
            four_rows,
            VMEM((rows, width, c), F32),
            VMEM((rows, width, c), F32),
            VMEM((slots, obs, obs), BF16),
            VMEM((slots, obs, c), BF16),
            VMEM((slots, obs, c), F32),
            SMEM((slots,), jnp.int32),
        ],
        {0: 2, 1: 3},
    )(x, beside, others, kept, w1, w2, bias, den_middle, den_own, block, swapped(block))

    back = lax.all_to_all(inn, "lat", split_axis=0, concat_axis=0, tiled=True)
    beside, mine = exchanged(g, tail)
    parts = width // 128
    kept, out_middle = call(
        backward_middle_kernel,
        [(kept_shape, VMEM), (shape(((rows - 4) // 2, parts, c, 128), F32), VMEM)],
        [VMEM] * 5 + [HBM],
        [
            all_rows,
            most_rows,
            keep(taps, BF16),
            keep(own_taps, BF16),
            most_slopes,
            pltpu.SemaphoreType.DMA(((rows - 2) // 2,)),
        ],
    )(g, beside, kernel_in, kernel_out, base, slope_middle)
    mine, kept, out_middle = lax.optimization_barrier((mine, kept, out_middle))
    others = swapped(mine)
    (out_own,) = call(
        backward_own_kernel,
        [(shape((parts, c, 128), F32), VMEM)],
        [VMEM] * 8,
        [four_rows, four_rows, keep(taps, BF16), keep(own_taps, BF16)],
    )(g, beside, mine, kept, kernel_in, kernel_out, base, slope_own)
    next_state, innovation = call(
        backward_kernel,
        [(shape((half, rows, width), F32), OUT), (shape(observed.shape, BF16), HBM)],
        [VMEM] * 11 + [HBM],
        [
            four_rows,
            four_rows,
            VMEM((parts, half * rows, 128), F32),
            keep(taps, BF16),
            keep(own_taps, BF16),
            SMEM((blocks,), jnp.int32),
            pltpu.SemaphoreType.DMA,
            pltpu.SemaphoreType.DMA((blocks,)),
        ],
    )(g, beside, others, kept, kernel_in, kernel_out, base, slope_other, out_middle, out_own, back, dest_tile)
    return next_state, innovation


def solution(mesh):
    return jax.shard_map(
        body,
        mesh=mesh,
        in_specs=(
            P(("grp", "ch"), "lat", "lon"),
            P(),
            P(),
            P(),
            P(("grp", "lat", "lon"), None, None),
            P(("grp", "lat", "lon"), "ch", None),
            P(("grp", "lat", "lon"), None),
            P(("grp", "lat", "lon")),
            P(("grp", "lat", "lon")),
            P(("grp", "lat", "lon")),
        ),
        out_specs=(P(("grp", "ch"), "lat", "lon"), P(("grp", "lat", "lon"), "ch", None)),
        check_vma=False,
    )
```

```python
import jax
import jax.numpy as jnp
from jax import lax
from jax.experimental import pallas as pl
from jax.experimental.pallas import tpu as pltpu
from jax.sharding import PartitionSpec as P


PH = 4
PW = 32
CAP = 2
TAIL = 16
META = 16

keep_rate = 0.6
blend_rate = 0.4
guide_rate = 0.3

F32 = jnp.float32
BF16 = jnp.bfloat16
VMEM = pltpu.VMEM
SMEM = pltpu.SMEM
HBM = pltpu.MemorySpace.HBM
OUT = "out"


def call(kernel, outs, ins, scratch, aliases={}):
    near = lambda v, space: v if space == OUT else space(v.shape, v.dtype)
    spec = lambda space: pl.BlockSpec(memory_space=VMEM if space == OUT else space)
    run = pl.pallas_call(
        kernel,
        out_shape=[near(v, space) for v, space in outs],
        in_specs=[spec(space) for space in ins],
        out_specs=[spec(space) for _, space in outs],
        scratch_shapes=scratch,
        compiler_params=pltpu.CompilerParams(vmem_limit_bytes=24 * 1024 * 1024),
        input_output_aliases=aliases,
    )

    def apply(*args):
        return run(
            *(pltpu.with_memory_space_constraint(a, space) if space in (VMEM, HBM) else a for a, space in zip(args, ins))
        )

    return apply


def place_taps(w_ref, tap_of):
    c = w_ref.shape[0] // 4
    for b in range(3):
        for a in range(3):
            tap = tap_of(a, b)
            for row in range(2):
                at = (2 * b + row) * c
                w_ref[(a + row) * c : (a + row + 1) * c, at : at + c] = tap
        w_ref[3 * c : 4 * c, 2 * b * c : (2 * b + 1) * c] = jnp.zeros((c, c), BF16)
        w_ref[0:c, (2 * b + 1) * c : (2 * b + 2) * c] = jnp.zeros((c, c), BF16)


def forward_taps(w1_ref, w2_ref, kin_ref, kout_ref):
    for w_ref, k_ref in ((w1_ref, kin_ref), (w2_ref, kout_ref)):
        place_taps(w_ref, lambda a, b: k_ref[a, b].astype(F32).T.astype(BF16))


def own_pair(first, second):
    core = lax.axis_index("ch")
    half = first.shape[-1] // 2
    lane = lax.broadcasted_iota(jnp.int32, first.shape, len(first.shape) - 1)
    stays = jnp.where(core == 0, first, second)
    moves = pltpu.roll(jnp.where(core == 0, second, first), half, len(first.shape) - 1)
    low = (lane < half).astype(jnp.int32)
    return jnp.where(low == 1 - core, stays, moves)


def backward_taps(w3_ref, w4_ref, kin_ref, kout_ref):
    c = kin_ref.shape[-1]
    place_taps(w3_ref, lambda a, b: kout_ref[2 - a, 2 - b])
    zero = jnp.zeros((c, c), F32)
    for b in range(3):
        taps = [zero] + [kin_ref[2 - a, 2 - b].astype(F32) for a in range(3)] + [zero]
        for k in range(4):
            w4_ref[k * c : (k + 1) * c, b * c : (b + 1) * c] = own_pair(taps[k + 1], taps[k]).astype(BF16)


def tail_of(row_ref, width):
    lane_rows = lax.broadcasted_iota(jnp.int32, (TAIL, row_ref.shape[-1]), 0)
    first = row_ref[0:TAIL, :].astype(F32)
    last = row_ref[width - TAIL : width, :].astype(F32)
    zero = jnp.zeros_like(first)
    return jnp.where(lane_rows < 2, first, jnp.where(lane_rows >= TAIL - 2, last, zero)).astype(BF16)


def write_tails(x_ref, tail_ref):
    for h in range(x_ref.shape[0]):
        tail_ref[h] = tail_of(x_ref.at[h], x_ref.shape[1])


def edge_kernel(x_ref, tail_ref, edge_ref):
    rows, width, _ = x_ref.shape
    first = lax.axis_index("ch") * (rows - 2)
    for i in range(2):
        edge_ref[i, 0:width, :] = x_ref[first + i]
        edge_ref[i, width : width + TAIL, :] = tail_ref[first + i]


MOST_PERMUTES = 8


def by_permutes(lats):
    return lats <= MOST_PERMUTES and lats & (lats - 1) == 0


def piece_of(tile):
    if by_permutes(lax.axis_size("lat")):
        return lax.bitwise_xor(tile, lax.axis_index("lat"))
    return tile


def sent(pieces):
    lats = len(pieces)
    if by_permutes(lats):
        moved = [lax.ppermute(pieces[k], "lat", [(i, i ^ k) for i in range(lats)]) for k in range(1, lats)]
        return [pieces[0], *moved]
    whole = lax.all_to_all(jnp.stack(pieces), "lat", split_axis=0, concat_axis=0, tiled=True)
    return [whole[k] for k in range(lats)]


def pack_kernel(
    dest_hbm,
    row_hbm,
    col_hbm,
    weight_hbm,
    obs_hbm,
    precision_hbm,
    noisy_hbm,
    near_ref,
    code_ref,
    *refs,
):
    *piece_refs, chunk_ref, dest_ref, row_ref, col_ref, weight_ref, obs_ref, precision_ref, scale_ref, sems = refs
    pairs = (
        (dest_hbm, dest_ref),
        (row_hbm, row_ref),
        (col_hbm, col_ref),
        (weight_hbm, weight_ref),
        (obs_hbm, obs_ref),
        (precision_hbm, precision_ref),
        (noisy_hbm, near_ref),
    )
    copies = [pltpu.make_async_copy(source, target, sems.at[n]) for n, (source, target) in enumerate(pairs)]
    for copy in copies:
        copy.start()
    core = lax.axis_index("ch")
    blocks, obs, _ = weight_ref.shape
    half = obs_ref.shape[1]
    first_meta = obs + CAP * half

    def clear(piece, _):
        chunk_ref[piece] = jnp.zeros(chunk_ref.shape[1:], BF16)
        return 0

    lax.fori_loop(0, chunk_ref.shape[0], clear, 0)
    for copy in copies[:-1]:
        copy.wait()
    scale_ref[...] = precision_ref[...].astype(F32)
    meta_rows = lax.broadcasted_iota(jnp.int32, (META, obs), 0)

    def pack(b, _):
        dest = dest_ref[b]
        rank = lax.fori_loop(0, b, lambda j, n: n + (dest_ref[j] == dest).astype(jnp.int32), 0)
        piece = piece_of(dest)
        chunk_ref[piece, pl.ds(pl.multiple_of(obs + rank * half, 16), half), :] = obs_ref[b]
        code_ref[pl.ds(b, 1), :] = jnp.full((1, 128), (piece * CAP + rank).astype(F32))

        @pl.when(rank == core)
        def _():
            chunk_ref[piece, 0:obs, :] = weight_ref[b]
            row = row_ref[b].astype(F32)
            high = lax.div(col_ref[b], 16).astype(F32)
            low = lax.rem(col_ref[b], 16).astype(F32)
            meta = jnp.where(
                meta_rows == 0,
                jnp.broadcast_to(scale_ref[pl.ds(b, 1), :], (META, obs)),
                jnp.where(meta_rows == 1, row, jnp.where(meta_rows == 2, high, low)),
            )
            chunk_ref[piece, first_meta : first_meta + META, :] = meta.astype(BF16)

        return 0

    lax.fori_loop(0, blocks, pack, 0)
    for k, piece_ref in enumerate(piece_refs):
        piece_ref[...] = chunk_ref[k]
    copies[-1].wait()


def join_kernel(*refs):
    *piece_refs, whole_ref = refs
    for k, piece_ref in enumerate(piece_refs):
        whole_ref[k] = piece_ref[...]


def prep_kernel(own_ref, other_ref, x_ref, tail_ref, flat_ref):
    core = lax.axis_index("ch")
    half, rows, width = own_ref.shape

    def place(ref, first):
        for part in range(width // 128):
            piece = ref[:, :, part * 128 : (part + 1) * 128].astype(F32)
            flat_ref[part, pl.ds(pl.multiple_of(first * rows, 8), half * rows), :] = piece.reshape(half * rows, 128)

    place(own_ref, core * half)
    place(other_ref, (1 - core) * half)
    for h in range(rows):
        for part in range(width // 128):
            plane = flat_ref[part, pl.ds(h, 2 * half, stride=rows), :]
            x_ref[h, part * 128 : (part + 1) * 128, :] = plane.T.astype(BF16)
    write_tails(x_ref, tail_ref)


def row_pair(src_ref, w_ref, first):
    c = src_ref.shape[-1]
    wide = src_ref.shape[1]
    lhs = jnp.concatenate([src_ref[first + k] for k in range(4)], axis=1)
    y = jnp.dot(lhs, w_ref[...], preferred_element_type=F32)
    out = []
    for row in range(2):
        left, mid, right = (y[:, (2 * b + row) * c : (2 * b + row + 1) * c] for b in range(3))
        out.append(pltpu.roll(left, 1, 0) + mid + pltpu.roll(right, wide - 1, 0))
    return out


def own_row_pair(src_ref, w_ref, base, first):
    c = src_ref.shape[-1]
    wide = src_ref.shape[1]
    width = base.shape[0]
    lhs = jnp.concatenate([src_ref[first + k] for k in range(4)], axis=1)
    y = jnp.dot(lhs, w_ref[...], preferred_element_type=F32)
    y = pltpu.roll(y[:, 0:c], 1, 0) + y[:, c : 2 * c] + pltpu.roll(y[:, 2 * c : 3 * c], wide - 1, 0)
    out = base - guide_rate * y[0:width, :]
    return [out[at : at + 128, :].T for at in range(0, width, 128)]


def inside(ext_row, ext_rows):
    at = lax.axis_index("lat")
    last = lax.axis_size("lat") - 1
    return ((ext_row > 0) | (at > 0)) & ((ext_row < ext_rows - 1) | (at < last))


def activate(y, bias):
    pre = y + bias
    s = 1.0 / (1.0 + jnp.exp(-pre))
    return pre * s, s * (1.0 + pre * (1.0 - s))


def copy_row(target_ref, at, x_ref, tail_ref, row):
    width = x_ref.shape[1]
    target_ref[at, 0:width, :] = x_ref[row]
    target_ref[at, width : width + TAIL, :] = tail_ref[row]


def fill_end(ext_ref, end, x_ref, tail_ref, halo_ref):
    rows = x_ref.shape[0]
    for i in range(2):
        ext_ref[2 * end + i] = halo_ref[i]
        copy_row(ext_ref, 2 * (1 - end) + i, x_ref, tail_ref, (rows - 2) * end + i)


def fill_between(between_ref, end, new, kept_ref):
    for i in range(2):
        between_ref[2 * end + i] = new[i]
        between_ref[2 * (1 - end) + i] = kept_ref[2 * end + i]


def forward_middle_kernel(
    x_ref,
    tail_ref,
    kin_ref,
    kout_ref,
    bias_ref,
    slope_hbm,
    kept_ref,
    den_ref,
    ext_ref,
    hidden_ref,
    w1_ref,
    w2_ref,
    slope_ref,
    save_sem,
):
    rows, width, _ = x_ref.shape
    forward_taps(w1_ref, w2_ref, kin_ref, kout_ref)
    for h in range(rows):
        copy_row(ext_ref, h, x_ref, tail_ref, h)
    bias = bias_ref[...]
    for g in range((rows - 2) // 2):
        for i, y in enumerate(row_pair(ext_ref, w1_ref, 2 * g)):
            hidden, slope = activate(y, bias)
            slope_ref[2 * g + i] = slope
            hidden_ref[2 * g + i] = hidden.astype(BF16)
    save = pltpu.make_async_copy(slope_ref, slope_hbm, save_sem)
    save.start()
    for i in range(2):
        kept_ref[i] = hidden_ref[i]
        kept_ref[2 + i] = hidden_ref[rows - 4 + i]
    for g in range((rows - 4) // 2):
        for i, y in enumerate(row_pair(hidden_ref, w2_ref, 2 * g)):
            den_ref[2 * g + i] = (x_ref[2 + 2 * g + i].astype(F32) + y[0:width, :]).astype(BF16)
    save.wait()


def forward_end(end, x_ref, tail_ref, halo_ref, kept_ref, w1_ref, w2_ref, bias_ref, slope_ref, ext_ref, between_ref):
    rows, width, _ = x_ref.shape
    fill_end(ext_ref, end, x_ref, tail_ref, halo_ref)
    bias = bias_ref[...]
    new = []
    for i, y in enumerate(row_pair(ext_ref, w1_ref, 0)):
        hidden, slope = activate(y, bias)
        slope_ref[i] = slope
        new.append(jnp.where(inside(rows * end + i, rows + 2), hidden, 0.0).astype(BF16))
    fill_between(between_ref, end, new, kept_ref)
    return [
        (x_ref[(rows - 2) * end + i].astype(F32) + y[0:width, :]).astype(BF16)
        for i, y in enumerate(row_pair(between_ref, w2_ref, 0))
    ]


def forward_own_kernel(
    x_ref, tail_ref, halo_ref, kept_ref, kin_ref, kout_ref, bias_ref, slope_ref, den_ref, w1_ref, w2_ref, ext_ref, between_ref
):
    forward_taps(w1_ref, w2_ref, kin_ref, kout_ref)
    core = lax.axis_index("ch")
    den = forward_end(
        core, x_ref, tail_ref, halo_ref, kept_ref, w1_ref, w2_ref, bias_ref, slope_ref, ext_ref, between_ref
    )
    for i in range(2):
        den_ref[i] = den[i]


def forward_kernel(
    x_ref,
    tail_ref,
    halo_ref,
    kept_ref,
    w1_ref,
    w2_ref,
    bias_ref,
    den_middle_ref,
    den_own_ref,
    block_ref,
    other_block_ref,
    slope_ref,
    base_ref,
    g_ref,
    gtail_ref,
    *refs,
):
    *inn_refs, ext_ref, between_ref, den_ref, field_ref, turned_ref, value_ref, scale_ref, inn_ref, code_ref = refs
    core = lax.axis_index("ch")
    rows, width, c = x_ref.shape
    half = inn_refs[0].shape[1]
    sources, obs = block_ref.shape[0], block_ref.shape[2]

    def read(source, cap, first, count):
        at = slice(first, first + count)
        return jnp.where(core == cap, block_ref[source, at, :], other_block_ref[source, at, :])

    def locate(source, cap):
        meta = read(source, cap, obs + c, META).astype(F32)
        code = meta[1:2, :] * 65536.0 + meta[2:3, :] * 16.0 + meta[3:4, :]
        code_ref[source * CAP + cap] = jnp.max(code).astype(jnp.int32)

    def turn(source, cap):
        slot = source * CAP + cap
        turned_ref[slot] = read(source, cap, 0, obs).T
        at = slice(obs + cap * half, obs + (cap + 1) * half)
        mine, theirs = block_ref[source, at, :], other_block_ref[source, at, :]
        low, high = jnp.where(core == 0, mine, theirs), jnp.where(core == 0, theirs, mine)
        value_ref[slot] = jnp.concatenate([low, high], axis=0).T
        row = read(source, cap, obs + c, META).astype(F32)[0:1, :]
        scale_ref[slot] = jnp.broadcast_to(row, (c, obs)).T

    def each(task):
        if sources <= 4:
            for source in range(sources):
                for cap in range(CAP):
                    task(source, cap)
            return

        def one(source, _):
            for cap in range(CAP):
                task(source, cap)
            return 0

        lax.fori_loop(0, sources, one, 0)

    each(locate)
    each(turn)
    end = 1 - core
    den = forward_end(
        end, x_ref, tail_ref, halo_ref, kept_ref, w1_ref, w2_ref, bias_ref, slope_ref, ext_ref, between_ref
    )
    for i in range(2):
        den_ref[(rows - 2) * end + i] = den[i].astype(F32)
        den_ref[(rows - 2) * core + i] = den_own_ref[i].astype(F32)
    for h in range(rows - 4):
        den_ref[2 + h] = den_middle_ref[h].astype(F32)
    for r in range(rows):
        field_ref[r] = jnp.zeros((width, c), F32)

    def observe(source, cap):
        slot = source * CAP + cap
        code = code_ref[slot]
        row = lax.shift_right_logical(code, 16)
        col = lax.bitwise_and(code, 65535)
        patch = jnp.concatenate([den_ref[row + i, pl.ds(col, PW), :] for i in range(PH)], axis=0).astype(BF16)
        predicted = jnp.dot(read(source, cap, 0, obs), patch, preferred_element_type=F32)
        residual = predicted - value_ref[slot].astype(F32)
        weighted = (residual * scale_ref[slot]).astype(BF16)
        pulled = jnp.dot(turned_ref[slot], weighted, preferred_element_type=F32)
        for i in range(PH):
            field_ref[row + i, pl.ds(col, PW), :] += pulled[i * PW : (i + 1) * PW, :]
        turned = residual.astype(BF16).T
        inn_ref[slot] = jnp.where(core == 0, turned[0:half], turned[half : 2 * half])

    each(observe)
    for source, out_ref in enumerate(inn_refs):
        for cap in range(CAP):
            out_ref[cap] = inn_ref[source * CAP + cap]

    for g in range(rows // 2):
        base = []
        for r in (2 * g, 2 * g + 1):
            field = field_ref[r]
            base.append(keep_rate * x_ref[r].astype(F32) + blend_rate * den_ref[r] - guide_rate * field)
            g_ref[r] = field.astype(BF16)
        base_ref[g] = own_pair(*base)
    write_tails(g_ref, gtail_ref)


def backward_middle_kernel(
    x_ref,
    tail_ref,
    kin_ref,
    kout_ref,
    base_ref,
    slope_hbm,
    kept_ref,
    out_ref,
    ext_ref,
    grad_ref,
    w3_ref,
    w4_ref,
    slope_ref,
    load_sems,
):
    rows = x_ref.shape[0]

    def load(g):
        at = pl.ds(2 * g, 2)
        return pltpu.make_async_copy(slope_hbm.at[at], slope_ref.at[at], load_sems.at[g])

    for g in range((rows - 2) // 2):
        load(g).start()
    backward_taps(w3_ref, w4_ref, kin_ref, kout_ref)
    for h in range(rows):
        copy_row(ext_ref, h, x_ref, tail_ref, h)
    for g in range((rows - 2) // 2):
        pair = row_pair(ext_ref, w3_ref, 2 * g)
        load(g).wait()
        for i, y in enumerate(pair):
            grad_ref[2 * g + i] = (y * slope_ref[2 * g + i]).astype(BF16)
    for i in range(2):
        kept_ref[i] = grad_ref[i]
        kept_ref[2 + i] = grad_ref[rows - 4 + i]
    for g in range((rows - 4) // 2):
        for part, plane in enumerate(own_row_pair(grad_ref, w4_ref, base_ref[1 + g], 2 * g)):
            out_ref[g, part] = plane


def backward_end(end, x_ref, tail_ref, halo_ref, kept_ref, w3_ref, w4_ref, base_ref, slope_ref, ext_ref, between_ref):
    rows = x_ref.shape[0]
    fill_end(ext_ref, end, x_ref, tail_ref, halo_ref)
    new = [
        jnp.where(inside(rows * end + i, rows + 2), y * slope_ref[i], 0.0).astype(BF16)
        for i, y in enumerate(row_pair(ext_ref, w3_ref, 0))
    ]
    fill_between(between_ref, end, new, kept_ref)
    return own_row_pair(between_ref, w4_ref, base_ref[(rows // 2 - 1) * end], 0)


def backward_own_kernel(
    x_ref, tail_ref, halo_ref, kept_ref, kin_ref, kout_ref, base_ref, slope_ref, out_ref, ext_ref, between_ref, w3_ref, w4_ref
):
    backward_taps(w3_ref, w4_ref, kin_ref, kout_ref)
    planes = backward_end(
        lax.axis_index("ch"), x_ref, tail_ref, halo_ref, kept_ref, w3_ref, w4_ref, base_ref, slope_ref, ext_ref, between_ref
    )
    for part, plane in enumerate(planes):
        out_ref[part] = plane


def backward_kernel(
    x_ref,
    tail_ref,
    halo_ref,
    kept_ref,
    kin_ref,
    kout_ref,
    base_ref,
    slope_ref,
    out_middle_ref,
    out_own_ref,
    code_ref,
    *refs,
):
    *back_refs, next_hbm, inn_hbm, ext_ref, between_ref, flat_ref, w3_ref, w4_ref, next_sems, inn_sems = refs
    core = lax.axis_index("ch")
    rows = x_ref.shape[0]
    half = next_hbm.shape[0]
    parts = flat_ref.shape[0]

    def give(b, _):
        code = jnp.max(code_ref[pl.ds(b, 1), :]).astype(jnp.int32)
        for k, back_ref in enumerate(back_refs):

            @pl.when(lax.div(code, CAP) == k)
            def _():
                pltpu.make_async_copy(back_ref.at[lax.rem(code, CAP)], inn_hbm.at[b], inn_sems.at[b]).start()

        return 0

    def given(b, _):
        pltpu.make_async_copy(back_refs[0].at[0], inn_hbm.at[b], inn_sems.at[b]).wait()
        return 0

    def put(pair, part, plane):
        for i in range(2):
            flat_ref[part, pl.ds(2 * pair + i, half, stride=rows), :] = plane[i * half : (i + 1) * half]

    lax.fori_loop(0, inn_hbm.shape[0], give, 0)
    backward_taps(w3_ref, w4_ref, kin_ref, kout_ref)
    for part in range(parts):
        for g in range((rows - 4) // 2):
            put(1 + g, part, out_middle_ref[g, part])
        put((rows // 2 - 1) * core, part, out_own_ref[part])
    planes = backward_end(
        1 - core, x_ref, tail_ref, halo_ref, kept_ref, w3_ref, w4_ref, base_ref, slope_ref, ext_ref, between_ref
    )
    copies = []
    for part, plane in enumerate(planes):
        put((rows // 2 - 1) * (1 - core), part, plane)
        source = flat_ref.at[part].reshape(half, rows, 128)
        target = next_hbm.at[:, :, pl.ds(part * 128, 128)]
        copies.append(pltpu.make_async_copy(source, target, next_sems.at[part]))
        copies[-1].start()
    for copy in copies:
        copy.wait()
    lax.fori_loop(0, inn_hbm.shape[0], given, 0)


def swapped(value):
    return lax.ppermute(value, "ch", [(0, 1), (1, 0)])


def from_row_neighbour(value):
    lats = lax.axis_size("lat")
    steps = ((0, -1), (1, 1))
    pairs = [
        (i * 2 + core, (i + step) * 2 + 1 - core) for i in range(lats) for core, step in steps if 0 <= i + step < lats
    ]
    return lax.ppermute(value, ("lat", "ch"), pairs)


def from_lon_neighbours(value):
    lons = lax.axis_size("lon")

    def move(step):
        pairs = [(j * 2 + core, (j + step) % lons * 2 + 1 - core) for j in range(lons) for core in range(2)]
        return lax.ppermute(value, ("lon", "ch"), pairs)

    if lons == 2:
        return move(1)
    at = lax.broadcasted_iota(jnp.int32, (1, TAIL, 1), 1)
    return jnp.where(at < TAIL // 2, move(-1), move(1))


def exchanged(x, tail):
    _, width, c = x.shape
    beside = from_lon_neighbours(tail)
    (edge,) = call(edge_kernel, [(shape((2, width + TAIL, c), BF16), VMEM)], [VMEM] * 2, [])(x, beside)
    mine = from_row_neighbour(edge)
    return beside, mine


def shape(dims, dtype):
    return jax.ShapeDtypeStruct(dims, dtype)


def body(
    noisy_state,
    kernel_in,
    bias_in,
    kernel_out,
    interp_weight,
    observed,
    obs_precision,
    dest_tile,
    row_offset,
    col_offset,
):
    half, rows, width = noisy_state.shape
    c = kernel_in.shape[-1]
    blocks, obs, _ = interp_weight.shape
    lats = lax.axis_size("lat")
    slots = lats * CAP
    wide = width + TAIL
    other = swapped(noisy_state)
    piece = (obs + CAP * half + META, obs)
    near, code, *pieces = call(
        pack_kernel,
        [(shape(noisy_state.shape, BF16), VMEM), (shape((blocks, 128), F32), VMEM)] + [(shape(piece, BF16), VMEM)] * lats,
        [HBM] * 7,
        [
            VMEM((lats, *piece), BF16),
            SMEM((blocks,), jnp.int32),
            SMEM((blocks,), jnp.int32),
            SMEM((blocks,), jnp.int32),
            VMEM(interp_weight.shape, BF16),
            VMEM(observed.shape, BF16),
            VMEM(obs_precision.shape, BF16),
            VMEM(obs_precision.shape, F32),
            pltpu.SemaphoreType.DMA((7,)),
        ],
    )(dest_tile, row_offset, col_offset, interp_weight, observed, obs_precision, noisy_state)
    pieces = sent(pieces)
    tail_shape = shape((rows, TAIL, c), BF16)
    x, tail = call(
        prep_kernel,
        [(shape((rows, width, c), BF16), VMEM), (tail_shape, VMEM)],
        [VMEM] * 2,
        [VMEM((width // 128, c * rows, 128), F32)],
    )(near, other)
    bias = bias_in.reshape(1, c)
    pair = shape((2, wide, c), F32)
    taps = shape((4 * c, 6 * c), BF16)
    own_taps = shape((4 * c, 3 * c), BF16)
    kept_shape = shape((4, wide, c), BF16)
    four_rows, most_rows, all_rows = VMEM((4, wide, c), BF16), VMEM((rows - 2, wide, c), BF16), VMEM((rows, wide, c), BF16)
    most_slopes = VMEM((rows - 2, wide, c), F32)
    keep = lambda dims, dtype: VMEM(dims.shape, dtype)

    beside, mine = exchanged(x, tail)
    slope_middle, kept, den_middle = call(
        forward_middle_kernel,
        [(shape((rows - 2, wide, c), F32), HBM), (kept_shape, VMEM), (shape((rows - 4, width, c), BF16), VMEM)],
        [VMEM] * 5,
        [all_rows, most_rows, keep(taps, BF16), keep(taps, BF16), most_slopes, pltpu.SemaphoreType.DMA],
    )(x, beside, kernel_in, kernel_out, bias)
    (block,) = call(join_kernel, [(shape((lats, *piece), BF16), VMEM)], [VMEM] * lats, [])(*pieces)
    mine, block, kept, slope_middle, den_middle = lax.optimization_barrier((mine, block, kept, slope_middle, den_middle))
    others = swapped(mine)
    slope_own, den_own, w1, w2 = call(
        forward_own_kernel,
        [(pair, VMEM), (shape((2, width, c), BF16), VMEM), (taps, VMEM), (taps, VMEM)],
        [VMEM] * 7,
        [four_rows, four_rows],
    )(x, beside, mine, kept, kernel_in, kernel_out, bias)
    slope_other, base, g, tail, *inn = call(
        forward_kernel,
        [
            (pair, VMEM),
            (shape((rows // 2, width, c), F32), VMEM),
            (shape((rows, width, c), BF16), VMEM),
            (tail_shape, VMEM),
            *[(shape((CAP, half, obs), BF16), VMEM)] * lats,
        ],
        [VMEM] * 11,
        [
            four_rows,
            four_rows,
            VMEM((rows, width, c), F32),
            VMEM((rows, width, c), F32),
            VMEM((slots, obs, obs), BF16),
            VMEM((slots, obs, c), BF16),
            VMEM((slots, obs, c), F32),
            VMEM((slots, half, obs), BF16),
            SMEM((slots,), jnp.int32),
        ],
        {0: 2, 1: 3},
    )(x, beside, others, kept, w1, w2, bias, den_middle, den_own, block, swapped(block))

    back = sent(inn)
    beside, mine = exchanged(g, tail)
    parts = width // 128
    kept, out_middle = call(
        backward_middle_kernel,
        [(kept_shape, VMEM), (shape(((rows - 4) // 2, parts, c, 128), F32), VMEM)],
        [VMEM] * 5 + [HBM],
        [
            all_rows,
            most_rows,
            keep(taps, BF16),
            keep(own_taps, BF16),
            most_slopes,
            pltpu.SemaphoreType.DMA(((rows - 2) // 2,)),
        ],
    )(g, beside, kernel_in, kernel_out, base, slope_middle)
    mine, kept, out_middle = lax.optimization_barrier((mine, kept, out_middle))
    others = swapped(mine)
    (out_own,) = call(
        backward_own_kernel,
        [(shape((parts, c, 128), F32), VMEM)],
        [VMEM] * 8,
        [four_rows, four_rows, keep(taps, BF16), keep(own_taps, BF16)],
    )(g, beside, mine, kept, kernel_in, kernel_out, base, slope_own)
    next_state, innovation = call(
        backward_kernel,
        [(shape((half, rows, width), F32), HBM), (shape(observed.shape, BF16), HBM)],
        [VMEM] * (11 + lats),
        [
            four_rows,
            four_rows,
            VMEM((parts, half * rows, 128), F32),
            keep(taps, BF16),
            keep(own_taps, BF16),
            pltpu.SemaphoreType.DMA((parts,)),
            pltpu.SemaphoreType.DMA((blocks,)),
        ],
    )(g, beside, others, kept, kernel_in, kernel_out, base, slope_other, out_middle, out_own, code, *back)
    return next_state, innovation


def solution(mesh):
    return jax.shard_map(
        body,
        mesh=mesh,
        in_specs=(
            P(("grp", "ch"), "lat", "lon"),
            P(),
            P(),
            P(),
            P(("grp", "lat", "lon"), None, None),
            P(("grp", "lat", "lon"), "ch", None),
            P(("grp", "lat", "lon"), None),
            P(("grp", "lat", "lon")),
            P(("grp", "lat", "lon")),
            P(("grp", "lat", "lon")),
        ),
        out_specs=(P(("grp", "ch"), "lat", "lon"), P(("grp", "lat", "lon"), "ch", None)),
        check_vma=False,
    )
```

```python
import jax
import jax.numpy as jnp
from jax import lax
from jax.experimental import pallas as pl
from jax.experimental.pallas import tpu as pltpu
from jax.sharding import PartitionSpec as P


PH = 4
PW = 32
CAP = 2
TAIL = 16
META = 16

keep_rate = 0.6
blend_rate = 0.4
guide_rate = 0.3

F32 = jnp.float32
BF16 = jnp.bfloat16
VMEM = pltpu.VMEM
SMEM = pltpu.SMEM
HBM = pltpu.MemorySpace.HBM
OUT = "out"


def call(kernel, outs, ins, scratch, aliases={}):
    near = lambda v, space: v if space == OUT else space(v.shape, v.dtype)
    spec = lambda space: pl.BlockSpec(memory_space=VMEM if space == OUT else space)
    run = pl.pallas_call(
        kernel,
        out_shape=[near(v, space) for v, space in outs],
        in_specs=[spec(space) for space in ins],
        out_specs=[spec(space) for _, space in outs],
        scratch_shapes=scratch,
        compiler_params=pltpu.CompilerParams(vmem_limit_bytes=24 * 1024 * 1024),
        input_output_aliases=aliases,
    )

    def apply(*args):
        return run(
            *(pltpu.with_memory_space_constraint(a, space) if space in (VMEM, HBM) else a for a, space in zip(args, ins))
        )

    return apply


def place_taps(w_ref, tap_of):
    c = w_ref.shape[0] // 4
    for b in range(3):
        for a in range(3):
            tap = tap_of(a, b)
            for row in range(2):
                at = (2 * b + row) * c
                w_ref[(a + row) * c : (a + row + 1) * c, at : at + c] = tap
        w_ref[3 * c : 4 * c, 2 * b * c : (2 * b + 1) * c] = jnp.zeros((c, c), BF16)
        w_ref[0:c, (2 * b + 1) * c : (2 * b + 2) * c] = jnp.zeros((c, c), BF16)


def forward_taps(w1_ref, w2_ref, kin_ref, kout_ref):
    for w_ref, k_ref in ((w1_ref, kin_ref), (w2_ref, kout_ref)):
        place_taps(w_ref, lambda a, b: k_ref[a, b].astype(F32).T.astype(BF16))


def own_pair(first, second):
    core = lax.axis_index("ch")
    half = first.shape[-1] // 2
    lane = lax.broadcasted_iota(jnp.int32, first.shape, len(first.shape) - 1)
    stays = jnp.where(core == 0, first, second)
    moves = pltpu.roll(jnp.where(core == 0, second, first), half, len(first.shape) - 1)
    low = (lane < half).astype(jnp.int32)
    return jnp.where(low == 1 - core, stays, moves)


def backward_taps(w3_ref, w4_ref, kin_ref, kout_ref):
    c = kin_ref.shape[-1]
    place_taps(w3_ref, lambda a, b: kout_ref[2 - a, 2 - b])
    zero = jnp.zeros((c, c), F32)
    for b in range(3):
        taps = [zero] + [kin_ref[2 - a, 2 - b].astype(F32) for a in range(3)] + [zero]
        for k in range(4):
            w4_ref[k * c : (k + 1) * c, b * c : (b + 1) * c] = own_pair(taps[k + 1], taps[k]).astype(BF16)


def tail_of(row_ref, width):
    lane_rows = lax.broadcasted_iota(jnp.int32, (TAIL, row_ref.shape[-1]), 0)
    first = row_ref[0:TAIL, :].astype(F32)
    last = row_ref[width - TAIL : width, :].astype(F32)
    zero = jnp.zeros_like(first)
    return jnp.where(lane_rows < 2, first, jnp.where(lane_rows >= TAIL - 2, last, zero)).astype(BF16)


def write_tails(x_ref, tail_ref):
    for h in range(x_ref.shape[0]):
        tail_ref[h] = tail_of(x_ref.at[h], x_ref.shape[1])


def edge_kernel(x_ref, tail_ref, edge_ref):
    rows, width, _ = x_ref.shape
    first = lax.axis_index("ch") * (rows - 2)
    for i in range(2):
        edge_ref[i, 0:width, :] = x_ref[first + i]
        edge_ref[i, width : width + TAIL, :] = tail_ref[first + i]


MOST_PERMUTES = 8


def by_permutes(lats):
    return lats <= MOST_PERMUTES and lats & (lats - 1) == 0


def piece_of(tile):
    if by_permutes(lax.axis_size("lat")):
        return lax.bitwise_xor(tile, lax.axis_index("lat"))
    return tile


def sent(pieces):
    lats = len(pieces)
    if by_permutes(lats):
        moved = [pieces[0]]
        for k in range(1, lats):
            moved.append(lax.ppermute(pieces[k], "lat", [(i, i ^ k) for i in range(lats)]))
        return moved
    whole = lax.all_to_all(jnp.stack(pieces), "lat", split_axis=0, concat_axis=0, tiled=True)
    return [whole[k] for k in range(lats)]


def pack_kernel(
    dest_hbm,
    row_hbm,
    col_hbm,
    weight_hbm,
    obs_hbm,
    precision_hbm,
    noisy_hbm,
    near_ref,
    code_ref,
    *refs,
):
    *piece_refs, chunk_ref, dest_ref, row_ref, col_ref, weight_ref, obs_ref, precision_ref, scale_ref, sems = refs
    pairs = (
        (dest_hbm, dest_ref),
        (row_hbm, row_ref),
        (col_hbm, col_ref),
        (weight_hbm, weight_ref),
        (obs_hbm, obs_ref),
        (precision_hbm, precision_ref),
        (noisy_hbm, near_ref),
    )
    copies = [pltpu.make_async_copy(source, target, sems.at[n]) for n, (source, target) in enumerate(pairs)]
    for copy in copies:
        copy.start()
    core = lax.axis_index("ch")
    blocks, obs, _ = weight_ref.shape
    half = obs_ref.shape[1]
    first_meta = obs + CAP * half

    def clear(piece, _):
        chunk_ref[piece] = jnp.zeros(chunk_ref.shape[1:], BF16)
        return 0

    lax.fori_loop(0, chunk_ref.shape[0], clear, 0)
    for copy in copies[:-1]:
        copy.wait()
    scale_ref[...] = precision_ref[...].astype(F32)
    meta_rows = lax.broadcasted_iota(jnp.int32, (META, obs), 0)

    def pack(b, _):
        dest = dest_ref[b]
        rank = lax.fori_loop(0, b, lambda j, n: n + (dest_ref[j] == dest).astype(jnp.int32), 0)
        piece = piece_of(dest)
        chunk_ref[piece, pl.ds(pl.multiple_of(obs + rank * half, 16), half), :] = obs_ref[b]
        code_ref[pl.ds(b, 1), :] = jnp.full((1, 128), (piece * CAP + rank).astype(F32))

        @pl.when(rank == core)
        def _():
            chunk_ref[piece, 0:obs, :] = weight_ref[b]
            row = row_ref[b].astype(F32)
            high = lax.div(col_ref[b], 16).astype(F32)
            low = lax.rem(col_ref[b], 16).astype(F32)
            meta = jnp.where(
                meta_rows == 0,
                jnp.broadcast_to(scale_ref[pl.ds(b, 1), :], (META, obs)),
                jnp.where(meta_rows == 1, row, jnp.where(meta_rows == 2, high, low)),
            )
            chunk_ref[piece, first_meta : first_meta + META, :] = meta.astype(BF16)

        return 0

    lax.fori_loop(0, blocks, pack, 0)
    for k, piece_ref in enumerate(piece_refs):
        piece_ref[...] = chunk_ref[k]
    copies[-1].wait()


def join_kernel(*refs):
    *piece_refs, whole_ref = refs
    for k, piece_ref in enumerate(piece_refs):
        whole_ref[k] = piece_ref[...]


def prep_kernel(own_ref, other_ref, x_ref, tail_ref, flat_ref):
    core = lax.axis_index("ch")
    half, rows, width = own_ref.shape

    def place(ref, first):
        for part in range(width // 128):
            piece = ref[:, :, part * 128 : (part + 1) * 128].astype(F32)
            flat_ref[part, pl.ds(pl.multiple_of(first * rows, 8), half * rows), :] = piece.reshape(half * rows, 128)

    place(own_ref, core * half)
    place(other_ref, (1 - core) * half)
    for h in range(rows):
        for part in range(width // 128):
            plane = flat_ref[part, pl.ds(h, 2 * half, stride=rows), :]
            x_ref[h, part * 128 : (part + 1) * 128, :] = plane.T.astype(BF16)
    write_tails(x_ref, tail_ref)


def row_pair(src_ref, w_ref, first):
    c = src_ref.shape[-1]
    wide = src_ref.shape[1]
    lhs = jnp.concatenate([src_ref[first + k] for k in range(4)], axis=1)
    y = jnp.dot(lhs, w_ref[...], preferred_element_type=F32)
    out = []
    for row in range(2):
        left, mid, right = (y[:, (2 * b + row) * c : (2 * b + row + 1) * c] for b in range(3))
        out.append(pltpu.roll(left, 1, 0) + mid + pltpu.roll(right, wide - 1, 0))
    return out


def own_row_pair(src_ref, w_ref, base, first):
    c = src_ref.shape[-1]
    wide = src_ref.shape[1]
    width = base.shape[0]
    lhs = jnp.concatenate([src_ref[first + k] for k in range(4)], axis=1)
    y = jnp.dot(lhs, w_ref[...], preferred_element_type=F32)
    y = pltpu.roll(y[:, 0:c], 1, 0) + y[:, c : 2 * c] + pltpu.roll(y[:, 2 * c : 3 * c], wide - 1, 0)
    out = base - guide_rate * y[0:width, :]
    return [out[at : at + 128, :].T for at in range(0, width, 128)]


def inside(ext_row, ext_rows):
    at = lax.axis_index("lat")
    last = lax.axis_size("lat") - 1
    return ((ext_row > 0) | (at > 0)) & ((ext_row < ext_rows - 1) | (at < last))


def activate(y, bias):
    pre = y + bias
    s = 1.0 / (1.0 + jnp.exp(-pre))
    return pre * s, s * (1.0 + pre * (1.0 - s))


def copy_row(target_ref, at, x_ref, tail_ref, row):
    width = x_ref.shape[1]
    target_ref[at, 0:width, :] = x_ref[row]
    target_ref[at, width : width + TAIL, :] = tail_ref[row]


def fill_end(ext_ref, end, x_ref, tail_ref, halo_ref):
    rows = x_ref.shape[0]
    for i in range(2):
        ext_ref[2 * end + i] = halo_ref[i]
        copy_row(ext_ref, 2 * (1 - end) + i, x_ref, tail_ref, (rows - 2) * end + i)


def fill_between(between_ref, end, new, kept_ref):
    for i in range(2):
        between_ref[2 * end + i] = new[i]
        between_ref[2 * (1 - end) + i] = kept_ref[2 * end + i]


def forward_middle_kernel(
    x_ref,
    tail_ref,
    kin_ref,
    kout_ref,
    bias_ref,
    slope_ref,
    kept_ref,
    den_ref,
    ext_ref,
    hidden_ref,
    w1_ref,
    w2_ref,
):
    rows, width, _ = x_ref.shape
    forward_taps(w1_ref, w2_ref, kin_ref, kout_ref)
    for h in range(rows):
        copy_row(ext_ref, h, x_ref, tail_ref, h)
    bias = bias_ref[...]
    for g in range((rows - 2) // 2):
        for i, y in enumerate(row_pair(ext_ref, w1_ref, 2 * g)):
            hidden, slope = activate(y, bias)
            slope_ref[2 * g + i] = slope
            hidden_ref[2 * g + i] = hidden.astype(BF16)
    for i in range(2):
        kept_ref[i] = hidden_ref[i]
        kept_ref[2 + i] = hidden_ref[rows - 4 + i]
    for g in range((rows - 4) // 2):
        for i, y in enumerate(row_pair(hidden_ref, w2_ref, 2 * g)):
            den_ref[2 * g + i] = (x_ref[2 + 2 * g + i].astype(F32) + y[0:width, :]).astype(BF16)


def forward_end(end, x_ref, tail_ref, halo_ref, kept_ref, w1_ref, w2_ref, bias_ref, slope_ref, ext_ref, between_ref):
    rows, width, _ = x_ref.shape
    fill_end(ext_ref, end, x_ref, tail_ref, halo_ref)
    bias = bias_ref[...]
    new = []
    for i, y in enumerate(row_pair(ext_ref, w1_ref, 0)):
        hidden, slope = activate(y, bias)
        slope_ref[i] = slope
        new.append(jnp.where(inside(rows * end + i, rows + 2), hidden, 0.0).astype(BF16))
    fill_between(between_ref, end, new, kept_ref)
    return [
        (x_ref[(rows - 2) * end + i].astype(F32) + y[0:width, :]).astype(BF16)
        for i, y in enumerate(row_pair(between_ref, w2_ref, 0))
    ]


def forward_own_kernel(
    x_ref, tail_ref, halo_ref, kept_ref, kin_ref, kout_ref, bias_ref, slope_ref, den_ref, w1_ref, w2_ref, ext_ref, between_ref
):
    forward_taps(w1_ref, w2_ref, kin_ref, kout_ref)
    core = lax.axis_index("ch")
    den = forward_end(
        core, x_ref, tail_ref, halo_ref, kept_ref, w1_ref, w2_ref, bias_ref, slope_ref, ext_ref, between_ref
    )
    for i in range(2):
        den_ref[i] = den[i]


def forward_kernel(
    x_ref,
    tail_ref,
    halo_ref,
    kept_ref,
    w1_ref,
    w2_ref,
    bias_ref,
    den_middle_ref,
    den_own_ref,
    block_ref,
    other_block_ref,
    slope_ref,
    base_ref,
    g_ref,
    gtail_ref,
    *refs,
):
    *inn_refs, ext_ref, between_ref, den_ref, field_ref, turned_ref, value_ref, scale_ref, inn_ref, code_ref = refs
    core = lax.axis_index("ch")
    rows, width, c = x_ref.shape
    half = inn_refs[0].shape[1]
    sources, obs = block_ref.shape[0], block_ref.shape[2]

    def read(source, cap, first, count):
        at = slice(first, first + count)
        return jnp.where(core == cap, block_ref[source, at, :], other_block_ref[source, at, :])

    def locate(source, cap):
        meta = read(source, cap, obs + c, META).astype(F32)
        code = meta[1:2, :] * 65536.0 + meta[2:3, :] * 16.0 + meta[3:4, :]
        code_ref[source * CAP + cap] = jnp.max(code).astype(jnp.int32)

    def turn(source, cap):
        slot = source * CAP + cap
        turned_ref[slot] = read(source, cap, 0, obs).T
        at = slice(obs + cap * half, obs + (cap + 1) * half)
        mine, theirs = block_ref[source, at, :], other_block_ref[source, at, :]
        low, high = jnp.where(core == 0, mine, theirs), jnp.where(core == 0, theirs, mine)
        value_ref[slot] = jnp.concatenate([low, high], axis=0).T
        row = read(source, cap, obs + c, META).astype(F32)[0:1, :]
        scale_ref[slot] = jnp.broadcast_to(row, (c, obs)).T

    def each(task):
        if sources <= 4:
            for source in range(sources):
                for cap in range(CAP):
                    task(source, cap)
            return

        def one(source, _):
            for cap in range(CAP):
                task(source, cap)
            return 0

        lax.fori_loop(0, sources, one, 0)

    each(locate)
    each(turn)
    end = 1 - core
    den = forward_end(
        end, x_ref, tail_ref, halo_ref, kept_ref, w1_ref, w2_ref, bias_ref, slope_ref, ext_ref, between_ref
    )
    for i in range(2):
        den_ref[(rows - 2) * end + i] = den[i].astype(F32)
        den_ref[(rows - 2) * core + i] = den_own_ref[i].astype(F32)
    for h in range(rows - 4):
        den_ref[2 + h] = den_middle_ref[h].astype(F32)
    for r in range(rows):
        field_ref[r] = jnp.zeros((width, c), F32)

    def observe(source, cap):
        slot = source * CAP + cap
        code = code_ref[slot]
        row = lax.shift_right_logical(code, 16)
        col = lax.bitwise_and(code, 65535)
        patch = jnp.concatenate([den_ref[row + i, pl.ds(col, PW), :] for i in range(PH)], axis=0).astype(BF16)
        predicted = jnp.dot(read(source, cap, 0, obs), patch, preferred_element_type=F32)
        residual = predicted - value_ref[slot].astype(F32)
        weighted = (residual * scale_ref[slot]).astype(BF16)
        pulled = jnp.dot(turned_ref[slot], weighted, preferred_element_type=F32)
        for i in range(PH):
            field_ref[row + i, pl.ds(col, PW), :] += pulled[i * PW : (i + 1) * PW, :]
        turned = residual.astype(BF16).T
        inn_ref[slot] = jnp.where(core == 0, turned[0:half], turned[half : 2 * half])

    each(observe)
    for source, out_ref in enumerate(inn_refs):
        for cap in range(CAP):
            out_ref[cap] = inn_ref[source * CAP + cap]

    for g in range(rows // 2):
        base = []
        for r in (2 * g, 2 * g + 1):
            field = field_ref[r]
            base.append(keep_rate * x_ref[r].astype(F32) + blend_rate * den_ref[r] - guide_rate * field)
            g_ref[r] = field.astype(BF16)
        base_ref[g] = own_pair(*base)
    write_tails(g_ref, gtail_ref)


def backward_middle_kernel(
    x_ref,
    tail_ref,
    kin_ref,
    kout_ref,
    base_ref,
    slope_ref,
    kept_ref,
    out_ref,
    ext_ref,
    grad_ref,
    w3_ref,
    w4_ref,
):
    rows = x_ref.shape[0]
    backward_taps(w3_ref, w4_ref, kin_ref, kout_ref)
    for h in range(rows):
        copy_row(ext_ref, h, x_ref, tail_ref, h)
    for g in range((rows - 2) // 2):
        for i, y in enumerate(row_pair(ext_ref, w3_ref, 2 * g)):
            grad_ref[2 * g + i] = (y * slope_ref[2 * g + i]).astype(BF16)
    for i in range(2):
        kept_ref[i] = grad_ref[i]
        kept_ref[2 + i] = grad_ref[rows - 4 + i]
    for g in range((rows - 4) // 2):
        for part, plane in enumerate(own_row_pair(grad_ref, w4_ref, base_ref[1 + g], 2 * g)):
            out_ref[g, part] = plane


def backward_end(end, x_ref, tail_ref, halo_ref, kept_ref, w3_ref, w4_ref, base_ref, slope_ref, ext_ref, between_ref):
    rows = x_ref.shape[0]
    fill_end(ext_ref, end, x_ref, tail_ref, halo_ref)
    new = [
        jnp.where(inside(rows * end + i, rows + 2), y * slope_ref[i], 0.0).astype(BF16)
        for i, y in enumerate(row_pair(ext_ref, w3_ref, 0))
    ]
    fill_between(between_ref, end, new, kept_ref)
    return own_row_pair(between_ref, w4_ref, base_ref[(rows // 2 - 1) * end], 0)


def backward_own_kernel(
    x_ref, tail_ref, halo_ref, kept_ref, kin_ref, kout_ref, base_ref, slope_ref, out_ref, ext_ref, between_ref, w3_ref, w4_ref
):
    backward_taps(w3_ref, w4_ref, kin_ref, kout_ref)
    planes = backward_end(
        lax.axis_index("ch"), x_ref, tail_ref, halo_ref, kept_ref, w3_ref, w4_ref, base_ref, slope_ref, ext_ref, between_ref
    )
    for part, plane in enumerate(planes):
        out_ref[part] = plane


def backward_kernel(
    x_ref,
    tail_ref,
    halo_ref,
    kept_ref,
    kin_ref,
    kout_ref,
    base_ref,
    slope_ref,
    out_middle_ref,
    out_own_ref,
    code_ref,
    *refs,
):
    *back_refs, next_hbm, inn_hbm, ext_ref, between_ref, flat_ref, w3_ref, w4_ref, next_sems, inn_sems = refs
    core = lax.axis_index("ch")
    rows = x_ref.shape[0]
    half = next_hbm.shape[0]
    parts = flat_ref.shape[0]

    def give(b, _):
        code = jnp.max(code_ref[pl.ds(b, 1), :]).astype(jnp.int32)
        for k, back_ref in enumerate(back_refs):

            @pl.when(lax.div(code, CAP) == k)
            def _():
                pltpu.make_async_copy(back_ref.at[lax.rem(code, CAP)], inn_hbm.at[b], inn_sems.at[b]).start()

        return 0

    def given(b, _):
        pltpu.make_async_copy(back_refs[0].at[0], inn_hbm.at[b], inn_sems.at[b]).wait()
        return 0

    def put(pair, part, plane):
        for i in range(2):
            flat_ref[part, pl.ds(2 * pair + i, half, stride=rows), :] = plane[i * half : (i + 1) * half]

    lax.fori_loop(0, inn_hbm.shape[0], give, 0, unroll=inn_hbm.shape[0] <= 8)
    backward_taps(w3_ref, w4_ref, kin_ref, kout_ref)
    for part in range(parts):
        for g in range((rows - 4) // 2):
            put(1 + g, part, out_middle_ref[g, part])
        put((rows // 2 - 1) * core, part, out_own_ref[part])
    planes = backward_end(
        1 - core, x_ref, tail_ref, halo_ref, kept_ref, w3_ref, w4_ref, base_ref, slope_ref, ext_ref, between_ref
    )
    copies = []
    for part, plane in enumerate(planes):
        put((rows // 2 - 1) * (1 - core), part, plane)
        source = flat_ref.at[part].reshape(half, rows, 128)
        target = next_hbm.at[:, :, pl.ds(part * 128, 128)]
        copies.append(pltpu.make_async_copy(source, target, next_sems.at[part]))
        copies[-1].start()
    for copy in copies:
        copy.wait()
    lax.fori_loop(0, inn_hbm.shape[0], given, 0)


def swapped(value):
    return lax.ppermute(value, "ch", [(0, 1), (1, 0)])


def from_row_neighbour(value):
    lats = lax.axis_size("lat")
    steps = ((0, -1), (1, 1))
    pairs = [
        (i * 2 + core, (i + step) * 2 + 1 - core) for i in range(lats) for core, step in steps if 0 <= i + step < lats
    ]
    return lax.ppermute(value, ("lat", "ch"), pairs)


def from_lon_neighbours(value):
    lons = lax.axis_size("lon")

    def move(step):
        pairs = [(j * 2 + core, (j + step) % lons * 2 + 1 - core) for j in range(lons) for core in range(2)]
        return lax.ppermute(value, ("lon", "ch"), pairs)

    if lons == 2:
        return move(1)
    at = lax.broadcasted_iota(jnp.int32, (1, TAIL, 1), 1)
    return jnp.where(at < TAIL // 2, move(-1), move(1))


def exchanged(x, tail):
    _, width, c = x.shape
    beside = from_lon_neighbours(tail)
    (edge,) = call(edge_kernel, [(shape((2, width + TAIL, c), BF16), VMEM)], [VMEM] * 2, [])(x, beside)
    mine = from_row_neighbour(edge)
    return beside, mine


def shape(dims, dtype):
    return jax.ShapeDtypeStruct(dims, dtype)


def body(
    noisy_state,
    kernel_in,
    bias_in,
    kernel_out,
    interp_weight,
    observed,
    obs_precision,
    dest_tile,
    row_offset,
    col_offset,
):
    half, rows, width = noisy_state.shape
    c = kernel_in.shape[-1]
    blocks, obs, _ = interp_weight.shape
    lats = lax.axis_size("lat")
    slots = lats * CAP
    wide = width + TAIL
    other = swapped(noisy_state)
    piece = (obs + CAP * half + META, obs)
    near, code, *pieces = call(
        pack_kernel,
        [(shape(noisy_state.shape, BF16), VMEM), (shape((blocks, 128), F32), VMEM)] + [(shape(piece, BF16), VMEM)] * lats,
        [HBM] * 7,
        [
            VMEM((lats, *piece), BF16),
            SMEM((blocks,), jnp.int32),
            SMEM((blocks,), jnp.int32),
            SMEM((blocks,), jnp.int32),
            VMEM(interp_weight.shape, BF16),
            VMEM(observed.shape, BF16),
            VMEM(obs_precision.shape, BF16),
            VMEM(obs_precision.shape, F32),
            pltpu.SemaphoreType.DMA((7,)),
        ],
    )(dest_tile, row_offset, col_offset, interp_weight, observed, obs_precision, noisy_state)
    pieces = sent(pieces)
    tail_shape = shape((rows, TAIL, c), BF16)
    x, tail = call(
        prep_kernel,
        [(shape((rows, width, c), BF16), VMEM), (tail_shape, VMEM)],
        [VMEM] * 2,
        [VMEM((width // 128, c * rows, 128), F32)],
    )(near, other)
    bias = bias_in.reshape(1, c)
    pair = shape((2, wide, c), F32)
    taps = shape((4 * c, 6 * c), BF16)
    own_taps = shape((4 * c, 3 * c), BF16)
    kept_shape = shape((4, wide, c), BF16)
    four_rows, most_rows, all_rows = VMEM((4, wide, c), BF16), VMEM((rows - 2, wide, c), BF16), VMEM((rows, wide, c), BF16)
    keep = lambda dims, dtype: VMEM(dims.shape, dtype)

    beside, mine = exchanged(x, tail)
    slope_middle, kept, den_middle = call(
        forward_middle_kernel,
        [(shape((rows - 2, wide, c), F32), VMEM), (kept_shape, VMEM), (shape((rows - 4, width, c), BF16), VMEM)],
        [VMEM] * 5,
        [all_rows, most_rows, keep(taps, BF16), keep(taps, BF16)],
    )(x, beside, kernel_in, kernel_out, bias)
    (block,) = call(join_kernel, [(shape((lats, *piece), BF16), VMEM)], [VMEM] * lats, [])(*pieces)
    mine, block, kept, slope_middle, den_middle = lax.optimization_barrier((mine, block, kept, slope_middle, den_middle))
    others = swapped(mine)
    slope_own, den_own, w1, w2 = call(
        forward_own_kernel,
        [(pair, VMEM), (shape((2, width, c), BF16), VMEM), (taps, VMEM), (taps, VMEM)],
        [VMEM] * 7,
        [four_rows, four_rows],
    )(x, beside, mine, kept, kernel_in, kernel_out, bias)
    slope_other, base, g, tail, *inn = call(
        forward_kernel,
        [
            (pair, VMEM),
            (shape((rows // 2, width, c), F32), VMEM),
            (shape((rows, width, c), BF16), VMEM),
            (tail_shape, VMEM),
            *[(shape((CAP, half, obs), BF16), VMEM)] * lats,
        ],
        [VMEM] * 11,
        [
            four_rows,
            four_rows,
            VMEM((rows, width, c), F32),
            VMEM((rows, width, c), F32),
            VMEM((slots, obs, obs), BF16),
            VMEM((slots, obs, c), BF16),
            VMEM((slots, obs, c), F32),
            VMEM((slots, half, obs), BF16),
            SMEM((slots,), jnp.int32),
        ],
        {0: 2, 1: 3},
    )(x, beside, others, kept, w1, w2, bias, den_middle, den_own, block, swapped(block))

    back = sent(inn)
    beside, mine = exchanged(g, tail)
    parts = width // 128
    kept, out_middle = call(
        backward_middle_kernel,
        [(kept_shape, VMEM), (shape(((rows - 4) // 2, parts, c, 128), F32), VMEM)],
        [VMEM] * 6,
        [all_rows, most_rows, keep(taps, BF16), keep(own_taps, BF16)],
    )(g, beside, kernel_in, kernel_out, base, slope_middle)
    mine, kept, out_middle = lax.optimization_barrier((mine, kept, out_middle))
    others = swapped(mine)
    (out_own,) = call(
        backward_own_kernel,
        [(shape((parts, c, 128), F32), VMEM)],
        [VMEM] * 8,
        [four_rows, four_rows, keep(taps, BF16), keep(own_taps, BF16)],
    )(g, beside, mine, kept, kernel_in, kernel_out, base, slope_own)
    next_state, innovation = call(
        backward_kernel,
        [(shape((half, rows, width), F32), HBM), (shape(observed.shape, BF16), HBM)],
        [VMEM] * (11 + lats),
        [
            four_rows,
            four_rows,
            VMEM((parts, half * rows, 128), F32),
            keep(taps, BF16),
            keep(own_taps, BF16),
            pltpu.SemaphoreType.DMA((parts,)),
            pltpu.SemaphoreType.DMA((blocks,)),
        ],
    )(g, beside, others, kept, kernel_in, kernel_out, base, slope_other, out_middle, out_own, code, *back)
    return next_state, innovation


def solution(mesh):
    return jax.shard_map(
        body,
        mesh=mesh,
        in_specs=(
            P(("grp", "ch"), "lat", "lon"),
            P(),
            P(),
            P(),
            P(("grp", "lat", "lon"), None, None),
            P(("grp", "lat", "lon"), "ch", None),
            P(("grp", "lat", "lon"), None),
            P(("grp", "lat", "lon")),
            P(("grp", "lat", "lon")),
            P(("grp", "lat", "lon")),
        ),
        out_specs=(P(("grp", "ch"), "lat", "lon"), P(("grp", "lat", "lon"), "ch", None)),
        check_vma=False,
    )
```

```python
import jax
import jax.numpy as jnp
from jax import lax
from jax.experimental import pallas as pl
from jax.experimental.pallas import tpu as pltpu
from jax.sharding import PartitionSpec as P


PH = 4
PW = 32
CAP = 2
TAIL = 16
META = 16

keep_rate = 0.6
blend_rate = 0.4
guide_rate = 0.3

F32 = jnp.float32
BF16 = jnp.bfloat16
VMEM = pltpu.VMEM
SMEM = pltpu.SMEM
HBM = pltpu.MemorySpace.HBM
OUT = "out"


def call(kernel, outs, ins, scratch, aliases={}):
    near = lambda v, space: v if space == OUT else space(v.shape, v.dtype)
    spec = lambda space: pl.BlockSpec(memory_space=VMEM if space == OUT else space)
    run = pl.pallas_call(
        kernel,
        out_shape=[near(v, space) for v, space in outs],
        in_specs=[spec(space) for space in ins],
        out_specs=[spec(space) for _, space in outs],
        scratch_shapes=scratch,
        compiler_params=pltpu.CompilerParams(vmem_limit_bytes=24 * 1024 * 1024),
        input_output_aliases=aliases,
    )

    def apply(*args):
        return run(
            *(pltpu.with_memory_space_constraint(a, space) if space in (VMEM, HBM) else a for a, space in zip(args, ins))
        )

    return apply


def place_taps(w_ref, tap_of):
    c = w_ref.shape[0] // 4
    for b in range(3):
        for a in range(3):
            tap = tap_of(a, b)
            for row in range(2):
                at = (2 * b + row) * c
                w_ref[(a + row) * c : (a + row + 1) * c, at : at + c] = tap
        w_ref[3 * c : 4 * c, 2 * b * c : (2 * b + 1) * c] = jnp.zeros((c, c), BF16)
        w_ref[0:c, (2 * b + 1) * c : (2 * b + 2) * c] = jnp.zeros((c, c), BF16)


def forward_taps(w1_ref, w2_ref, kin_ref, kout_ref):
    for w_ref, k_ref in ((w1_ref, kin_ref), (w2_ref, kout_ref)):
        place_taps(w_ref, lambda a, b: k_ref[a, b].astype(F32).T.astype(BF16))


def own_pair(first, second):
    core = lax.axis_index("ch")
    half = first.shape[-1] // 2
    lane = lax.broadcasted_iota(jnp.int32, first.shape, len(first.shape) - 1)
    stays = jnp.where(core == 0, first, second)
    moves = pltpu.roll(jnp.where(core == 0, second, first), half, len(first.shape) - 1)
    low = (lane < half).astype(jnp.int32)
    return jnp.where(low == 1 - core, stays, moves)


def backward_taps(w3_ref, w4_ref, kin_ref, kout_ref):
    c = kin_ref.shape[-1]
    place_taps(w3_ref, lambda a, b: kout_ref[2 - a, 2 - b])
    zero = jnp.zeros((c, c), F32)
    for b in range(3):
        taps = [zero] + [kin_ref[2 - a, 2 - b].astype(F32) for a in range(3)] + [zero]
        for k in range(4):
            w4_ref[k * c : (k + 1) * c, b * c : (b + 1) * c] = own_pair(taps[k + 1], taps[k]).astype(BF16)


def tail_of(row_ref, width):
    lane_rows = lax.broadcasted_iota(jnp.int32, (TAIL, row_ref.shape[-1]), 0)
    first = row_ref[0:TAIL, :].astype(F32)
    last = row_ref[width - TAIL : width, :].astype(F32)
    zero = jnp.zeros_like(first)
    return jnp.where(lane_rows < 2, first, jnp.where(lane_rows >= TAIL - 2, last, zero)).astype(BF16)


def write_tails(x_ref, tail_ref):
    for h in range(x_ref.shape[0]):
        tail_ref[h] = tail_of(x_ref.at[h], x_ref.shape[1])


def edge_kernel(x_ref, tail_ref, edge_ref):
    rows, width, _ = x_ref.shape
    first = lax.axis_index("ch") * (rows - 2)
    for i in range(2):
        edge_ref[i, 0:width, :] = x_ref[first + i]
        edge_ref[i, width : width + TAIL, :] = tail_ref[first + i]


MOST_PERMUTES = 8


def by_permutes(lats):
    return lats <= MOST_PERMUTES and lats & (lats - 1) == 0


def piece_of(tile):
    if by_permutes(lax.axis_size("lat")):
        return lax.bitwise_xor(tile, lax.axis_index("lat"))
    return tile


def sent(pieces):
    lats = len(pieces)
    if by_permutes(lats):
        moved = [pieces[0]]
        for k in range(1, lats):
            moved.append(lax.ppermute(pieces[k], "lat", [(i, i ^ k) for i in range(lats)]))
        return moved
    whole = lax.all_to_all(jnp.stack(pieces), "lat", split_axis=0, concat_axis=0, tiled=True)
    return [whole[k] for k in range(lats)]


def pack_kernel(
    dest_hbm,
    row_hbm,
    col_hbm,
    weight_hbm,
    obs_hbm,
    precision_hbm,
    noisy_hbm,
    near_ref,
    code_ref,
    *refs,
):
    *piece_refs, chunk_ref, dest_ref, row_ref, col_ref, weight_ref, obs_ref, precision_ref, scale_ref, sems = refs
    pairs = (
        (dest_hbm, dest_ref),
        (row_hbm, row_ref),
        (col_hbm, col_ref),
        (weight_hbm, weight_ref),
        (obs_hbm, obs_ref),
        (precision_hbm, precision_ref),
        (noisy_hbm, near_ref),
    )
    copies = [pltpu.make_async_copy(source, target, sems.at[n]) for n, (source, target) in enumerate(pairs)]
    for copy in copies:
        copy.start()
    core = lax.axis_index("ch")
    blocks, obs, _ = weight_ref.shape
    half = obs_ref.shape[1]
    first_meta = obs + CAP * half

    def clear(piece, _):
        chunk_ref[piece] = jnp.zeros(chunk_ref.shape[1:], BF16)
        return 0

    lax.fori_loop(0, chunk_ref.shape[0], clear, 0)
    for copy in copies[:-1]:
        copy.wait()
    scale_ref[...] = precision_ref[...].astype(F32)
    meta_rows = lax.broadcasted_iota(jnp.int32, (META, obs), 0)

    def pack(b, _):
        dest = dest_ref[b]
        rank = lax.fori_loop(0, b, lambda j, n: n + (dest_ref[j] == dest).astype(jnp.int32), 0)
        piece = piece_of(dest)
        chunk_ref[piece, pl.ds(pl.multiple_of(obs + rank * half, 16), half), :] = obs_ref[b]
        code_ref[pl.ds(b, 1), :] = jnp.full((1, 128), (piece * CAP + rank).astype(F32))

        @pl.when(rank == core)
        def _():
            chunk_ref[piece, 0:obs, :] = weight_ref[b]
            row = row_ref[b].astype(F32)
            high = lax.div(col_ref[b], 16).astype(F32)
            low = lax.rem(col_ref[b], 16).astype(F32)
            meta = jnp.where(
                meta_rows == 0,
                jnp.broadcast_to(scale_ref[pl.ds(b, 1), :], (META, obs)),
                jnp.where(meta_rows == 1, row, jnp.where(meta_rows == 2, high, low)),
            )
            chunk_ref[piece, first_meta : first_meta + META, :] = meta.astype(BF16)

        return 0

    lax.fori_loop(0, blocks, pack, 0)
    for k, piece_ref in enumerate(piece_refs):
        piece_ref[...] = chunk_ref[k]
    copies[-1].wait()


def join_kernel(*refs):
    *piece_refs, whole_ref = refs
    for k, piece_ref in enumerate(piece_refs):
        whole_ref[k] = piece_ref[...]


def prep_kernel(own_ref, other_ref, x_ref, tail_ref, flat_ref):
    core = lax.axis_index("ch")
    half, rows, width = own_ref.shape

    def place(ref, first):
        for part in range(width // 128):
            piece = ref[:, :, part * 128 : (part + 1) * 128].astype(F32)
            flat_ref[part, pl.ds(pl.multiple_of(first * rows, 8), half * rows), :] = piece.reshape(half * rows, 128)

    place(own_ref, core * half)
    place(other_ref, (1 - core) * half)
    for h in range(rows):
        for part in range(width // 128):
            plane = flat_ref[part, pl.ds(h, 2 * half, stride=rows), :]
            x_ref[h, part * 128 : (part + 1) * 128, :] = plane.T.astype(BF16)
    write_tails(x_ref, tail_ref)


def row_pair(src_ref, w_ref, first):
    c = src_ref.shape[-1]
    wide = src_ref.shape[1]
    lhs = jnp.concatenate([src_ref[first + k] for k in range(4)], axis=1)
    y = jnp.dot(lhs, w_ref[...], preferred_element_type=F32)
    out = []
    for row in range(2):
        left, mid, right = (y[:, (2 * b + row) * c : (2 * b + row + 1) * c] for b in range(3))
        out.append(pltpu.roll(left, 1, 0) + mid + pltpu.roll(right, wide - 1, 0))
    return out


def own_row_pair(src_ref, w_ref, base, first):
    c = src_ref.shape[-1]
    wide = src_ref.shape[1]
    width = base.shape[0]
    lhs = jnp.concatenate([src_ref[first + k] for k in range(4)], axis=1)
    y = jnp.dot(lhs, w_ref[...], preferred_element_type=F32)
    y = pltpu.roll(y[:, 0:c], 1, 0) + y[:, c : 2 * c] + pltpu.roll(y[:, 2 * c : 3 * c], wide - 1, 0)
    out = base - guide_rate * y[0:width, :]
    return [out[at : at + 128, :].T for at in range(0, width, 128)]


def inside(ext_row, ext_rows):
    at = lax.axis_index("lat")
    last = lax.axis_size("lat") - 1
    return ((ext_row > 0) | (at > 0)) & ((ext_row < ext_rows - 1) | (at < last))


def activate(y, bias):
    pre = y + bias
    s = 1.0 / (1.0 + jnp.exp(-pre))
    return pre * s, s * (1.0 + pre * (1.0 - s))


def copy_row(target_ref, at, x_ref, tail_ref, row):
    width = x_ref.shape[1]
    target_ref[at, 0:width, :] = x_ref[row]
    target_ref[at, width : width + TAIL, :] = tail_ref[row]


def fill_end(ext_ref, end, x_ref, tail_ref, halo_ref):
    rows = x_ref.shape[0]
    for i in range(2):
        ext_ref[2 * end + i] = halo_ref[i]
        copy_row(ext_ref, 2 * (1 - end) + i, x_ref, tail_ref, (rows - 2) * end + i)


def fill_between(between_ref, end, new, kept_ref):
    for i in range(2):
        between_ref[2 * end + i] = new[i]
        between_ref[2 * (1 - end) + i] = kept_ref[2 * end + i]


def forward_middle_kernel(
    x_ref,
    tail_ref,
    kin_ref,
    kout_ref,
    bias_ref,
    slope_ref,
    kept_ref,
    den_ref,
    w1_ref,
    w2_ref,
    ext_ref,
    hidden_ref,
):
    rows, width, _ = x_ref.shape
    forward_taps(w1_ref, w2_ref, kin_ref, kout_ref)
    for h in range(rows):
        copy_row(ext_ref, h, x_ref, tail_ref, h)
    bias = bias_ref[...]
    for g in range((rows - 2) // 2):
        for i, y in enumerate(row_pair(ext_ref, w1_ref, 2 * g)):
            hidden, slope = activate(y, bias)
            slope_ref[2 * g + i] = slope
            hidden_ref[2 * g + i] = hidden.astype(BF16)
    for i in range(2):
        kept_ref[i] = hidden_ref[i]
        kept_ref[2 + i] = hidden_ref[rows - 4 + i]
    for g in range((rows - 4) // 2):
        for i, y in enumerate(row_pair(hidden_ref, w2_ref, 2 * g)):
            den_ref[2 * g + i] = (x_ref[2 + 2 * g + i].astype(F32) + y[0:width, :]).astype(BF16)


def forward_end(end, x_ref, tail_ref, halo_ref, kept_ref, w1_ref, w2_ref, bias_ref, slope_ref, ext_ref, between_ref):
    rows, width, _ = x_ref.shape
    fill_end(ext_ref, end, x_ref, tail_ref, halo_ref)
    bias = bias_ref[...]
    new = []
    for i, y in enumerate(row_pair(ext_ref, w1_ref, 0)):
        hidden, slope = activate(y, bias)
        slope_ref[i] = slope
        new.append(jnp.where(inside(rows * end + i, rows + 2), hidden, 0.0).astype(BF16))
    fill_between(between_ref, end, new, kept_ref)
    return [
        (x_ref[(rows - 2) * end + i].astype(F32) + y[0:width, :]).astype(BF16)
        for i, y in enumerate(row_pair(between_ref, w2_ref, 0))
    ]


def forward_own_kernel(
    x_ref, tail_ref, halo_ref, kept_ref, w1_ref, w2_ref, bias_ref, slope_ref, den_ref, ext_ref, between_ref
):
    core = lax.axis_index("ch")
    den = forward_end(
        core, x_ref, tail_ref, halo_ref, kept_ref, w1_ref, w2_ref, bias_ref, slope_ref, ext_ref, between_ref
    )
    for i in range(2):
        den_ref[i] = den[i]


def forward_kernel(
    x_ref,
    tail_ref,
    halo_ref,
    kept_ref,
    w1_ref,
    w2_ref,
    bias_ref,
    den_middle_ref,
    den_own_ref,
    block_ref,
    other_block_ref,
    slope_ref,
    base_ref,
    g_ref,
    gtail_ref,
    *refs,
):
    *inn_refs, ext_ref, between_ref, den_ref, field_ref, turned_ref, value_ref, scale_ref, inn_ref, code_ref = refs
    core = lax.axis_index("ch")
    rows, width, c = x_ref.shape
    half = inn_refs[0].shape[1]
    sources, obs = block_ref.shape[0], block_ref.shape[2]

    def read(source, cap, first, count):
        at = slice(first, first + count)
        return jnp.where(core == cap, block_ref[source, at, :], other_block_ref[source, at, :])

    def locate(source, cap):
        meta = read(source, cap, obs + c, META).astype(F32)
        code = meta[1:2, :] * 65536.0 + meta[2:3, :] * 16.0 + meta[3:4, :]
        code_ref[source * CAP + cap] = jnp.max(code).astype(jnp.int32)

    def turn(source, cap):
        slot = source * CAP + cap
        turned_ref[slot] = read(source, cap, 0, obs).T
        at = slice(obs + cap * half, obs + (cap + 1) * half)
        mine, theirs = block_ref[source, at, :], other_block_ref[source, at, :]
        low, high = jnp.where(core == 0, mine, theirs), jnp.where(core == 0, theirs, mine)
        value_ref[slot] = jnp.concatenate([low, high], axis=0).T
        row = read(source, cap, obs + c, META).astype(F32)[0:1, :]
        scale_ref[slot] = jnp.broadcast_to(row, (c, obs)).T

    def each(task):
        if sources <= 4:
            for source in range(sources):
                for cap in range(CAP):
                    task(source, cap)
            return

        def one(source, _):
            for cap in range(CAP):
                task(source, cap)
            return 0

        lax.fori_loop(0, sources, one, 0)

    each(locate)
    each(turn)
    end = 1 - core
    den = forward_end(
        end, x_ref, tail_ref, halo_ref, kept_ref, w1_ref, w2_ref, bias_ref, slope_ref, ext_ref, between_ref
    )
    for i in range(2):
        den_ref[(rows - 2) * end + i] = den[i].astype(F32)
        den_ref[(rows - 2) * core + i] = den_own_ref[i].astype(F32)
    for h in range(rows - 4):
        den_ref[2 + h] = den_middle_ref[h].astype(F32)
    for r in range(rows):
        field_ref[r] = jnp.zeros((width, c), F32)

    def observe(source, cap):
        slot = source * CAP + cap
        code = code_ref[slot]
        row = lax.shift_right_logical(code, 16)
        col = lax.bitwise_and(code, 65535)
        patch = jnp.concatenate([den_ref[row + i, pl.ds(col, PW), :] for i in range(PH)], axis=0).astype(BF16)
        predicted = jnp.dot(read(source, cap, 0, obs), patch, preferred_element_type=F32)
        residual = predicted - value_ref[slot].astype(F32)
        weighted = (residual * scale_ref[slot]).astype(BF16)
        pulled = jnp.dot(turned_ref[slot], weighted, preferred_element_type=F32)
        for i in range(PH):
            field_ref[row + i, pl.ds(col, PW), :] += pulled[i * PW : (i + 1) * PW, :]
        turned = residual.astype(BF16).T
        inn_ref[slot] = jnp.where(core == 0, turned[0:half], turned[half : 2 * half])

    each(observe)
    for source, out_ref in enumerate(inn_refs):
        for cap in range(CAP):
            out_ref[cap] = inn_ref[source * CAP + cap]

    for g in range(rows // 2):
        base = []
        for r in (2 * g, 2 * g + 1):
            field = field_ref[r]
            base.append(keep_rate * x_ref[r].astype(F32) + blend_rate * den_ref[r] - guide_rate * field)
            g_ref[r] = field.astype(BF16)
        base_ref[g] = own_pair(*base)
    write_tails(g_ref, gtail_ref)


def backward_middle_kernel(
    x_ref,
    tail_ref,
    kin_ref,
    kout_ref,
    base_ref,
    slope_ref,
    kept_ref,
    out_ref,
    w3_ref,
    w4_ref,
    ext_ref,
    grad_ref,
):
    rows = x_ref.shape[0]
    backward_taps(w3_ref, w4_ref, kin_ref, kout_ref)
    for h in range(rows):
        copy_row(ext_ref, h, x_ref, tail_ref, h)
    for g in range((rows - 2) // 2):
        for i, y in enumerate(row_pair(ext_ref, w3_ref, 2 * g)):
            grad_ref[2 * g + i] = (y * slope_ref[2 * g + i]).astype(BF16)
    for i in range(2):
        kept_ref[i] = grad_ref[i]
        kept_ref[2 + i] = grad_ref[rows - 4 + i]
    for g in range((rows - 4) // 2):
        for part, plane in enumerate(own_row_pair(grad_ref, w4_ref, base_ref[1 + g], 2 * g)):
            out_ref[g, part] = plane


def backward_end(end, x_ref, tail_ref, halo_ref, kept_ref, w3_ref, w4_ref, base_ref, slope_ref, ext_ref, between_ref):
    rows = x_ref.shape[0]
    fill_end(ext_ref, end, x_ref, tail_ref, halo_ref)
    new = [
        jnp.where(inside(rows * end + i, rows + 2), y * slope_ref[i], 0.0).astype(BF16)
        for i, y in enumerate(row_pair(ext_ref, w3_ref, 0))
    ]
    fill_between(between_ref, end, new, kept_ref)
    return own_row_pair(between_ref, w4_ref, base_ref[(rows // 2 - 1) * end], 0)


def backward_own_kernel(
    x_ref, tail_ref, halo_ref, kept_ref, w3_ref, w4_ref, base_ref, slope_ref, out_ref, ext_ref, between_ref
):
    planes = backward_end(
        lax.axis_index("ch"), x_ref, tail_ref, halo_ref, kept_ref, w3_ref, w4_ref, base_ref, slope_ref, ext_ref, between_ref
    )
    for part, plane in enumerate(planes):
        out_ref[part] = plane


def backward_kernel(
    x_ref,
    tail_ref,
    halo_ref,
    kept_ref,
    w3_ref,
    w4_ref,
    base_ref,
    slope_ref,
    out_middle_ref,
    out_own_ref,
    code_ref,
    *refs,
):
    *back_refs, next_hbm, inn_hbm, ext_ref, between_ref, flat_ref, next_sems, inn_sems = refs
    core = lax.axis_index("ch")
    rows = x_ref.shape[0]
    half = next_hbm.shape[0]
    parts = flat_ref.shape[0]

    def give(b, _):
        code = jnp.max(code_ref[pl.ds(b, 1), :]).astype(jnp.int32)
        for k, back_ref in enumerate(back_refs):

            @pl.when(lax.div(code, CAP) == k)
            def _():
                pltpu.make_async_copy(back_ref.at[lax.rem(code, CAP)], inn_hbm.at[b], inn_sems.at[b]).start()

        return 0

    def given(b, _):
        pltpu.make_async_copy(back_refs[0].at[0], inn_hbm.at[b], inn_sems.at[b]).wait()
        return 0

    def put(pair, part, plane):
        for i in range(2):
            flat_ref[part, pl.ds(2 * pair + i, half, stride=rows), :] = plane[i * half : (i + 1) * half]

    lax.fori_loop(0, inn_hbm.shape[0], give, 0, unroll=inn_hbm.shape[0] <= 8)
    for part in range(parts):
        for g in range((rows - 4) // 2):
            put(1 + g, part, out_middle_ref[g, part])
        put((rows // 2 - 1) * core, part, out_own_ref[part])
    planes = backward_end(
        1 - core, x_ref, tail_ref, halo_ref, kept_ref, w3_ref, w4_ref, base_ref, slope_ref, ext_ref, between_ref
    )
    copies = []
    for part, plane in enumerate(planes):
        put((rows // 2 - 1) * (1 - core), part, plane)
        source = flat_ref.at[part].reshape(half, rows, 128)
        target = next_hbm.at[:, :, pl.ds(part * 128, 128)]
        copies.append(pltpu.make_async_copy(source, target, next_sems.at[part]))
        copies[-1].start()
    for copy in copies:
        copy.wait()
    lax.fori_loop(0, inn_hbm.shape[0], given, 0)


def swapped(value):
    return lax.ppermute(value, "ch", [(0, 1), (1, 0)])


def from_row_neighbour(value):
    lats = lax.axis_size("lat")
    steps = ((0, -1), (1, 1))
    pairs = [
        (i * 2 + core, (i + step) * 2 + 1 - core) for i in range(lats) for core, step in steps if 0 <= i + step < lats
    ]
    return lax.ppermute(value, ("lat", "ch"), pairs)


def from_lon_neighbours(value):
    lons = lax.axis_size("lon")

    def move(step):
        pairs = [(j * 2 + core, (j + step) % lons * 2 + 1 - core) for j in range(lons) for core in range(2)]
        return lax.ppermute(value, ("lon", "ch"), pairs)

    if lons == 2:
        return move(1)
    at = lax.broadcasted_iota(jnp.int32, (1, TAIL, 1), 1)
    return jnp.where(at < TAIL // 2, move(-1), move(1))


def exchanged(x, tail):
    _, width, c = x.shape
    beside = from_lon_neighbours(tail)
    (edge,) = call(edge_kernel, [(shape((2, width + TAIL, c), BF16), VMEM)], [VMEM] * 2, [])(x, beside)
    mine = from_row_neighbour(edge)
    return beside, mine


def shape(dims, dtype):
    return jax.ShapeDtypeStruct(dims, dtype)


def body(
    noisy_state,
    kernel_in,
    bias_in,
    kernel_out,
    interp_weight,
    observed,
    obs_precision,
    dest_tile,
    row_offset,
    col_offset,
):
    half, rows, width = noisy_state.shape
    c = kernel_in.shape[-1]
    blocks, obs, _ = interp_weight.shape
    lats = lax.axis_size("lat")
    slots = lats * CAP
    wide = width + TAIL
    other = swapped(noisy_state)
    piece = (obs + CAP * half + META, obs)
    near, code, *pieces = call(
        pack_kernel,
        [(shape(noisy_state.shape, BF16), VMEM), (shape((blocks, 128), F32), VMEM)] + [(shape(piece, BF16), VMEM)] * lats,
        [HBM] * 7,
        [
            VMEM((lats, *piece), BF16),
            SMEM((blocks,), jnp.int32),
            SMEM((blocks,), jnp.int32),
            SMEM((blocks,), jnp.int32),
            VMEM(interp_weight.shape, BF16),
            VMEM(observed.shape, BF16),
            VMEM(obs_precision.shape, BF16),
            VMEM(obs_precision.shape, F32),
            pltpu.SemaphoreType.DMA((7,)),
        ],
    )(dest_tile, row_offset, col_offset, interp_weight, observed, obs_precision, noisy_state)
    pieces = sent(pieces)
    tail_shape = shape((rows, TAIL, c), BF16)
    x, tail = call(
        prep_kernel,
        [(shape((rows, width, c), BF16), VMEM), (tail_shape, VMEM)],
        [VMEM] * 2,
        [VMEM((width // 128, c * rows, 128), F32)],
    )(near, other)
    bias = bias_in.reshape(1, c)
    pair = shape((2, wide, c), F32)
    taps = shape((4 * c, 6 * c), BF16)
    own_taps = shape((4 * c, 3 * c), BF16)
    kept_shape = shape((4, wide, c), BF16)
    four_rows, most_rows, all_rows = VMEM((4, wide, c), BF16), VMEM((rows - 2, wide, c), BF16), VMEM((rows, wide, c), BF16)

    beside, mine = exchanged(x, tail)
    slope_middle, kept, den_middle, w1, w2 = call(
        forward_middle_kernel,
        [
            (shape((rows - 2, wide, c), F32), VMEM),
            (kept_shape, VMEM),
            (shape((rows - 4, width, c), BF16), VMEM),
            (taps, VMEM),
            (taps, VMEM),
        ],
        [VMEM] * 5,
        [all_rows, most_rows],
    )(x, beside, kernel_in, kernel_out, bias)
    pieces, kept = lax.optimization_barrier((pieces, kept))
    (block,) = call(join_kernel, [(shape((lats, *piece), BF16), VMEM)], [VMEM] * lats, [])(*pieces)
    other_block = swapped(block)
    mine, kept, slope_middle, den_middle = lax.optimization_barrier((mine, kept, slope_middle, den_middle))
    others = swapped(mine)
    slope_own, den_own = call(
        forward_own_kernel, [(pair, VMEM), (shape((2, width, c), BF16), VMEM)], [VMEM] * 7, [four_rows, four_rows]
    )(x, beside, mine, kept, w1, w2, bias)
    slope_other, base, g, tail, *inn = call(
        forward_kernel,
        [
            (pair, VMEM),
            (shape((rows // 2, width, c), F32), VMEM),
            (shape((rows, width, c), BF16), VMEM),
            (tail_shape, VMEM),
            *[(shape((CAP, half, obs), BF16), VMEM)] * lats,
        ],
        [VMEM] * 11,
        [
            four_rows,
            four_rows,
            VMEM((rows, width, c), F32),
            VMEM((rows, width, c), F32),
            VMEM((slots, obs, obs), BF16),
            VMEM((slots, obs, c), BF16),
            VMEM((slots, obs, c), F32),
            VMEM((slots, half, obs), BF16),
            SMEM((slots,), jnp.int32),
        ],
        {0: 2, 1: 3},
    )(x, beside, others, kept, w1, w2, bias, den_middle, den_own, block, other_block)

    back = sent(inn)
    beside, mine = exchanged(g, tail)
    parts = width // 128
    kept, out_middle, w3, w4 = call(
        backward_middle_kernel,
        [
            (kept_shape, VMEM),
            (shape(((rows - 4) // 2, parts, c, 128), F32), VMEM),
            (taps, VMEM),
            (own_taps, VMEM),
        ],
        [VMEM] * 6,
        [all_rows, most_rows],
    )(g, beside, kernel_in, kernel_out, base, slope_middle)
    mine, kept, out_middle = lax.optimization_barrier((mine, kept, out_middle))
    others = swapped(mine)
    (out_own,) = call(
        backward_own_kernel, [(shape((parts, c, 128), F32), VMEM)], [VMEM] * 8, [four_rows, four_rows]
    )(g, beside, mine, kept, w3, w4, base, slope_own)
    next_state, innovation = call(
        backward_kernel,
        [(shape((half, rows, width), F32), HBM), (shape(observed.shape, BF16), HBM)],
        [VMEM] * (11 + lats),
        [
            four_rows,
            four_rows,
            VMEM((parts, half * rows, 128), F32),
            pltpu.SemaphoreType.DMA((parts,)),
            pltpu.SemaphoreType.DMA((blocks,)),
        ],
    )(g, beside, others, kept, w3, w4, base, slope_other, out_middle, out_own, code, *back)
    return next_state, innovation


def solution(mesh):
    return jax.shard_map(
        body,
        mesh=mesh,
        in_specs=(
            P(("grp", "ch"), "lat", "lon"),
            P(),
            P(),
            P(),
            P(("grp", "lat", "lon"), None, None),
            P(("grp", "lat", "lon"), "ch", None),
            P(("grp", "lat", "lon"), None),
            P(("grp", "lat", "lon")),
            P(("grp", "lat", "lon")),
            P(("grp", "lat", "lon")),
        ),
        out_specs=(P(("grp", "ch"), "lat", "lon"), P(("grp", "lat", "lon"), "ch", None)),
        check_vma=False,
    )
```

```python
import jax
import jax.numpy as jnp
from jax import lax
from jax.experimental import pallas as pl
from jax.experimental.pallas import tpu as pltpu
from jax.sharding import PartitionSpec as P


PH = 4
PW = 32
CAP = 2
TAIL = 16
META = 8

keep_rate = 0.6
blend_rate = 0.4
guide_rate = 0.3

F32 = jnp.float32
BF16 = jnp.bfloat16
VMEM = pltpu.VMEM
SMEM = pltpu.SMEM
HBM = pltpu.MemorySpace.HBM
OUT = "out"


def call(kernel, outs, ins, scratch, aliases={}):
    near = lambda v, space: v if space == OUT else space(v.shape, v.dtype)
    spec = lambda space: pl.BlockSpec(memory_space=VMEM if space == OUT else space)
    run = pl.pallas_call(
        kernel,
        out_shape=[near(v, space) for v, space in outs],
        in_specs=[spec(space) for space in ins],
        out_specs=[spec(space) for _, space in outs],
        scratch_shapes=scratch,
        compiler_params=pltpu.CompilerParams(vmem_limit_bytes=24 * 1024 * 1024),
        input_output_aliases=aliases,
    )

    def apply(*args):
        return run(
            *(pltpu.with_memory_space_constraint(a, space) if space in (VMEM, HBM) else a for a, space in zip(args, ins))
        )

    return apply


def place_taps(w_ref, tap_of):
    c = w_ref.shape[0] // 4
    for b in range(3):
        for a in range(3):
            tap = tap_of(a, b)
            for row in range(2):
                at = (2 * b + row) * c
                w_ref[(a + row) * c : (a + row + 1) * c, at : at + c] = tap
        w_ref[3 * c : 4 * c, 2 * b * c : (2 * b + 1) * c] = jnp.zeros((c, c), BF16)
        w_ref[0:c, (2 * b + 1) * c : (2 * b + 2) * c] = jnp.zeros((c, c), BF16)


def forward_taps(w1_ref, w2_ref, kin_ref, kout_ref):
    for w_ref, k_ref in ((w1_ref, kin_ref), (w2_ref, kout_ref)):
        place_taps(w_ref, lambda a, b: k_ref[a, b].astype(F32).T.astype(BF16))


def own_pair(first, second):
    core = lax.axis_index("ch")
    half = first.shape[-1] // 2
    lane = lax.broadcasted_iota(jnp.int32, first.shape, len(first.shape) - 1)
    stays = jnp.where(core == 0, first, second)
    moves = pltpu.roll(jnp.where(core == 0, second, first), half, len(first.shape) - 1)
    low = (lane < half).astype(jnp.int32)
    return jnp.where(low == 1 - core, stays, moves)


def backward_taps(w3_ref, w4_ref, kin_ref, kout_ref):
    c = kin_ref.shape[-1]
    place_taps(w3_ref, lambda a, b: kout_ref[2 - a, 2 - b])
    zero = jnp.zeros((c, c), F32)
    for b in range(3):
        taps = [zero] + [kin_ref[2 - a, 2 - b].astype(F32) for a in range(3)] + [zero]
        for k in range(4):
            w4_ref[k * c : (k + 1) * c, b * c : (b + 1) * c] = own_pair(taps[k + 1], taps[k]).astype(BF16)


def tail_of(row_ref, width):
    lane_rows = lax.broadcasted_iota(jnp.int32, (TAIL, row_ref.shape[-1]), 0)
    first = row_ref[0:TAIL, :].astype(F32)
    last = row_ref[width - TAIL : width, :].astype(F32)
    zero = jnp.zeros_like(first)
    return jnp.where(lane_rows < 2, first, jnp.where(lane_rows >= TAIL - 2, last, zero)).astype(BF16)


def write_tails(x_ref, tail_ref):
    for h in range(x_ref.shape[0]):
        tail_ref[h] = tail_of(x_ref.at[h], x_ref.shape[1])


def edge_kernel(x_ref, tail_ref, edge_ref):
    rows, width, _ = x_ref.shape
    first = lax.axis_index("ch") * (rows - 2)
    for i in range(2):
        edge_ref[i, 0:width, :] = x_ref[first + i]
        edge_ref[i, width : width + TAIL, :] = tail_ref[first + i]


MOST_PERMUTES = 8


def by_permutes(lats):
    return lats <= MOST_PERMUTES and lats & (lats - 1) == 0


def piece_of(tile):
    if by_permutes(lax.axis_size("lat")):
        return lax.bitwise_xor(tile, lax.axis_index("lat"))
    return tile


def sent(pieces):
    lats = len(pieces)
    if by_permutes(lats):
        moved = [pieces[0]]
        for k in range(1, lats):
            moved.append(lax.ppermute(pieces[k], "lat", [(i, i ^ k) for i in range(lats)]))
        return moved
    whole = lax.all_to_all(jnp.stack(pieces), "lat", split_axis=0, concat_axis=0, tiled=True)
    return [whole[k] for k in range(lats)]


def pack_kernel(
    dest_hbm,
    row_hbm,
    col_hbm,
    weight_hbm,
    obs_hbm,
    precision_hbm,
    noisy_hbm,
    near_ref,
    code_ref,
    *refs,
):
    *piece_refs, chunk_ref, dest_ref, row_ref, col_ref, weight_ref, obs_ref, precision_ref, scale_ref, sems = refs
    pairs = (
        (dest_hbm, dest_ref),
        (row_hbm, row_ref),
        (col_hbm, col_ref),
        (weight_hbm, weight_ref),
        (obs_hbm, obs_ref),
        (precision_hbm, precision_ref),
        (noisy_hbm, near_ref),
    )
    copies = [pltpu.make_async_copy(source, target, sems.at[n]) for n, (source, target) in enumerate(pairs)]
    for copy in copies:
        copy.start()
    core = lax.axis_index("ch")
    blocks, obs, _ = weight_ref.shape
    half = obs_ref.shape[1]
    first_meta = obs + CAP * half

    def clear(piece, _):
        chunk_ref[piece] = jnp.zeros(chunk_ref.shape[1:], BF16)
        return 0

    lax.fori_loop(0, chunk_ref.shape[0], clear, 0)
    for copy in copies[:-1]:
        copy.wait()
    scale_ref[...] = precision_ref[...].astype(F32)
    meta_rows = lax.broadcasted_iota(jnp.int32, (META, obs), 0)

    def pack(b, _):
        dest = dest_ref[b]
        rank = lax.fori_loop(0, b, lambda j, n: n + (dest_ref[j] == dest).astype(jnp.int32), 0)
        piece = piece_of(dest)
        chunk_ref[piece, pl.ds(pl.multiple_of(obs + rank * half, 16), half), :] = obs_ref[b]
        code_ref[pl.ds(b, 1), :] = jnp.full((1, 128), (piece * CAP + rank).astype(F32))

        @pl.when(rank == core)
        def _():
            chunk_ref[piece, 0:obs, :] = weight_ref[b]
            row = row_ref[b].astype(F32)
            high = lax.div(col_ref[b], 16).astype(F32)
            low = lax.rem(col_ref[b], 16).astype(F32)
            meta = jnp.where(
                meta_rows == 0,
                jnp.broadcast_to(scale_ref[pl.ds(b, 1), :], (META, obs)),
                jnp.where(meta_rows == 1, row, jnp.where(meta_rows == 2, high, low)),
            )
            chunk_ref[piece, first_meta : first_meta + META, :] = meta.astype(BF16)

        return 0

    lax.fori_loop(0, blocks, pack, 0)
    for k, piece_ref in enumerate(piece_refs):
        piece_ref[...] = chunk_ref[k]
    copies[-1].wait()


def join_kernel(*refs):
    *piece_refs, whole_ref = refs
    for k, piece_ref in enumerate(piece_refs):
        whole_ref[k] = piece_ref[...]


def prep_kernel(own_ref, other_ref, x_ref, tail_ref, flat_ref):
    core = lax.axis_index("ch")
    half, rows, width = own_ref.shape

    def place(ref, first):
        for part in range(width // 128):
            piece = ref[:, :, part * 128 : (part + 1) * 128].astype(F32)
            flat_ref[part, pl.ds(pl.multiple_of(first * rows, 8), half * rows), :] = piece.reshape(half * rows, 128)

    place(own_ref, core * half)
    place(other_ref, (1 - core) * half)
    for h in range(rows):
        for part in range(width // 128):
            plane = flat_ref[part, pl.ds(h, 2 * half, stride=rows), :]
            x_ref[h, part * 128 : (part + 1) * 128, :] = plane.T.astype(BF16)
    write_tails(x_ref, tail_ref)


def row_pair(src_ref, w_ref, first):
    c = src_ref.shape[-1]
    wide = src_ref.shape[1]
    lhs = jnp.concatenate([src_ref[first + k] for k in range(4)], axis=1)
    y = jnp.dot(lhs, w_ref[...], preferred_element_type=F32)
    out = []
    for row in range(2):
        left, mid, right = (y[:, (2 * b + row) * c : (2 * b + row + 1) * c] for b in range(3))
        out.append(pltpu.roll(left, 1, 0) + mid + pltpu.roll(right, wide - 1, 0))
    return out


def own_row_pair(src_ref, w_ref, base, first):
    c = src_ref.shape[-1]
    wide = src_ref.shape[1]
    width = base.shape[0]
    lhs = jnp.concatenate([src_ref[first + k] for k in range(4)], axis=1)
    y = jnp.dot(lhs, w_ref[...], preferred_element_type=F32)
    y = pltpu.roll(y[:, 0:c], 1, 0) + y[:, c : 2 * c] + pltpu.roll(y[:, 2 * c : 3 * c], wide - 1, 0)
    out = base - guide_rate * y[0:width, :]
    return [out[at : at + 128, :].T for at in range(0, width, 128)]


def inside(ext_row, ext_rows):
    at = lax.axis_index("lat")
    last = lax.axis_size("lat") - 1
    return ((ext_row > 0) | (at > 0)) & ((ext_row < ext_rows - 1) | (at < last))


def activate(y, bias):
    pre = y + bias
    s = 1.0 / (1.0 + jnp.exp(-pre))
    return pre * s, s * (1.0 + pre * (1.0 - s))


def copy_row(target_ref, at, x_ref, tail_ref, row):
    width = x_ref.shape[1]
    target_ref[at, 0:width, :] = x_ref[row]
    target_ref[at, width : width + TAIL, :] = tail_ref[row]


def fill_end(ext_ref, end, x_ref, tail_ref, halo_ref):
    rows = x_ref.shape[0]
    for i in range(2):
        ext_ref[2 * end + i] = halo_ref[i]
        copy_row(ext_ref, 2 * (1 - end) + i, x_ref, tail_ref, (rows - 2) * end + i)


def fill_between(between_ref, end, new, kept_ref):
    for i in range(2):
        between_ref[2 * end + i] = new[i]
        between_ref[2 * (1 - end) + i] = kept_ref[2 * end + i]


def forward_middle_kernel(
    x_ref,
    tail_ref,
    kin_ref,
    kout_ref,
    bias_ref,
    slope_ref,
    kept_ref,
    den_ref,
    w1_ref,
    w2_ref,
    ext_ref,
    hidden_ref,
):
    rows, width, _ = x_ref.shape
    forward_taps(w1_ref, w2_ref, kin_ref, kout_ref)
    for h in range(rows):
        copy_row(ext_ref, h, x_ref, tail_ref, h)
    bias = bias_ref[...]
    for g in range((rows - 2) // 2):
        for i, y in enumerate(row_pair(ext_ref, w1_ref, 2 * g)):
            hidden, slope = activate(y, bias)
            slope_ref[2 * g + i] = slope
            hidden_ref[2 * g + i] = hidden.astype(BF16)
    for i in range(2):
        kept_ref[i] = hidden_ref[i]
        kept_ref[2 + i] = hidden_ref[rows - 4 + i]
    for g in range((rows - 4) // 2):
        for i, y in enumerate(row_pair(hidden_ref, w2_ref, 2 * g)):
            den_ref[2 * g + i] = (x_ref[2 + 2 * g + i].astype(F32) + y[0:width, :]).astype(BF16)


def forward_end(end, x_ref, tail_ref, halo_ref, kept_ref, w1_ref, w2_ref, bias_ref, slope_ref, ext_ref, between_ref):
    rows, width, _ = x_ref.shape
    fill_end(ext_ref, end, x_ref, tail_ref, halo_ref)
    bias = bias_ref[...]
    new = []
    for i, y in enumerate(row_pair(ext_ref, w1_ref, 0)):
        hidden, slope = activate(y, bias)
        slope_ref[i] = slope
        new.append(jnp.where(inside(rows * end + i, rows + 2), hidden, 0.0).astype(BF16))
    fill_between(between_ref, end, new, kept_ref)
    return [
        (x_ref[(rows - 2) * end + i].astype(F32) + y[0:width, :]).astype(BF16)
        for i, y in enumerate(row_pair(between_ref, w2_ref, 0))
    ]


def forward_own_kernel(
    x_ref, tail_ref, halo_ref, kept_ref, w1_ref, w2_ref, bias_ref, slope_ref, den_ref, ext_ref, between_ref
):
    core = lax.axis_index("ch")
    den = forward_end(
        core, x_ref, tail_ref, halo_ref, kept_ref, w1_ref, w2_ref, bias_ref, slope_ref, ext_ref, between_ref
    )
    for i in range(2):
        den_ref[i] = den[i]


def forward_kernel(
    x_ref,
    tail_ref,
    halo_ref,
    kept_ref,
    w1_ref,
    w2_ref,
    bias_ref,
    den_middle_ref,
    den_own_ref,
    block_ref,
    other_block_ref,
    slope_ref,
    base_ref,
    g_ref,
    gtail_ref,
    *refs,
):
    *inn_refs, ext_ref, between_ref, den_ref, field_ref, turned_ref, value_ref, scale_ref, inn_ref, code_ref = refs
    core = lax.axis_index("ch")
    rows, width, c = x_ref.shape
    half = inn_refs[0].shape[1]
    sources, obs = block_ref.shape[0], block_ref.shape[2]

    def read(source, cap, first, count):
        at = slice(first, first + count)
        return jnp.where(core == cap, block_ref[source, at, :], other_block_ref[source, at, :])

    def locate(source, cap):
        meta = read(source, cap, obs + c, META).astype(F32)
        code = meta[1:2, :] * 65536.0 + meta[2:3, :] * 16.0 + meta[3:4, :]
        code_ref[source * CAP + cap] = jnp.max(code).astype(jnp.int32)

    def turn(source, cap):
        slot = source * CAP + cap
        turned_ref[slot] = read(source, cap, 0, obs).T
        at = slice(obs + cap * half, obs + (cap + 1) * half)
        mine, theirs = block_ref[source, at, :], other_block_ref[source, at, :]
        low, high = jnp.where(core == 0, mine, theirs), jnp.where(core == 0, theirs, mine)
        value_ref[slot] = jnp.concatenate([low, high], axis=0).T
        row = read(source, cap, obs + c, META).astype(F32)[0:1, :]
        scale_ref[slot] = jnp.broadcast_to(row, (c, obs)).T

    def each(task):
        if sources <= 4:
            for source in range(sources):
                for cap in range(CAP):
                    task(source, cap)
            return

        def one(source, _):
            for cap in range(CAP):
                task(source, cap)
            return 0

        lax.fori_loop(0, sources, one, 0)

    each(locate)
    each(turn)
    end = 1 - core
    den = forward_end(
        end, x_ref, tail_ref, halo_ref, kept_ref, w1_ref, w2_ref, bias_ref, slope_ref, ext_ref, between_ref
    )
    for i in range(2):
        den_ref[(rows - 2) * end + i] = den[i].astype(F32)
        den_ref[(rows - 2) * core + i] = den_own_ref[i].astype(F32)
    for h in range(rows - 4):
        den_ref[2 + h] = den_middle_ref[h].astype(F32)
    for r in range(rows):
        field_ref[r] = jnp.zeros((width, c), F32)

    def observe(source, cap):
        slot = source * CAP + cap
        code = code_ref[slot]
        row = lax.shift_right_logical(code, 16)
        col = lax.bitwise_and(code, 65535)
        patch = jnp.concatenate([den_ref[row + i, pl.ds(col, PW), :] for i in range(PH)], axis=0).astype(BF16)
        predicted = jnp.dot(read(source, cap, 0, obs), patch, preferred_element_type=F32)
        residual = predicted - value_ref[slot].astype(F32)
        weighted = (residual * scale_ref[slot]).astype(BF16)
        pulled = jnp.dot(turned_ref[slot], weighted, preferred_element_type=F32)
        for i in range(PH):
            field_ref[row + i, pl.ds(col, PW), :] += pulled[i * PW : (i + 1) * PW, :]
        turned = residual.astype(BF16).T
        inn_ref[slot] = jnp.where(core == 0, turned[0:half], turned[half : 2 * half])

    each(observe)
    for source, out_ref in enumerate(inn_refs):
        for cap in range(CAP):
            out_ref[cap] = inn_ref[source * CAP + cap]

    for r in range(rows):
        field = field_ref[r]
        base_ref[r] = keep_rate * x_ref[r].astype(F32) + blend_rate * den_ref[r] - guide_rate * field
        g_ref[r] = field.astype(BF16)
    write_tails(g_ref, gtail_ref)


def backward_middle_kernel(
    x_ref,
    tail_ref,
    kin_ref,
    kout_ref,
    base_ref,
    slope_ref,
    kept_ref,
    out_ref,
    w3_ref,
    w4_ref,
    ext_ref,
    grad_ref,
):
    rows = x_ref.shape[0]
    backward_taps(w3_ref, w4_ref, kin_ref, kout_ref)
    for h in range(rows):
        copy_row(ext_ref, h, x_ref, tail_ref, h)
    for g in range((rows - 2) // 2):
        for i, y in enumerate(row_pair(ext_ref, w3_ref, 2 * g)):
            grad_ref[2 * g + i] = (y * slope_ref[2 * g + i]).astype(BF16)
    for i in range(2):
        kept_ref[i] = grad_ref[i]
        kept_ref[2 + i] = grad_ref[rows - 4 + i]
    for g in range((rows - 4) // 2):
        for part, plane in enumerate(own_row_pair(grad_ref, w4_ref, own_pair(base_ref[2 + 2 * g], base_ref[3 + 2 * g]), 2 * g)):
            out_ref[g, part] = plane


def backward_end(end, x_ref, tail_ref, halo_ref, kept_ref, w3_ref, w4_ref, base_ref, slope_ref, ext_ref, between_ref):
    rows = x_ref.shape[0]
    fill_end(ext_ref, end, x_ref, tail_ref, halo_ref)
    new = [
        jnp.where(inside(rows * end + i, rows + 2), y * slope_ref[i], 0.0).astype(BF16)
        for i, y in enumerate(row_pair(ext_ref, w3_ref, 0))
    ]
    fill_between(between_ref, end, new, kept_ref)
    base = own_pair(base_ref[(rows - 2) * end], base_ref[(rows - 2) * end + 1])
    return own_row_pair(between_ref, w4_ref, base, 0)


def backward_own_kernel(
    x_ref, tail_ref, halo_ref, kept_ref, w3_ref, w4_ref, base_ref, slope_ref, out_ref, ext_ref, between_ref
):
    planes = backward_end(
        lax.axis_index("ch"), x_ref, tail_ref, halo_ref, kept_ref, w3_ref, w4_ref, base_ref, slope_ref, ext_ref, between_ref
    )
    for part, plane in enumerate(planes):
        out_ref[part] = plane


def backward_kernel(
    x_ref,
    tail_ref,
    halo_ref,
    kept_ref,
    w3_ref,
    w4_ref,
    base_ref,
    slope_ref,
    out_middle_ref,
    out_own_ref,
    code_ref,
    *refs,
):
    *back_refs, next_hbm, inn_hbm, ext_ref, between_ref, flat_ref, next_sems, inn_sems = refs
    core = lax.axis_index("ch")
    rows = x_ref.shape[0]
    half = next_hbm.shape[0]
    parts = flat_ref.shape[0]

    def give(b, _):
        code = jnp.max(code_ref[pl.ds(b, 1), :]).astype(jnp.int32)
        for k, back_ref in enumerate(back_refs):

            @pl.when(lax.div(code, CAP) == k)
            def _():
                pltpu.make_async_copy(back_ref.at[lax.rem(code, CAP)], inn_hbm.at[b], inn_sems.at[b]).start()

        return 0

    def given(b, _):
        pltpu.make_async_copy(back_refs[0].at[0], inn_hbm.at[b], inn_sems.at[b]).wait()
        return 0

    def put(pair, part, plane):
        for i in range(2):
            flat_ref[part, pl.ds(2 * pair + i, half, stride=rows), :] = plane[i * half : (i + 1) * half]

    for part in range(parts):
        for g in range((rows - 4) // 2):
            put(1 + g, part, out_middle_ref[g, part])
        put((rows // 2 - 1) * core, part, out_own_ref[part])
    planes = backward_end(
        1 - core, x_ref, tail_ref, halo_ref, kept_ref, w3_ref, w4_ref, base_ref, slope_ref, ext_ref, between_ref
    )
    copies = []
    for part, plane in enumerate(planes):
        put((rows // 2 - 1) * (1 - core), part, plane)
        source = flat_ref.at[part].reshape(half, rows, 128)
        target = next_hbm.at[:, :, pl.ds(part * 128, 128)]
        copies.append(pltpu.make_async_copy(source, target, next_sems.at[part]))
        copies[-1].start()
    lax.fori_loop(0, inn_hbm.shape[0], give, 0, unroll=inn_hbm.shape[0] <= 8)
    for copy in copies:
        copy.wait()
    lax.fori_loop(0, inn_hbm.shape[0], given, 0)


def swapped(value):
    return lax.ppermute(value, "ch", [(0, 1), (1, 0)])


def from_row_neighbour(value):
    lats = lax.axis_size("lat")
    steps = ((0, -1), (1, 1))
    pairs = [
        (i * 2 + core, (i + step) * 2 + 1 - core) for i in range(lats) for core, step in steps if 0 <= i + step < lats
    ]
    return lax.ppermute(value, ("lat", "ch"), pairs)


def from_lon_neighbours(value):
    lons = lax.axis_size("lon")

    def move(step):
        pairs = [(j * 2 + core, (j + step) % lons * 2 + 1 - core) for j in range(lons) for core in range(2)]
        return lax.ppermute(value, ("lon", "ch"), pairs)

    if lons == 2:
        return move(1)
    at = lax.broadcasted_iota(jnp.int32, (1, TAIL, 1), 1)
    return jnp.where(at < TAIL // 2, move(-1), move(1))


def exchanged(x, tail):
    _, width, c = x.shape
    beside = from_lon_neighbours(tail)
    (edge,) = call(edge_kernel, [(shape((2, width + TAIL, c), BF16), VMEM)], [VMEM] * 2, [])(x, beside)
    mine = from_row_neighbour(edge)
    return beside, mine


def shape(dims, dtype):
    return jax.ShapeDtypeStruct(dims, dtype)


def body(
    noisy_state,
    kernel_in,
    bias_in,
    kernel_out,
    interp_weight,
    observed,
    obs_precision,
    dest_tile,
    row_offset,
    col_offset,
):
    half, rows, width = noisy_state.shape
    c = kernel_in.shape[-1]
    blocks, obs, _ = interp_weight.shape
    lats = lax.axis_size("lat")
    slots = lats * CAP
    wide = width + TAIL
    other = swapped(noisy_state)
    piece = (obs + CAP * half + META, obs)
    near, code, *pieces = call(
        pack_kernel,
        [(shape(noisy_state.shape, BF16), VMEM), (shape((blocks, 128), F32), VMEM)] + [(shape(piece, BF16), VMEM)] * lats,
        [HBM] * 7,
        [
            VMEM((lats, *piece), BF16),
            SMEM((blocks,), jnp.int32),
            SMEM((blocks,), jnp.int32),
            SMEM((blocks,), jnp.int32),
            VMEM(interp_weight.shape, BF16),
            VMEM(observed.shape, BF16),
            VMEM(obs_precision.shape, BF16),
            VMEM(obs_precision.shape, F32),
            pltpu.SemaphoreType.DMA((7,)),
        ],
    )(dest_tile, row_offset, col_offset, interp_weight, observed, obs_precision, noisy_state)
    pieces = sent(pieces)
    tail_shape = shape((rows, TAIL, c), BF16)
    x, tail = call(
        prep_kernel,
        [(shape((rows, width, c), BF16), VMEM), (tail_shape, VMEM)],
        [VMEM] * 2,
        [VMEM((width // 128, c * rows, 128), F32)],
    )(near, other)
    bias = bias_in.reshape(1, c)
    pair = shape((2, wide, c), F32)
    taps = shape((4 * c, 6 * c), BF16)
    own_taps = shape((4 * c, 3 * c), BF16)
    kept_shape = shape((4, wide, c), BF16)
    four_rows, most_rows, all_rows = VMEM((4, wide, c), BF16), VMEM((rows - 2, wide, c), BF16), VMEM((rows, wide, c), BF16)

    beside, mine = exchanged(x, tail)
    slope_middle, kept, den_middle, w1, w2 = call(
        forward_middle_kernel,
        [
            (shape((rows - 2, wide, c), F32), VMEM),
            (kept_shape, VMEM),
            (shape((rows - 4, width, c), BF16), VMEM),
            (taps, VMEM),
            (taps, VMEM),
        ],
        [VMEM] * 5,
        [all_rows, most_rows],
    )(x, beside, kernel_in, kernel_out, bias)
    pieces, kept = lax.optimization_barrier((pieces, kept))
    (block,) = call(join_kernel, [(shape((lats, *piece), BF16), VMEM)], [VMEM] * lats, [])(*pieces)
    other_block = swapped(block)
    mine, kept, slope_middle, den_middle = lax.optimization_barrier((mine, kept, slope_middle, den_middle))
    others = swapped(mine)
    slope_own, den_own = call(
        forward_own_kernel, [(pair, VMEM), (shape((2, width, c), BF16), VMEM)], [VMEM] * 7, [four_rows, four_rows]
    )(x, beside, mine, kept, w1, w2, bias)
    slope_other, base, g, tail, *inn = call(
        forward_kernel,
        [
            (pair, VMEM),
            (shape((rows, width, c), F32), VMEM),
            (shape((rows, width, c), BF16), VMEM),
            (tail_shape, VMEM),
            *[(shape((CAP, half, obs), BF16), VMEM)] * lats,
        ],
        [VMEM] * 11,
        [
            four_rows,
            four_rows,
            VMEM((rows, width, c), F32),
            VMEM((rows, width, c), F32),
            VMEM((slots, obs, obs), BF16),
            VMEM((slots, obs, c), BF16),
            VMEM((slots, obs, c), F32),
            VMEM((slots, half, obs), BF16),
            SMEM((slots,), jnp.int32),
        ],
        {0: 2, 1: 3},
    )(x, beside, others, kept, w1, w2, bias, den_middle, den_own, block, other_block)

    back = sent(inn)
    beside, mine = exchanged(g, tail)
    parts = width // 128
    kept, out_middle, w3, w4 = call(
        backward_middle_kernel,
        [
            (kept_shape, VMEM),
            (shape(((rows - 4) // 2, parts, c, 128), F32), VMEM),
            (taps, VMEM),
            (own_taps, VMEM),
        ],
        [VMEM] * 6,
        [all_rows, most_rows],
    )(g, beside, kernel_in, kernel_out, base, slope_middle)
    mine, kept, out_middle = lax.optimization_barrier((mine, kept, out_middle))
    others = swapped(mine)
    (out_own,) = call(
        backward_own_kernel, [(shape((parts, c, 128), F32), VMEM)], [VMEM] * 8, [four_rows, four_rows]
    )(g, beside, mine, kept, w3, w4, base, slope_own)
    next_state, innovation = call(
        backward_kernel,
        [(shape((half, rows, width), F32), HBM), (shape(observed.shape, BF16), HBM)],
        [VMEM] * (11 + lats),
        [
            four_rows,
            four_rows,
            VMEM((parts, half * rows, 128), F32),
            pltpu.SemaphoreType.DMA((parts,)),
            pltpu.SemaphoreType.DMA((blocks,)),
        ],
    )(g, beside, others, kept, w3, w4, base, slope_other, out_middle, out_own, code, *back)
    return next_state, innovation


def solution(mesh):
    return jax.shard_map(
        body,
        mesh=mesh,
        in_specs=(
            P(("grp", "ch"), "lat", "lon"),
            P(),
            P(),
            P(),
            P(("grp", "lat", "lon"), None, None),
            P(("grp", "lat", "lon"), "ch", None),
            P(("grp", "lat", "lon"), None),
            P(("grp", "lat", "lon")),
            P(("grp", "lat", "lon")),
            P(("grp", "lat", "lon")),
        ),
        out_specs=(P(("grp", "ch"), "lat", "lon"), P(("grp", "lat", "lon"), "ch", None)),
        check_vma=False,
    )
```
